512 devices in a mesh: enc: 16 (over y, x_lo), slab: 32 (over x_hi, z, core).
Axes of the slice: x: 4 (x_hi: 2, x_lo: 2; x = x_hi * 2 + x_lo), y: 8, z: 8, core: 2. Of those that a mesh axis runs over, the one named last changes fastest.
Arguments:
- tokens: bfloat16 [32768, 1024], P(('slab', 'enc')), may hold values from -6 to 6
- cotangent: bfloat16 [32768, 1024], P(('slab', 'enc')), may hold values from -6 to 6
- w_qkv: bfloat16 [1024, 3072], P('slab', 'enc'), may hold values from -0.5 to 0.5
- w_out: bfloat16 [1024, 1024], P('enc', 'slab'), may hold values from -0.1875 to 0.1875
- mod_scale: float32 [1024], replicated, may hold values from -0.5 to 0.5
- mod_shift: float32 [1024], replicated, may hold values from -0.5 to 0.5
- mod_gate: float32 [1024], replicated, may hold values from 0.5 to 1.5
- counts: int32 [64], P('slab'), may hold values from 64 to 512
- edge_index: int32 [64, 128], P('slab'), may hold values from 0 to 1023
Outputs:
- grad_tokens: bfloat16 [32768, 1024], P(('slab', 'enc'))
- grad_qkv: float32 [1024, 3072], P('slab', 'enc')
- grad_out: float32 [1024, 1024], P('enc', 'slab')
The draws below stay inside these ranges and needn't reach their ends.
Inputs may be any that keep to these rules, and one draw needn't show every extreme that they name: The first counts[w] slots of window w hold voxels; the rest are padding. `edge_index`: A row index within the preceding slab's 2 * 512 rows.
All inputs are finite; a program needn't handle non-finite values.
Results may differ from the reference program's by a relative error of at most 0.023.
Values may be sent and summed in bfloat16 or wider, within the bound.
A program may use at most 64 MiB of HBM per device.

```python
import math
import jax
import jax.numpy as jnp
from jax import lax

D = 1024
HEADS = 16
HD = 64
WIN = 512
EDGE = 128
W_DEV = 2
NWIN = 64
TOKENS = 32768
N_ENC = 16


def common_direction(key):
    raw = jax.random.normal(jax.random.fold_in(key, 101), (D,), jnp.float32)
    raw = raw - jnp.mean(raw)
    return raw / jnp.sqrt(jnp.sum(raw * raw))


def draw_tokens(key, part):
    direction = common_direction(key)
    noise = jax.random.normal(jax.random.fold_in(key, 13), (TOKENS, D), jnp.float32)
    lowest = 0.55
    highest = 0.9
    noise = noise - jnp.sum(noise * direction[None, :], 1, keepdims=True) * direction[None, :]
    strength = jax.random.uniform(jax.random.fold_in(key, 14), (NWIN, 1), jnp.float32, lowest, highest)
    span = WIN // 8
    first = jax.random.randint(jax.random.fold_in(key, 15), (NWIN, 1), 0, span)
    second = (first + 1 + jax.random.randint(jax.random.fold_in(key, 16), (NWIN, 1), 0, span - 1)) % span
    position = jnp.arange(WIN, dtype=jnp.int32)[None, :]
    aligned = jnp.where(position == first, strength, jnp.where(position == second, strength - 0.005, 0.0))
    aligned = aligned.reshape(TOKENS, 1)
    rows = aligned * math.sqrt(D) * direction[None, :] + jnp.sqrt(1.0 - aligned * aligned) * noise
    return jnp.clip(rows, -6.0, 6.0).astype(jnp.bfloat16)


def draw_w_qkv(key, part):
    direction = common_direction(key)
    base = jax.random.normal(jax.random.fold_in(key, 22), (D, HEADS, 3, HD), jnp.float32)
    base = base / math.sqrt(D)
    head_dir = jax.random.normal(jax.random.fold_in(key, 23), (HEADS, HD), jnp.float32)
    head_dir = head_dir / jnp.sqrt(jnp.sum(head_dir * head_dir, 1, keepdims=True))
    strength = 1.8
    boost = strength * direction[:, None, None] * head_dir[None, :, :]
    extra = jnp.stack([boost, boost, jnp.zeros_like(boost)], 2)
    return jnp.clip(base + extra, -0.5, 0.5).reshape(D, 3 * D).astype(jnp.bfloat16)


def touch_ends(result, rng, low, high):
    longest = result.shape.index(max(result.shape))
    spots = []
    for shift in (0, 1):
        where = [jax.random.randint(jax.random.fold_in(rng, axis), (), 0, length) for axis, length in enumerate(result.shape)]
        where[longest] = (where[longest] + shift) % result.shape[longest]
        spots.append(tuple(where))
    return result.at[spots[0]].set(low).at[spots[1]].set(high)


def block_levels(own_key, shape, shards, least, high):
    loudness = 1.0
    for dim, shards_of in shards:
        heights = jax.random.uniform(jax.random.fold_in(jax.random.fold_in(own_key, 6), dim), (shards_of,), jnp.float32, least / len(shards), high / len(shards))
        loudness = loudness * jnp.repeat(jnp.exp(heights), shape[dim] // shards_of).reshape((-1,) + (1,) * (len(shape) - 1 - dim))
    return loudness


def scatter_about(rng, extent, scale, most, split=(), kind=jnp.bfloat16):
    result = scale * jax.random.normal(rng, extent, jnp.float32)
    if split:
        result = result * block_levels(rng, extent, split, -0.22, 0.18)
    return jnp.clip(result, -most, most).astype(kind)


def setup_inputs(seed: int = 0) -> dict:
    key_of = jax.random.split(jax.random.key(seed), 10)
    tokens = draw_tokens(jax.random.fold_in(key_of[9], 71), 0)
    cotangent = scatter_about(key_of[1], (TOKENS, D), 1.0, 6.0, ((0, 512),))
    w_qkv = draw_w_qkv(jax.random.fold_in(key_of[9], 71), 0)
    w_out = scatter_about(key_of[3], (D, D), D ** -0.5, 0.1875, ((0, 16), (1, 32)))
    mod_scale = jnp.clip(jax.random.uniform(key_of[4], (D,), jnp.float32, -0.5, 0.5), -0.5, 0.5)
    mod_shift = jnp.clip(jax.random.uniform(key_of[5], (D,), jnp.float32, -0.5, 0.5), -0.5, 0.5)
    mod_gate = jnp.clip(jax.random.uniform(key_of[6], (D,), jnp.float32, 0.5, 1.5), 0.5, 1.5)
    counts = touch_ends(jax.random.randint(key_of[7], (NWIN,), WIN // 8, WIN + 1), jax.random.fold_in(key_of[7], 1), WIN // 8, WIN).astype(jnp.int32)
    edge_index = touch_ends(jax.random.randint(key_of[8], (NWIN, EDGE), 0, W_DEV * WIN), jax.random.fold_in(key_of[8], 1), 0, (W_DEV * WIN) - 1).astype(jnp.int32)
    return {"tokens": tokens, "cotangent": cotangent, "w_qkv": w_qkv, "w_out": w_out, "mod_scale": mod_scale, "mod_shift": mod_shift, "mod_gate": mod_gate, "counts": counts, "edge_index": edge_index}


EPS = 1e-06

def rounded(value):
    return lax.optimization_barrier(value.astype(jnp.bfloat16)).astype(jnp.float32)

def statistics(features):
    widened = features.astype(jnp.float32)
    average = lax.optimization_barrier(jnp.mean(widened, 1, keepdims=True))
    centred = widened - average
    variance = lax.optimization_barrier(jnp.mean(centred * centred, 1, keepdims=True))
    inv_std = lax.rsqrt(variance + EPS)
    return (centred * inv_std, inv_std)

def attend(query, key_vals, edge_vals, counts, edge_live, upstream, out_rows):
    windows = counts.shape[0]
    row_count = query.shape[0]
    win_size = row_count // windows
    head_size = query.shape[1]
    factor = head_size ** (-0.5)
    query_win = query.reshape(windows, win_size, head_size).astype(jnp.float32)
    keys_all = jnp.concatenate([key_vals.reshape(windows, win_size, 2 * head_size), edge_vals], 1).astype(jnp.float32)
    key_part = keys_all[:, :, :head_size]
    value_part = keys_all[:, :, head_size:]
    position = jnp.arange(win_size, dtype=jnp.int32)
    own_live = position[None, :] < counts[:, None]
    key_live = jnp.concatenate([own_live, jnp.broadcast_to(edge_live[:, None], (windows, edge_vals.shape[1]))], 1)
    row_live = own_live.astype(jnp.float32)[:, :, None]
    scores = jnp.einsum('wqd,wkd->wqk', query_win, key_part) * factor
    scores = jnp.where(key_live[:, None, :], scores, -1000000000.0)
    largest = lax.optimization_barrier(jnp.max(scores, -1, keepdims=True))
    exponent = jnp.exp(scores - largest)
    softmax_p = exponent / lax.optimization_barrier(jnp.sum(exponent, -1, keepdims=True))
    weights_b = rounded(softmax_p)
    attended = (jnp.einsum('wqk,wkd->wqd', weights_b, value_part) * row_live).astype(jnp.bfloat16)
    attended = attended.reshape(row_count, head_size)
    grad_att = jnp.dot(upstream, out_rows.T, preferred_element_type=jnp.float32).reshape(windows, win_size, head_size)
    grad_att = rounded(grad_att * row_live)
    grad_prob = jnp.einsum('wqd,wkd->wqk', grad_att, value_part)
    grad_value = jnp.einsum('wqk,wqd->wkd', weights_b, grad_att)
    grad_score = rounded(softmax_p * (grad_prob - lax.optimization_barrier(jnp.sum(grad_prob * softmax_p, -1, keepdims=True))) * factor)
    grad_query = jnp.einsum('wqk,wkd->wqd', grad_score, key_part)
    grad_key = jnp.einsum('wqk,wqd->wkd', grad_score, query_win)
    grad_pair = jnp.concatenate([grad_key, grad_value], -1)
    own_pair = grad_pair[:, :win_size].reshape(row_count, 2 * head_size)
    return (attended, grad_query.reshape(row_count, head_size), own_pair, grad_pair[:, win_size:])

def reference(tokens, cotangent, w_qkv, w_out, mod_scale, mod_shift, mod_gate, counts, edge_index):
    row_block = W_DEV * WIN
    normal_x, inv_std = statistics(tokens)
    gain = 1.0 + mod_scale
    normed = (normal_x * gain + mod_shift).astype(jnp.bfloat16)
    upstream = (cotangent.astype(jnp.float32) * mod_gate).astype(jnp.bfloat16)
    windows = counts.shape[0]
    slab_of = jnp.arange(windows, dtype=jnp.int32) // W_DEV
    edge_rows = (jnp.maximum(slab_of - 1, 0) * row_block).astype(jnp.int32)[:, None] + edge_index
    flat_rows = edge_rows.reshape(-1).astype(jnp.int32)
    edge_live = slab_of > 0
    group_heads = HEADS // N_ENC
    wq_groups = w_qkv.reshape(D, N_ENC, group_heads * 3 * HD).transpose(1, 0, 2)
    wo_groups = w_out.reshape(N_ENC, group_heads * HD, D)

    def per_group(running, weights):
        weight_in, weight_out = weights
        projected = jnp.dot(normed, weight_in, preferred_element_type=jnp.float32).astype(jnp.bfloat16)
        pieces = []
        outputs = []
        for head_pos in range(group_heads):
            block = projected[:, head_pos * 3 * HD:(head_pos + 1) * 3 * HD]
            key_vals = block[:, HD:]
            edge_vals = key_vals[flat_rows].reshape(windows, EDGE, 2 * HD)
            attended, grad_query, own_pair, edge_pair = attend(block[:, :HD], key_vals, edge_vals, counts, edge_live, upstream, weight_out[head_pos * HD:(head_pos + 1) * HD])
            own_pair = own_pair.at[flat_rows].add(edge_pair.reshape(-1, 2 * HD))
            pieces.append(jnp.concatenate([grad_query, own_pair], 1))
            outputs.append(attended)
        grad_proj = jnp.concatenate(pieces, 1).astype(jnp.bfloat16)
        attended_all = jnp.concatenate(outputs, 1)
        grad_q = jnp.dot(normed.T, grad_proj, preferred_element_type=jnp.float32)
        grad_o = jnp.dot(attended_all.T, upstream, preferred_element_type=jnp.float32)
        partial_value = jnp.dot(grad_proj, weight_in.T, preferred_element_type=jnp.float32)
        return (running + rounded(partial_value), (grad_q, grad_o))
    start_sum = jnp.zeros((tokens.shape[0], D), jnp.float32)
    grad_normed, (grad_q_all, grad_o_all) = lax.scan(per_group, start_sum, (wq_groups, wo_groups))
    grad_hat = grad_normed * gain
    grad_tokens = cotangent.astype(jnp.float32) + inv_std * (grad_hat - lax.optimization_barrier(jnp.mean(grad_hat, 1, keepdims=True)) - normal_x * lax.optimization_barrier(jnp.mean(grad_hat * normal_x, 1, keepdims=True)))
    grad_qkv = grad_q_all.transpose(1, 0, 2).reshape(D, 3 * D)
    grad_out = grad_o_all.reshape(D, D)
    return (grad_tokens.astype(jnp.bfloat16), grad_qkv, grad_out)
```

```python
import functools

import jax
import jax.numpy as jnp
from jax import lax
from jax.experimental import pallas as pl
from jax.experimental.pallas import tpu as pltpu
from jax.sharding import PartitionSpec as P

HD = 64
EPS = 1e-06
NEG = -1000000000.0
MESH = pl.DeviceIdType.MESH
F32 = jnp.float32
BF16 = jnp.bfloat16


def dot(a, b, dims=((1,), (0,))):
    return lax.dot_general(a, b, (dims, ((), ())), preferred_element_type=F32)


def kernel(
    ny, nxh, nz, win, edge,
    tok, cot, wq, wo, scale, shift, gate, counts, edges,
    out_tok, out_w,
    nrm, nx, inv, act, xt, wbuf, meta_nat, meta_own, meta_next,
    kv, kvt, qa, oh, e_send, e_recv, g_send, g_recv, gkv, gg,
    pv_send, pv_recv, dwf, dwb, r1, s2, r2, s3, r3,
    f1s, f1r, f2s, f2r, wzs, wzr, wxs, wxr, wcs, wcr,
    ms, mr, es, er, gs, gr, dcs, dcr, dxs, dxr, dzs, dzr, ps, pr,
):
    ns = nxh * nz * 2
    nyh = ny // 2
    nxx = 2 * nxh
    own = tok.shape[0]
    blk = 2 * own
    d_model = tok.shape[1]
    wr = wq.shape[0]

    enc = lax.axis_index("enc")
    slab = lax.axis_index("slab")
    y, xl = enc // 2, enc % 2
    xh, z, c = slab // (2 * nz), (slab // 2) % nz, slab % 2
    x = xh * 2 + xl
    mine = xh * 2 * nz + z * 2 + xl
    after = (mine + 1) % ns
    before = (mine + ns - 1) % ns
    half = y // nyh

    def at(y_, xl_, xh_, z_, c_):
        return {"enc": y_ * 2 + xl_, "slab": xh_ * (2 * nz) + z_ * 2 + c_}

    def at_slab(s_, c_):
        return {"enc": y * 2 + s_ % 2, "slab": (s_ // 2) * 2 + c_}

    sibling = at(y, xl, xh, z, 1 - c)
    up = at((y + 1) % ny, xl, xh, z, c)
    down = at((y + ny - 1) % ny, xl, xh, z, c)

    def z_peer(j):
        return at(y, xl, xh, (z + j) % nz, c)

    def x_peer(j):
        xx = (x + j) % nxx
        return at(y, xx % 2, xx // 2, z, c)

    def copy(src, dst, send, recv, to):
        return pltpu.make_async_remote_copy(
            src_ref=src, dst_ref=dst, send_sem=send, recv_sem=recv, device_id=to, device_id_type=MESH
        )

    at_home = jnp.logical_and(c == xl, half == c)
    away = jnp.logical_not(at_home)
    diag = c == xl

    barrier = pltpu.get_barrier_semaphore()

    def greet(to):
        pl.semaphore_signal(barrier, inc=1, device_id=to, device_id_type=MESH)

    greet(sibling)
    greet(up)
    greet(down)
    for j in range(1, nz):
        greet(z_peer(j))
    for j in range(1, nxx):
        greet(x_peer(j))
    for k in range(2):
        greet(at_slab(after, k))
        greet(at_slab(before, k))

    @pl.when(half == c)
    def _():
        greet(at(y, 1 - xl, xh, z, xl))

    @pl.when(jnp.logical_and(half == c, xl != c))
    def _():
        greet(at(y, xl, xh, z, xl))

    for yy in range(ny):

        @pl.when(jnp.logical_or(away, yy != y))
        def _():
            greet(at(yy, c, xh, z, half))

    greeted = 3 + (nz - 1) + (nxx - 1) + 4 + (ny + 1) - 2 * at_home.astype(jnp.int32)

    widened = tok[...].astype(F32)
    average = jnp.mean(widened, 1, keepdims=True)
    centred = widened - average
    variance = jnp.mean(centred * centred, 1, keepdims=True)
    inv_std = lax.rsqrt(variance + EPS)
    normal = centred * inv_std
    gain = 1.0 + scale[...]
    nx[...] = normal
    inv[...] = jnp.broadcast_to(inv_std, inv.shape)
    nrm[0] = (normal * gain + shift[...]).astype(BF16)
    nrm[1] = (cot[...].astype(F32) * gate[...]).astype(BF16)

    hd = wo.shape[0]
    eye = (
        lax.broadcasted_iota(jnp.int32, (wr, wr), 0) == lax.broadcasted_iota(jnp.int32, (wr, wr), 1)
    ).astype(F32).astype(BF16)
    wo_t = dot(eye, wo[...], ((1,), (1,))).astype(BF16)
    wq_here = wq[...]
    wbuf[xl, xh, z, c] = jnp.concatenate([wq_here[:, hd : 3 * hd], wq_here[:, :hd], wo_t], 1)

    meta_nat[...] = jnp.zeros(meta_nat.shape, jnp.int32)
    meta_nat[0:2, :] = edges[...]
    meta_nat[2:3, :] = jnp.full((1, edge), counts[0], jnp.int32)
    meta_nat[3:4, :] = jnp.full((1, edge), counts[1], jnp.int32)

    @pl.when(diag)
    def _():
        meta_own[...] = meta_nat[...]

    r_own = (y % nyh) * blk + xl * own
    home = at(y, c, xh, z, half)

    @pl.when(at_home)
    def _():
        for p in range(2):
            act[p, pl.ds(pl.multiple_of(r_own, own), own), :] = nrm[p]

    pl.semaphore_wait(barrier, greeted)

    def f1(p):
        return copy(
            nrm.at[p],
            act.at[p, pl.ds(pl.multiple_of(r_own, own), own)],
            f1s.at[p],
            f1r.at[xl, p],
            home,
        )

    for p in range(2):

        @pl.when(away)
        def _():
            f1(p).start()

    def wz(j):
        return copy(wbuf.at[xl, xh, z, c], wbuf.at[xl, xh, z, c], wzs.at[j], wzr.at[j], z_peer(j))

    def wz_in(j):
        block = wbuf.at[xl, xh, (z + nz - j) % nz, c]
        return copy(block, block, wzs.at[j], wzr.at[j], z_peer(j))

    for j in range(1, nz):
        wz(j).start()

    def meta_out(n):
        if n == 0:
            return copy(meta_nat, meta_own, ms.at[0], mr.at[0], sibling)
        return copy(meta_nat, meta_next, ms.at[n], mr.at[1], at_slab(before, n - 1))

    @pl.when(diag)
    def _():
        for n in range(3):
            meta_out(n).start()

    def f1_in(h, p):
        rows = pl.ds(pl.multiple_of((y % nyh) * blk + h * own, own), own)
        return copy(nrm.at[p], act.at[p, rows], f1s.at[p], f1r.at[h, p], sibling)

    def ring(i, p, way):
        rows = pl.ds(pl.multiple_of(i * blk, blk), blk)
        return copy(
            act.at[p, rows], act.at[p, rows], f2s.at[i, p, way], f2r.at[i, p], up if way == 0 else down
        )

    here = y % nyh

    for p in range(2):
        for h in range(2):

            @pl.when(jnp.logical_and(half == c, jnp.logical_or(away, h != xl)))
            def _():
                f1_in(h, p).wait_recv()

        @pl.when(half == c)
        def _():
            ring(here, p, p).start()

    if nyh > 1:

        @pl.when(half == c)
        def _():
            ring(here, 1, 0).start()
            ring(here, 0, 1).start()

    def turn(i):
        rows = pl.ds(pl.multiple_of(i * blk, blk), blk)
        for p in range(2):
            cols = pl.ds(pl.multiple_of(p * win + i * blk, blk), blk)
            xt[:, cols] = act[p, rows, :].T

    def project(i):
        rows = pl.ds(pl.multiple_of(i * blk, blk), blk)
        lane = lax.broadcasted_iota(jnp.int32, (blk, 2 * HD), 1)
        row = lax.broadcasted_iota(jnp.int32, (blk, 2 * HD), 0) + i * blk
        live = row < jnp.where(c == 0, meta_own[2:3, :], meta_own[3:4, :])
        for h in range(2):
            w = wbuf[h].reshape(d_model, 4 * HD)
            from_normed = dot(act[0, rows, :], w)
            from_upstream = dot(act[1, rows, :], w[:, 2 * HD :])
            kv[h, rows, :] = from_normed[:, : 2 * HD].astype(BF16)
            query = from_normed[:, 2 * HD :].astype(BF16).astype(F32) * (HD**-0.5)
            qa[h, 0, rows, :] = jnp.where(lane < HD, query, 0.0).astype(BF16)
            qa[h, 1, rows, :] = jnp.where(
                jnp.logical_and(lane >= HD, live), from_upstream, 0.0
            ).astype(BF16)

    @pl.when(half == c)
    def _():
        turn(here)

    def wx(j):
        block = wbuf.at[xl, xh, :, c]
        return copy(block, block, wxs.at[j], wxr.at[j], x_peer(j))

    def wx_in(j):
        xx = (x + nxx - j) % nxx
        block = wbuf.at[xx % 2, xx // 2, :, c]
        return copy(block, block, wxs.at[j], wxr.at[j], x_peer(j))

    def wc(k):
        block = wbuf.at[:, :, :, k]
        return copy(block, block, wcs, wcr, sibling)

    def weights_x():
        for j in range(1, nz):
            wz_in(j).wait_recv()
        for j in range(1, nxx):
            wx(j).start()

    def weights_core():
        for j in range(1, nxx):
            wx_in(j).wait_recv()
        wc(c).start()

    def weights_done():
        wc(1 - c).wait_recv()

        @pl.when(jnp.logical_not(diag))
        def _():
            meta_out(0).wait_recv()

        meta_out(1).wait_recv()

    def far(i):
        return (y + ny - i - nyh * c) % ny == nyh

    stages = [weights_x, weights_core, weights_done]
    for t in range(1, nyh + 1):
        if t == nyh:
            for stage in stages:
                stage()
            stages = []

            @pl.loop(0, nyh)
            def _(i):
                @pl.when(jnp.logical_not(far(i)))
                def _():
                    project(i)

        elif stages:
            stages.pop(0)()
        from_below = (y + 2 * ny - t - nyh * c) % ny
        from_above = (y + 2 * ny + t - nyh * c) % ny
        has_below = from_below < nyh
        has_above = from_above < nyh

        @pl.when(has_below)
        def _():
            ring(from_below, 0, 0).wait_recv()
            if t < nyh:
                ring(from_below, 0, 0).start()

        @pl.when(has_above)
        def _():
            ring(from_above, 1, 1).wait_recv()
            if t < nyh:
                ring(from_above, 1, 1).start()

        if t < nyh:

            @pl.when(has_below)
            def _():
                ring(from_below, 1, 0).wait_recv()
                if t < nyh - 1:
                    ring(from_below, 1, 0).start()

            @pl.when(has_above)
            def _():
                ring(from_above, 0, 1).wait_recv()
                if t < nyh - 1:
                    ring(from_above, 0, 1).start()

            @pl.when(has_above)
            def _():
                turn(from_above)

        @pl.when(has_below)
        def _():
            turn(from_below)
            if t == nyh:
                project(from_below)

    row_id = lax.broadcasted_iota(jnp.int32, (win, edge), 0) + c * win
    for k in range(2):
        oh[:, k * edge : (k + 1) * edge] = (row_id == meta_next[k : k + 1, :]).astype(F32).astype(BF16)
    for h in range(2):
        kvt[h, :, :win] = kv[h, :win, :].T
    for h in range(2):
        picked = dot(kvt[h, :, :win], oh[...]).astype(BF16)
        for k in range(2):
            e_send[k, h] = picked[:, k * edge : (k + 1) * edge]

    def edge_out(k):
        return copy(e_send.at[k], e_recv.at[c], es.at[k], er.at[c], at_slab(after, k))

    def edge_in(k):
        return copy(e_send.at[k], e_recv.at[k], es.at[k], er.at[k], sibling)

    for k in range(2):
        edge_out(k).start()
    for k in range(2):
        edge_in(k).wait_recv()
    for h in range(2):
        arrived = e_recv[0, h].astype(F32) + e_recv[1, h].astype(F32)
        kvt[h, :, win:] = arrived.astype(BF16)
        kv[h, win:, :] = arrived.T.astype(BF16)

    keys = win + edge
    step = 256 if win % 256 == 0 else win
    has_edge = mine > 0
    count = jnp.where(c == 0, meta_own[2:3, :], meta_own[3:4, :])
    limit = jnp.concatenate([count] * (step // edge), 1)

    def attend(h):
        gkv[h] = jnp.zeros(gkv.shape[1:], F32)

        @pl.loop(0, win // step)
        def _(n):
            q_rows = pl.ds(pl.multiple_of(n * step, step), step)
            query = qa[h, 0, q_rows, :]
            g_att = qa[h, 1, q_rows, :]
            key_id = lax.broadcasted_iota(jnp.int32, (keys, step), 0)
            key_live = jnp.logical_or(
                key_id < limit, jnp.logical_and(key_id >= win, has_edge)
            )
            scores = jnp.where(key_live, dot(kv[h], query, ((1,), (1,))), NEG)
            exponent = jnp.exp(scores - jnp.max(scores, 0, keepdims=True))
            probs = exponent * (1.0 / jnp.sum(exponent, 0, keepdims=True))
            weights = probs.astype(BF16)
            g_prob = dot(kv[h], g_att, ((1,), (1,)))
            centre = jnp.sum(g_prob * probs, 0, keepdims=True)
            g_score = (probs * (g_prob - centre)).astype(BF16)
            lane = lax.broadcasted_iota(jnp.int32, (HD, step), 1) + n * step
            attended = jnp.where(lane < limit, dot(kvt[h, HD:, :], weights), 0.0)
            g_query = dot(kvt[h, :HD, :], g_score) * (HD**-0.5)
            pair = jnp.concatenate([g_query, attended], 0).T
            side = lax.broadcasted_iota(jnp.int32, (step, 2 * HD), 1)
            gg[h, q_rows, 2 * HD :] = jnp.where(side < HD, pair, 0.0).astype(BF16)
            low = pl.ds(pl.multiple_of(win + n * step, step), step)
            gg[h, low, 2 * HD :] = jnp.where(side >= HD, pair, 0.0).astype(BF16)
            gg[h, low, : 2 * HD] = jnp.zeros((step, 2 * HD), BF16)
            gkv[h] += dot(g_score, query) + dot(weights, g_att)

        g_send[h] = gkv[h, win:, :].astype(BF16)

    def grad_out(h, k):
        return copy(g_send.at[h], g_recv.at[h, c], gs.at[h, k], gr.at[h, c], at_slab(before, k))

    def grad_in(h, k):
        return copy(g_send.at[h], g_recv.at[h, k], gs.at[h, k], gr.at[h, k], sibling)

    for h in range(2):
        attend(h)
        for k in range(2):
            grad_out(h, k).start()
    for h in range(2):
        for k in range(2):
            grad_in(h, k).wait_recv()
        returned = dot(oh[...], g_recv[h].reshape(2 * edge, 2 * HD))
        gg[h, :win, : 2 * HD] = (gkv[h, :win, :] + returned).astype(BF16)

    def part_out(j):
        yy = nyh * c + j // 2
        return copy(pv_send.at[j], pv_recv.at[y], ps.at[j], pr.at[y], at(yy, j % 2, xh, z, xl))

    def part_in(yy):
        return copy(pv_send.at[0], pv_recv.at[yy], ps.at[0], pr.at[yy], sibling)

    def is_mine(j):
        return jnp.logical_and(at_home, enc == 2 * nyh * c + j)

    for b in range(nyh):
        rows = pl.ds(b * blk, blk)
        total = jnp.zeros((blk, d_model), F32)
        for h in range(2):
            total += dot(gg[h, rows, :], wbuf[h].reshape(d_model, 4 * HD), ((1,), (1,)))
        value = total.astype(BF16)
        for k in range(2):
            j = 2 * b + k
            pv_send[j] = value[k * own : (k + 1) * own, :]

            @pl.when(jnp.logical_not(is_mine(j)))
            def _():
                part_out(j).start()

            @pl.when(is_mine(j))
            def _():
                pv_recv[y] = pv_send[j]

    for h in range(2):
        grad_w = dot(xt[...], gg[h]).reshape(nxh, nz, 2, wr, 4 * HD)
        dwf[h] = grad_w
        dwb[h] = grad_w.astype(BF16)

    def dc(k):
        return copy(dwb.at[:, :, :, k], r1, dcs, dcr, sibling)

    dc(1 - c).start()
    dc(1 - c).wait_recv()
    for h in range(2):
        s2[h] = (dwf[h, :, :, c] + r1[h].astype(F32)).astype(BF16)

    def dx(j):
        xx = (x + j) % nxx
        return copy(s2.at[xx % 2, xx // 2], r2.at[j], dxs.at[j], dxr.at[j], x_peer(j))

    for j in range(1, nxx):
        dx(j).start()
    total = dwf[xl, xh, :, c] + r1[xl, xh].astype(F32)
    for j in range(1, nxx):
        dx(j).wait_recv()
        total += r2[j].astype(F32)
    dwf[0, 0, :, 0] = total
    s3[...] = total.astype(BF16)

    def dz(j):
        return copy(s3.at[(z + j) % nz], r3.at[j], dzs.at[j], dzr.at[j], z_peer(j))

    for j in range(1, nz):
        dz(j).start()
    final = dwf[0, 0, z, 0]
    for j in range(1, nz):
        dz(j).wait_recv()
        final += r3[j].astype(F32)
    out_w[...] = final

    mine_sum = jnp.zeros((own, d_model), F32)
    for yy in range(ny):

        @pl.when(jnp.logical_or(away, yy != y))
        def _():
            part_in(yy).wait_recv()

    for yy in range(ny):
        mine_sum += pv_recv[yy].astype(F32)
    g_hat = mine_sum * gain
    normal_own = nx[...]
    g_tok = cot[...].astype(F32) + inv[:, 0:1] * (
        g_hat
        - jnp.mean(g_hat, 1, keepdims=True)
        - normal_own * jnp.mean(g_hat * normal_own, 1, keepdims=True)
    )
    out_tok[...] = g_tok.astype(BF16)

    for p in range(2):

        @pl.when(away)
        def _():
            f1(p).wait_send()

    for j in range(1, nz):
        wz(j).wait_send()
        dz(j).wait_send()
    for j in range(1, nxx):
        wx(j).wait_send()
        dx(j).wait_send()
    wc(c).wait_send()
    dc(1 - c).wait_send()

    @pl.when(diag)
    def _():
        for n in range(3):
            meta_out(n).wait_send()

    for i in range(nyh):
        apart = (y + ny - i - nyh * c) % ny

        @pl.when(apart < nyh)
        def _():
            ring(i, 0, 0).wait_send()

        @pl.when(apart < nyh - 1)
        def _():
            ring(i, 1, 0).wait_send()

        back = (ny - apart) % ny

        @pl.when(back < nyh)
        def _():
            ring(i, 1, 1).wait_send()

        @pl.when(back < nyh - 1)
        def _():
            ring(i, 0, 1).wait_send()

    for k in range(2):
        edge_out(k).wait_send()
        for h in range(2):
            grad_out(h, k).wait_send()
    for j in range(2 * nyh):

        @pl.when(jnp.logical_not(is_mine(j)))
        def _():
            part_out(j).wait_send()


def on_device(nxh, tokens, cotangent, w_qkv, w_out, mod_scale, mod_shift, mod_gate, counts, edge_index):
    ny = lax.axis_size("enc") // 2
    nz = lax.axis_size("slab") // (2 * nxh)
    own, d_model = tokens.shape
    edge = edge_index.shape[1]
    win = own * ny
    wr = w_qkv.shape[0]
    nyh, nxx = ny // 2, 2 * nxh
    wide = 4 * HD
    dma = pltpu.SemaphoreType.DMA
    vmem = pl.BlockSpec(memory_space=pltpu.VMEM)
    scratch = [
        pltpu.VMEM((2, own, d_model), BF16),
        pltpu.VMEM((own, d_model), F32),
        pltpu.VMEM((own, 128), F32),
        pltpu.VMEM((2, win, d_model), BF16),
        pltpu.VMEM((d_model, 2 * win), BF16),
        pltpu.VMEM((2, nxh, nz, 2, wr, wide), BF16),
        pltpu.VMEM((8, edge), jnp.int32),
        pltpu.VMEM((8, edge), jnp.int32),
        pltpu.VMEM((8, edge), jnp.int32),
        pltpu.VMEM((2, win + edge, 2 * HD), BF16),
        pltpu.VMEM((2, 2 * HD, win + edge), BF16),
        pltpu.VMEM((2, 2, win, 2 * HD), BF16),
        pltpu.VMEM((win, 2 * edge), BF16),
        pltpu.VMEM((2, 2, 2 * HD, edge), BF16),
        pltpu.VMEM((2, 2, 2 * HD, edge), BF16),
        pltpu.VMEM((2, edge, 2 * HD), BF16),
        pltpu.VMEM((2, 2, edge, 2 * HD), BF16),
        pltpu.VMEM((2, win + edge, 2 * HD), F32),
        pltpu.VMEM((2, 2 * win, wide), BF16),
        pltpu.VMEM((2 * nyh, own, d_model), BF16),
        pltpu.VMEM((ny, own, d_model), BF16),
        pltpu.VMEM((2, nxh, nz, 2, wr, wide), F32),
        pltpu.VMEM((2, nxh, nz, 2, wr, wide), BF16),
        pltpu.VMEM((2, nxh, nz, wr, wide), BF16),
        pltpu.VMEM((2, nxh, nz, wr, wide), BF16),
        pltpu.VMEM((nxx, nz, wr, wide), BF16),
        pltpu.VMEM((nz, wr, wide), BF16),
        pltpu.VMEM((nz, wr, wide), BF16),
        dma((2,)), dma((2, 2)), dma((nyh, 2, 2)), dma((nyh, 2)),
        dma((nz,)), dma((nz,)), dma((nxx,)), dma((nxx,)), dma, dma,
        dma((3,)), dma((2,)), dma((2,)), dma((2,)), dma((2, 2)), dma((2, 2)),
        dma, dma, dma((nxx,)), dma((nxx,)), dma((nz,)), dma((nz,)),
        dma((2 * nyh,)), dma((ny,)),
    ]
    grad_tokens, grad_w = pl.pallas_call(
        functools.partial(kernel, ny, nxh, nz, win, edge),
        out_shape=(
            jax.ShapeDtypeStruct((own, d_model), BF16),
            jax.ShapeDtypeStruct((wr, wide), F32),
        ),
        in_specs=[vmem] * 7 + [pl.BlockSpec(memory_space=pltpu.SMEM), vmem],
        out_specs=(vmem, vmem),
        scratch_shapes=scratch,
        compiler_params=pltpu.CompilerParams(collective_id=0, has_side_effects=True),
    )(
        tokens, cotangent, w_qkv, w_out,
        mod_scale[None, :], mod_shift[None, :], mod_gate[None, :], counts, edge_index,
    )
    grad_qkv = jnp.concatenate([grad_w[:, 2 * HD : 3 * HD], grad_w[:, : 2 * HD]], 1)
    grad_out = grad_w[:, 3 * HD :].T
    return (grad_tokens, grad_qkv, grad_out)


def solution(mesh, nxh=2):
    placed = (
        P(("slab", "enc"), None),
        P(("slab", "enc"), None),
        P("slab", "enc"),
        P("enc", "slab"),
        P(),
        P(),
        P(),
        P("slab"),
        P("slab", None),
    )
    return jax.shard_map(
        functools.partial(on_device, nxh),
        mesh=mesh,
        in_specs=placed,
        out_specs=(P(("slab", "enc"), None), P("slab", "enc"), P("enc", "slab")),
        check_vma=False,
    )
```

```python
import functools

import jax
import jax.numpy as jnp
from jax import lax
from jax.experimental import pallas as pl
from jax.experimental.pallas import tpu as pltpu
from jax.sharding import PartitionSpec as P

HD = 64
EPS = 1e-06
NEG = -1000000000.0
MESH = pl.DeviceIdType.MESH
F32 = jnp.float32
BF16 = jnp.bfloat16


def dot(a, b, dims=((1,), (0,))):
    return lax.dot_general(a, b, (dims, ((), ())), preferred_element_type=F32)


def kernel(
    ny, nxh, nz, win, edge,
    tok_in, cot_in, wq_in, wo_in, scale_in, shift_in, gate_in, counts_in, edges_in,
    out_tok, out_qkv, out_o,
    tok, cot, wq, wo, scale, shift, gate, counts, edges,
    nrm, nx, inv, act, xt, wbuf, meta_nat, meta_own, meta_next,
    kv, kvt, qa, oh, e_send, e_recv, g_send, g_recv, wts, gsc, gkvb, qab,
    pvf, csd, crv, osd, oself, orv, dwf, dwb, r1, s2, r2, s3, r3,
    ins, f1s, f1r, f2s, f2r, wzs, wzr, wxs, wxr, wcs, wcr,
    ms, mr, es, er, gs, gr, dcs, dcr, dxs, dxr, dzs, dzr, ccs, ccr, ows, owr, oss, osr,
):
    ns = nxh * nz * 2
    nyh = ny // 2
    nxx = 2 * nxh
    own = tok.shape[0]
    blk = 2 * own
    d_model = tok.shape[1]
    wr = wq.shape[0]
    halfcol = d_model // 2

    enc = lax.axis_index("enc")
    slab = lax.axis_index("slab")
    y, xl = enc // 2, enc % 2
    xh, z, c = slab // (2 * nz), (slab // 2) % nz, slab % 2
    x = xh * 2 + xl
    mine = xh * 2 * nz + z * 2 + xl
    after = (mine + 1) % ns
    before = (mine + ns - 1) % ns
    half = y // nyh

    def at(y_, xl_, xh_, z_, c_):
        return {"enc": y_ * 2 + xl_, "slab": xh_ * (2 * nz) + z_ * 2 + c_}

    def at_slab(s_, c_):
        return {"enc": y * 2 + s_ % 2, "slab": (s_ // 2) * 2 + c_}

    sibling = at(y, xl, xh, z, 1 - c)
    up = at((y + 1) % ny, xl, xh, z, c)
    down = at((y + ny - 1) % ny, xl, xh, z, c)

    def z_peer(j):
        return at(y, xl, xh, (z + j) % nz, c)

    def x_peer(j):
        xx = (x + j) % nxx
        return at(y, xx % 2, xx // 2, z, c)

    def copy(src, dst, send, recv, to):
        return pltpu.make_async_remote_copy(
            src_ref=src, dst_ref=dst, send_sem=send, recv_sem=recv, device_id=to, device_id_type=MESH
        )

    at_home = jnp.logical_and(c == xl, half == c)
    away = jnp.logical_not(at_home)
    diag = c == xl

    pending = []

    def launch(make, when=None):
        if when is None:
            make().start()
            pending.append((make, None))
        else:

            @pl.when(when)
            def _():
                make().start()

            pending.append((make, when))

    def drain():
        for make, when in pending:
            if when is None:
                make().wait_send()
            else:

                @pl.when(when)
                def _():
                    make().wait_send()

    barrier = pltpu.get_barrier_semaphore()

    def greet(to):
        pl.semaphore_signal(barrier, inc=1, device_id=to, device_id_type=MESH)

    greet(sibling)
    greet(up)
    greet(down)
    for j in range(1, nz):
        greet(z_peer(j))
    for j in range(1, nxx):
        greet(x_peer(j))
    for k in range(2):
        greet(at_slab(after, k))
        greet(at_slab(before, k))

    @pl.when(half == c)
    def _():
        greet(at(y, 1 - xl, xh, z, xl))

    @pl.when(jnp.logical_and(half == c, xl != c))
    def _():
        greet(at(y, xl, xh, z, xl))

    above, below = (y + 1) % ny, (y + ny - 1) % ny
    greet(at(above, c, xh, z, half))
    greet(at(below, c, xh, z, half))

    @pl.when(away)
    def _():
        greet(at(y, c, xh, z, half))

    def count_of(flag):
        return flag.astype(jnp.int32)

    greeted = (
        3 + (nz - 1) + (nxx - 1) + 4 + 1
        - 2 * count_of(at_home)
        + 2 * count_of(half == c)
        + 2 * count_of(above // nyh == c)
        + 2 * count_of(below // nyh == c)
    )

    arrivals = [
        pltpu.make_async_copy(src, dst, ins.at[n])
        for n, (src, dst) in enumerate(
            (
                (tok_in, tok), (cot_in, cot), (wq_in, wq), (wo_in, wo), (scale_in, scale),
                (shift_in, shift), (gate_in, gate), (counts_in, counts), (edges_in, edges),
            )
        )
    ]
    for arrival in arrivals:
        arrival.start()
    for arrival in arrivals:
        arrival.wait()

    widened = tok[...].astype(F32)
    average = jnp.mean(widened, 1, keepdims=True)
    centred = widened - average
    variance = jnp.mean(centred * centred, 1, keepdims=True)
    inv_std = lax.rsqrt(variance + EPS)
    normal = centred * inv_std
    gain = 1.0 + scale[...]
    nx[...] = normal
    inv[...] = jnp.broadcast_to(inv_std, inv.shape)
    nrm[0] = (normal * gain + shift[...]).astype(BF16)
    nrm[1] = (cot[...].astype(F32) * gate[...]).astype(BF16)

    hd = HD
    wq_here = wq[...]
    wbuf[xl, xh, z, c] = jnp.concatenate([wq_here[:, hd : 3 * hd], wq_here[:, :hd], wo[...]], 1)

    meta_nat[...] = jnp.zeros(meta_nat.shape, jnp.int32)
    meta_nat[0:2, :] = edges[...]
    meta_nat[2:3, :] = jnp.full((1, edge), counts[0], jnp.int32)
    meta_nat[3:4, :] = jnp.full((1, edge), counts[1], jnp.int32)

    @pl.when(diag)
    def _():
        meta_own[...] = meta_nat[...]

    r_own = (y % nyh) * blk + xl * own
    home = at(y, c, xh, z, half)

    @pl.when(at_home)
    def _():
        for p in range(2):
            act[p, pl.ds(pl.multiple_of(r_own, own), own), :] = nrm[p]

    pl.semaphore_wait(barrier, greeted)

    def f1(p):
        return copy(
            nrm.at[p],
            act.at[p, pl.ds(pl.multiple_of(r_own, own), own)],
            f1s.at[p],
            f1r.at[xl, p],
            home,
        )

    for p in range(2):
        launch(functools.partial(f1, p), away)

    def wz(j):
        return copy(wbuf.at[xl, xh, z, c], wbuf.at[xl, xh, z, c], wzs.at[j], wzr.at[j], z_peer(j))

    def wz_in(j):
        block = wbuf.at[xl, xh, (z + nz - j) % nz, c]
        return copy(block, block, wzs.at[j], wzr.at[j], z_peer(j))

    for j in range(1, nz):
        launch(functools.partial(wz, j))

    def meta_out(n):
        if n == 0:
            return copy(meta_nat, meta_own, ms.at[0], mr.at[0], sibling)
        return copy(meta_nat, meta_next, ms.at[n], mr.at[1], at_slab(before, n - 1))

    for n in range(3):
        launch(functools.partial(meta_out, n), diag)

    def f1_in(h, p):
        rows = pl.ds(pl.multiple_of((y % nyh) * blk + h * own, own), own)
        return copy(nrm.at[p], act.at[p, rows], f1s.at[p], f1r.at[h, p], sibling)

    def ring(i, p, way):
        rows = pl.ds(pl.multiple_of(i * blk, blk), blk)
        return copy(
            act.at[p, rows], act.at[p, rows], f2s.at[i, p, way], f2r.at[i, p], up if way == 0 else down
        )

    here = y % nyh
    for i in range(nyh):
        apart = (y + ny - i - nyh * c) % ny
        back = (ny - apart) % ny
        pending.append((functools.partial(ring, i, 0, 0), apart < nyh))
        pending.append((functools.partial(ring, i, 1, 0), apart < nyh - 1))
        pending.append((functools.partial(ring, i, 1, 1), back < nyh))
        pending.append((functools.partial(ring, i, 0, 1), back < nyh - 1))

    for p in range(2):
        for h in range(2):

            @pl.when(jnp.logical_and(half == c, jnp.logical_or(away, h != xl)))
            def _():
                f1_in(h, p).wait_recv()

        @pl.when(half == c)
        def _():
            ring(here, p, p).start()

    if nyh > 1:

        @pl.when(half == c)
        def _():
            ring(here, 1, 0).start()
            ring(here, 0, 1).start()

    def turn(i):
        rows = pl.ds(pl.multiple_of(i * blk, blk), blk)
        for p in range(2):
            cols = pl.ds(pl.multiple_of(p * win + i * blk, blk), blk)
            xt[:, cols] = act[p, rows, :].T

    def project(i):
        rows = pl.ds(pl.multiple_of(i * blk, blk), blk)
        lane = lax.broadcasted_iota(jnp.int32, (blk, 2 * HD), 1)
        row = lax.broadcasted_iota(jnp.int32, (blk, 2 * HD), 0) + i * blk
        live = row < jnp.where(c == 0, meta_own[2:3, :], meta_own[3:4, :])
        for h in range(2):
            w = wbuf[h].reshape(d_model, 4 * HD)
            from_normed = dot(act[0, rows, :], w)
            from_upstream = dot(act[1, rows, :], w[:, 2 * HD :])
            kv[h, rows, :] = from_normed[:, : 2 * HD].astype(BF16)
            query = from_normed[:, 2 * HD :].astype(BF16).astype(F32) * (HD**-0.5)
            qa[h, 0, rows, :] = jnp.where(lane < HD, query, 0.0).astype(BF16)
            qa[h, 1, rows, :] = jnp.where(
                jnp.logical_and(lane >= HD, live), from_upstream, 0.0
            ).astype(BF16)

    @pl.when(half == c)
    def _():
        turn(here)

    def wx(j):
        block = wbuf.at[xl, xh, :, c]
        return copy(block, block, wxs.at[j], wxr.at[j], x_peer(j))

    def wx_in(j):
        xx = (x + nxx - j) % nxx
        block = wbuf.at[xx % 2, xx // 2, :, c]
        return copy(block, block, wxs.at[j], wxr.at[j], x_peer(j))

    def wc(k):
        block = wbuf.at[:, :, :, k]
        return copy(block, block, wcs, wcr, sibling)

    def weights_x():
        for j in range(1, nz):
            wz_in(j).wait_recv()
        for j in range(1, nxx):
            launch(functools.partial(wx, j))

    def weights_core():
        for j in range(1, nxx):
            wx_in(j).wait_recv()
        launch(functools.partial(wc, c))

    def weights_done():
        wc(1 - c).wait_recv()

        @pl.when(jnp.logical_not(diag))
        def _():
            meta_out(0).wait_recv()

        meta_out(1).wait_recv()

    def far(i):
        return (y + ny - i - nyh * c) % ny == nyh

    stages = [weights_x, weights_core, weights_done]
    for t in range(1, nyh + 1):
        if t == nyh:
            for stage in stages:
                stage()
            stages = []

            @pl.loop(0, nyh)
            def _(i):
                @pl.when(jnp.logical_not(far(i)))
                def _():
                    project(i)

        elif stages:
            stages.pop(0)()
        from_below = (y + 2 * ny - t - nyh * c) % ny
        from_above = (y + 2 * ny + t - nyh * c) % ny
        has_below = from_below < nyh
        has_above = from_above < nyh

        @pl.when(has_below)
        def _():
            ring(from_below, 0, 0).wait_recv()
            if t < nyh:
                ring(from_below, 0, 0).start()

        @pl.when(has_above)
        def _():
            ring(from_above, 1, 1).wait_recv()
            if t < nyh:
                ring(from_above, 1, 1).start()

        if t < nyh:

            @pl.when(has_below)
            def _():
                ring(from_below, 1, 0).wait_recv()
                if t < nyh - 1:
                    ring(from_below, 1, 0).start()

            @pl.when(has_above)
            def _():
                ring(from_above, 0, 1).wait_recv()
                if t < nyh - 1:
                    ring(from_above, 0, 1).start()

            @pl.when(has_above)
            def _():
                turn(from_above)

        @pl.when(has_below)
        def _():
            turn(from_below)
            if t == nyh:
                project(from_below)

    row_id = lax.broadcasted_iota(jnp.int32, (win, edge), 0) + c * win
    for k in range(2):
        oh[:, k * edge : (k + 1) * edge] = (row_id == meta_next[k : k + 1, :]).astype(F32).astype(BF16)
    for h in range(2):
        kvt[h, :, :win] = kv[h, :win, :].T
    for h in range(2):
        picked = dot(kvt[h, :, :win], oh[...]).astype(BF16)
        for k in range(2):
            e_send[k, h] = picked[:, k * edge : (k + 1) * edge]

    def edge_out(k):
        return copy(e_send.at[k], e_recv.at[c], es.at[k], er.at[c], at_slab(after, k))

    def edge_in(k):
        return copy(e_send.at[k], e_recv.at[k], es.at[k], er.at[k], sibling)

    for k in range(2):
        launch(functools.partial(edge_out, k))
    for k in range(2):
        edge_in(k).wait_recv()
    for h in range(2):
        arrived = e_recv[0, h].astype(F32) + e_recv[1, h].astype(F32)
        kvt[h, :, win:] = arrived.astype(BF16)
        kv[h, win:, :] = arrived.T.astype(BF16)

    keys = win + edge
    step = 256 if win % 256 == 0 else win
    has_edge = mine > 0
    count = jnp.where(c == 0, meta_own[2:3, :], meta_own[3:4, :])
    limit = jnp.concatenate([count] * (step // edge), 1)

    def scores_of(h):
        @pl.loop(0, win // step)
        def _(n):
            q_rows = pl.ds(pl.multiple_of(n * step, step), step)
            query = qa[h, 0, q_rows, :]
            g_att = qa[h, 1, q_rows, :]
            key_id = lax.broadcasted_iota(jnp.int32, (keys, step), 0)
            key_live = jnp.logical_or(
                key_id < limit, jnp.logical_and(key_id >= win, has_edge)
            )
            scores = jnp.where(key_live, dot(kv[h], query, ((1,), (1,))), NEG)
            exponent = jnp.exp(scores - jnp.max(scores, 0, keepdims=True))
            probs = exponent * (1.0 / jnp.sum(exponent, 0, keepdims=True))
            wts[h, :, q_rows] = probs.astype(BF16)
            g_prob = dot(kv[h], g_att, ((1,), (1,)))
            centre = jnp.sum(g_prob * probs, 0, keepdims=True)
            gsc[h, :, q_rows] = (probs * (g_prob - centre)).astype(BF16)

        g_send[h] = (dot(gsc[h, win:, :], qa[h, 0]) + dot(wts[h, win:, :], qa[h, 1])).astype(BF16)

    def grad_out(h, k):
        return copy(g_send.at[h], g_recv.at[h, c], gs.at[h, k], gr.at[h, c], at_slab(before, k))

    def grad_in(h, k):
        return copy(g_send.at[h], g_recv.at[h, k], gs.at[h, k], gr.at[h, k], sibling)

    for h in range(2):
        scores_of(h)
        for k in range(2):
            launch(functools.partial(grad_out, h, k))

    row_limit = jnp.concatenate([count] * (win // edge), 1)
    lane = lax.broadcasted_iota(jnp.int32, (HD, win), 1)
    side = lax.broadcasted_iota(jnp.int32, (win, 2 * HD), 1)
    for h in range(2):
        cols = pl.ds(h * 2 * HD, 2 * HD)
        attended = jnp.where(lane < row_limit, dot(kvt[h, HD:, :], wts[h]), 0.0)
        g_query = dot(kvt[h, :HD, :], gsc[h]) * (HD**-0.5)
        pair = jnp.concatenate([g_query, attended], 0).T
        qab[:win, cols] = jnp.where(side < HD, pair, 0.0).astype(BF16)
        qab[win:, cols] = jnp.where(side >= HD, pair, 0.0).astype(BF16)
    grad_w = dot(xt[...], qab[...]).reshape(nxh, nz, 2, wr, 4 * HD)
    for h in range(2):
        dwf[h, :, :, :, :, 2 * HD :] = grad_w[:, :, :, :, h * 2 * HD : (h + 1) * 2 * HD]

    for h in range(2):
        cols = pl.ds(h * 2 * HD, 2 * HD)
        own_pair = dot(gsc[h, :win, :], qa[h, 0]) + dot(wts[h, :win, :], qa[h, 1])
        for k in range(2):
            grad_in(h, k).wait_recv()
        returned = dot(oh[...], g_recv[h].reshape(2 * edge, 2 * HD))
        gkvb[:, cols] = (own_pair + returned).astype(BF16)

    def hops(way, part):
        return nyh if way == part else nyh - 1

    def chain_link(way, part, i):
        return copy(
            csd.at[way, part, i], crv.at[way, part, i], ccs.at[way, part, i], ccr.at[way, part, i],
            up if way == 0 else down,
        )

    def chain_end(way, part, i, h, yy):
        return copy(
            csd.at[way, part, i, pl.ds(h * own, own)], orv.at[way, part],
            ows.at[way, part, h], owr.at[way, part], at(yy, h, xh, z, xl),
        )

    def own_out(h):
        return copy(osd.at[h], oself, oss.at[h], osr, at(y, h, xh, z, xl))

    def chain(r):
        for way in range(2):
            yy = (y + (r if way == 0 else ny - r)) % ny
            i = (yy + ny - nyh * c) % ny
            held = i < nyh
            for part in (way, 1 - way):
                if r > hops(way, part):
                    continue

                @pl.when(held)
                def _():
                    total = pvf[i, :, part * halfcol : (part + 1) * halfcol]
                    if r < hops(way, part):
                        chain_link(way, part, i).wait_recv()
                        total += crv[way, part, i].astype(F32)
                    csd[way, part, i] = total.astype(BF16)

                if r > 1:
                    launch(functools.partial(chain_link, way, part, i), held)
                else:
                    for h in range(2):
                        launch(functools.partial(chain_end, way, part, i, h, yy), held)

    for b in range(nyh):
        rows = pl.ds(b * blk, blk)
        total = jnp.zeros((blk, d_model), F32)
        for h in range(2):
            cols = pl.ds(h * 2 * HD, 2 * HD)
            both = jnp.concatenate([gkvb[rows, cols], qab[rows, cols]], 1)
            total += dot(both, wbuf[h].reshape(d_model, 4 * HD), ((1,), (1,)))
        pvf[b] = total

    chain(nyh)

    @pl.when(half == c)
    def _():
        for h in range(2):
            osd[h] = pvf[here, h * own : (h + 1) * own, :].astype(BF16)

    for h in range(2):
        launch(
            functools.partial(own_out, h),
            jnp.logical_and(half == c, jnp.logical_or(xl != c, h != xl)),
        )

    @pl.when(at_home)
    def _():
        oself[...] = osd[xl]

    grad_w = dot(xt[:, :win], gkvb[...]).reshape(nxh, nz, 2, wr, 4 * HD)
    for h in range(2):
        dwf[h, :, :, :, :, : 2 * HD] = grad_w[:, :, :, :, h * 2 * HD : (h + 1) * 2 * HD]
        dwb[h] = dwf[h].astype(BF16)

    def dc(k):
        return copy(dwb.at[:, :, :, k], r1, dcs, dcr, sibling)

    launch(functools.partial(dc, 1 - c))
    if nyh > 1:
        chain(nyh - 1)
    dc(1 - c).wait_recv()
    for h in range(2):
        s2[h] = (dwf[h, :, :, c] + r1[h].astype(F32)).astype(BF16)

    def dx(j):
        xx = (x + j) % nxx
        return copy(s2.at[xx % 2, xx // 2], r2.at[j], dxs.at[j], dxr.at[j], x_peer(j))

    for j in range(1, nxx):
        launch(functools.partial(dx, j))
    for r in range(nyh - 2, 0, -1):
        chain(r)
    total = dwf[xl, xh, :, c] + r1[xl, xh].astype(F32)
    for j in range(1, nxx):
        dx(j).wait_recv()
        total += r2[j].astype(F32)
    dwf[0, 0, :, 0] = total
    s3[...] = total.astype(BF16)

    def dz(j):
        return copy(s3.at[(z + j) % nz], r3.at[j], dzs.at[j], dzr.at[j], z_peer(j))

    for j in range(1, nz):
        launch(functools.partial(dz, j))

    def owner_in(way, part):
        return copy(
            csd.at[way, part, 0, pl.ds(0, own)], orv.at[way, part],
            ows.at[way, part, 0], owr.at[way, part], sibling,
        )

    for way in range(2):
        for part in range(2):
            owner_in(way, part).wait_recv()

    @pl.when(away)
    def _():
        own_out_arrived = copy(osd.at[0], oself, oss.at[0], osr, sibling)
        own_out_arrived.wait_recv()

    mine_sum = oself[...].astype(F32) + jnp.concatenate(
        [orv[0, part].astype(F32) + orv[1, part].astype(F32) for part in range(2)], 1
    )
    g_hat = mine_sum * gain
    normal_own = nx[...]
    g_tok = cot[...].astype(F32) + inv[:, 0:1] * (
        g_hat
        - jnp.mean(g_hat, 1, keepdims=True)
        - normal_own * jnp.mean(g_hat * normal_own, 1, keepdims=True)
    )
    out_tok[...] = g_tok.astype(BF16)

    final = dwf[0, 0, z, 0]
    for j in range(1, nz):
        dz(j).wait_recv()
        final += r3[j].astype(F32)
    out_qkv[...] = jnp.concatenate([final[:, 2 * HD : 3 * HD], final[:, : 2 * HD]], 1)
    out_o[...] = final[:, 3 * HD :]

    drain()


def on_device(nxh, tokens, cotangent, w_qkv, w_out, mod_scale, mod_shift, mod_gate, counts, edge_index):
    ny = lax.axis_size("enc") // 2
    nz = lax.axis_size("slab") // (2 * nxh)
    own, d_model = tokens.shape
    edge = edge_index.shape[1]
    win = own * ny
    wr = w_qkv.shape[0]
    nyh, nxx = ny // 2, 2 * nxh
    wide = 4 * HD
    dma = pltpu.SemaphoreType.DMA
    vmem = pl.BlockSpec(memory_space=pltpu.VMEM)
    anywhere = pl.BlockSpec(memory_space=pl.ANY)
    keys = win + edge
    blk = 2 * own
    scratch = [
        pltpu.VMEM((own, d_model), BF16),
        pltpu.VMEM((own, d_model), BF16),
        pltpu.VMEM((wr, 3 * HD), BF16),
        pltpu.VMEM((wr, HD), BF16),
        pltpu.VMEM((1, d_model), F32),
        pltpu.VMEM((1, d_model), F32),
        pltpu.VMEM((1, d_model), F32),
        pltpu.SMEM((2,), jnp.int32),
        pltpu.VMEM((2, edge), jnp.int32),
        pltpu.VMEM((2, own, d_model), BF16),
        pltpu.VMEM((own, d_model), F32),
        pltpu.VMEM((own, 128), F32),
        pltpu.VMEM((2, win, d_model), BF16),
        pltpu.VMEM((d_model, 2 * win), BF16),
        pltpu.VMEM((2, nxh, nz, 2, wr, wide), BF16),
        pltpu.VMEM((8, edge), jnp.int32),
        pltpu.VMEM((8, edge), jnp.int32),
        pltpu.VMEM((8, edge), jnp.int32),
        pltpu.VMEM((2, keys, 2 * HD), BF16),
        pltpu.VMEM((2, 2 * HD, keys), BF16),
        pltpu.VMEM((2, 2, win, 2 * HD), BF16),
        pltpu.VMEM((win, 2 * edge), BF16),
        pltpu.VMEM((2, 2, 2 * HD, edge), BF16),
        pltpu.VMEM((2, 2, 2 * HD, edge), BF16),
        pltpu.VMEM((2, edge, 2 * HD), BF16),
        pltpu.VMEM((2, 2, edge, 2 * HD), BF16),
        pltpu.VMEM((2, keys, win), BF16),
        pltpu.VMEM((2, keys, win), BF16),
        pltpu.VMEM((win, wide), BF16),
        pltpu.VMEM((2 * win, wide), BF16),
        pltpu.VMEM((nyh, blk, d_model), F32),
        pltpu.VMEM((2, 2, nyh, blk, d_model // 2), BF16),
        pltpu.VMEM((2, 2, nyh, blk, d_model // 2), BF16),
        pltpu.VMEM((2, own, d_model), BF16),
        pltpu.VMEM((own, d_model), BF16),
        pltpu.VMEM((2, 2, own, d_model // 2), BF16),
        pltpu.VMEM((2, nxh, nz, 2, wr, wide), F32),
        pltpu.VMEM((2, nxh, nz, 2, wr, wide), BF16),
        pltpu.VMEM((2, nxh, nz, wr, wide), BF16),
        pltpu.VMEM((2, nxh, nz, wr, wide), BF16),
        pltpu.VMEM((nxx, nz, wr, wide), BF16),
        pltpu.VMEM((nz, wr, wide), BF16),
        pltpu.VMEM((nz, wr, wide), BF16),
        dma((9,)),
        dma((2,)), dma((2, 2)), dma((nyh, 2, 2)), dma((nyh, 2)),
        dma((nz,)), dma((nz,)), dma((nxx,)), dma((nxx,)), dma, dma,
        dma((3,)), dma((2,)), dma((2,)), dma((2,)), dma((2, 2)), dma((2, 2)),
        dma, dma, dma((nxx,)), dma((nxx,)), dma((nz,)), dma((nz,)),
        dma((2, 2, nyh)), dma((2, 2, nyh)), dma((2, 2, 2)), dma((2, 2)), dma((2,)), dma,
    ]
    grad_tokens, grad_qkv, grad_out = pl.pallas_call(
        functools.partial(kernel, ny, nxh, nz, win, edge),
        out_shape=(
            jax.ShapeDtypeStruct((own, d_model), BF16),
            jax.ShapeDtypeStruct((wr, 3 * HD), F32),
            jax.ShapeDtypeStruct((wr, HD), F32),
        ),
        in_specs=[anywhere] * 9,
        out_specs=(vmem, vmem, vmem),
        scratch_shapes=scratch,
        compiler_params=pltpu.CompilerParams(collective_id=0, has_side_effects=True),
    )(
        tokens, cotangent, w_qkv, w_out.T,
        mod_scale[None, :], mod_shift[None, :], mod_gate[None, :], counts, edge_index,
    )
    return (grad_tokens, grad_qkv, grad_out.T)


def solution(mesh, nxh=2):
    placed = (
        P(("slab", "enc"), None),
        P(("slab", "enc"), None),
        P("slab", "enc"),
        P("enc", "slab"),
        P(),
        P(),
        P(),
        P("slab"),
        P("slab", None),
    )
    return jax.shard_map(
        functools.partial(on_device, nxh),
        mesh=mesh,
        in_specs=placed,
        out_specs=(P(("slab", "enc"), None), P("slab", "enc"), P("enc", "slab")),
        check_vma=False,
    )
```

```python
import functools

import jax
import jax.numpy as jnp
from jax import lax
from jax.experimental import pallas as pl
from jax.experimental.pallas import tpu as pltpu
from jax.sharding import PartitionSpec as P

HD = 64
EPS = 1e-06
NEG = -1000000000.0
MESH = pl.DeviceIdType.MESH
F32 = jnp.float32
BF16 = jnp.bfloat16


def dot(a, b, dims=((1,), (0,))):
    return lax.dot_general(a, b, (dims, ((), ())), preferred_element_type=F32)


def kernel(
    ny, nxh, nz, win, edge,
    tok_in, cot_in, wq_in, wo_in, scale_in, shift_in, gate_in, counts_in, edges_in,
    out_tok, out_qkv, out_o,
    tok, cot, wq, wo, scale, shift, gate, counts, edges,
    nrm, nx, inv, act, xt, wbuf, meta_nat, meta_own, meta_next,
    kv, kvt, qa, oh, e_send, e_recv, g_send, g_recv, wts, gsc, part_e, part_g, stat, gkvb, qab,
    pvf, csd, crv, osd, oself, orv, dwf, dwb, r1, s2, r2, tot, s3, r3,
    ins, f1s, f1r, f2s, f2r, wzs, wzr, wxs, wxr, wcs, wcr,
    ms, mr, es, er, gs, gr, dcs, dcr, dxs, dxr, dzs, dzr, ccs, ccr, ows, owr, oss, osr,
):
    ns = nxh * nz * 2
    nyh = ny // 2
    nxx = 2 * nxh
    own = tok.shape[0]
    blk = 2 * own
    d_model = tok.shape[1]
    wr = wq.shape[0]
    halfcol = d_model // 2

    enc = lax.axis_index("enc")
    slab = lax.axis_index("slab")
    y, xl = enc // 2, enc % 2
    xh, z, c = slab // (2 * nz), (slab // 2) % nz, slab % 2
    x = xh * 2 + xl
    mine = xh * 2 * nz + z * 2 + xl
    after = (mine + 1) % ns
    before = (mine + ns - 1) % ns
    half = y // nyh

    def at(y_, xl_, xh_, z_, c_):
        return {"enc": y_ * 2 + xl_, "slab": xh_ * (2 * nz) + z_ * 2 + c_}

    def at_slab(s_, c_):
        return {"enc": y * 2 + s_ % 2, "slab": (s_ // 2) * 2 + c_}

    sibling = at(y, xl, xh, z, 1 - c)
    up = at((y + 1) % ny, xl, xh, z, c)
    down = at((y + ny - 1) % ny, xl, xh, z, c)

    def z_peer(j):
        return at(y, xl, xh, (z + j) % nz, c)

    def x_peer(j):
        xx = (x + j) % nxx
        return at(y, xx % 2, xx // 2, z, c)

    def copy(src, dst, send, recv, to):
        return pltpu.make_async_remote_copy(
            src_ref=src, dst_ref=dst, send_sem=send, recv_sem=recv, device_id=to, device_id_type=MESH
        )

    at_home = jnp.logical_and(c == xl, half == c)
    away = jnp.logical_not(at_home)
    diag = c == xl

    pending = []

    def launch(make, when=None):
        if when is None:
            make().start()
            pending.append((make, None))
        else:

            @pl.when(when)
            def _():
                make().start()

            pending.append((make, when))

    def drain():
        for make, when in pending:
            if when is None:
                make().wait_send()
            else:

                @pl.when(when)
                def _():
                    make().wait_send()

    barrier = pltpu.get_barrier_semaphore()

    def greet(to):
        pl.semaphore_signal(barrier, inc=1, device_id=to, device_id_type=MESH)

    greet(sibling)
    greet(up)
    greet(down)
    for j in range(1, nz):
        greet(z_peer(j))
    for j in range(1, nxx):
        greet(x_peer(j))
    for k in range(2):
        greet(at_slab(after, k))
        greet(at_slab(before, k))

    @pl.when(half == c)
    def _():
        greet(at(y, 1 - xl, xh, z, xl))

    @pl.when(jnp.logical_and(half == c, xl != c))
    def _():
        greet(at(y, xl, xh, z, xl))

    above, below = (y + 1) % ny, (y + ny - 1) % ny
    greet(at(above, c, xh, z, half))
    greet(at(below, c, xh, z, half))

    @pl.when(away)
    def _():
        greet(at(y, c, xh, z, half))

    def count_of(flag):
        return flag.astype(jnp.int32)

    greeted = (
        3 + (nz - 1) + (nxx - 1) + 4 + 1
        - 2 * count_of(at_home)
        + 2 * count_of(half == c)
        + 2 * count_of(above // nyh == c)
        + 2 * count_of(below // nyh == c)
    )

    arrivals = [
        pltpu.make_async_copy(src, dst, ins.at[n])
        for n, (src, dst) in enumerate(
            (
                (tok_in, tok), (cot_in, cot), (wq_in, wq), (wo_in, wo), (scale_in, scale),
                (shift_in, shift), (gate_in, gate), (counts_in, counts), (edges_in, edges),
            )
        )
    ]
    for arrival in arrivals:
        arrival.start()
    for arrival in arrivals:
        arrival.wait()

    widened = tok[...].astype(F32)
    average = jnp.mean(widened, 1, keepdims=True)
    centred = widened - average
    variance = jnp.mean(centred * centred, 1, keepdims=True)
    inv_std = lax.rsqrt(variance + EPS)
    normal = centred * inv_std
    gain = 1.0 + scale[...]
    nx[...] = normal
    inv[...] = jnp.broadcast_to(inv_std, inv.shape)
    nrm[0] = (normal * gain + shift[...]).astype(BF16)
    nrm[1] = (cot[...].astype(F32) * gate[...]).astype(BF16)

    hd = HD
    wq_here = wq[...]
    wbuf[xl, xh, z, c] = jnp.concatenate([wq_here[:, hd : 3 * hd], wq_here[:, :hd], wo[...]], 1)

    meta_nat[...] = jnp.zeros(meta_nat.shape, jnp.int32)
    meta_nat[0:2, :] = edges[...]
    meta_nat[2:3, :] = jnp.full((1, edge), counts[0], jnp.int32)
    meta_nat[3:4, :] = jnp.full((1, edge), counts[1], jnp.int32)

    @pl.when(diag)
    def _():
        meta_own[...] = meta_nat[...]

    r_own = (y % nyh) * blk + xl * own
    home = at(y, c, xh, z, half)

    @pl.when(at_home)
    def _():
        for p in range(2):
            act[p, pl.ds(pl.multiple_of(r_own, own), own), :] = nrm[p]

    pl.semaphore_wait(barrier, greeted)

    def f1(p):
        return copy(
            nrm.at[p],
            act.at[p, pl.ds(pl.multiple_of(r_own, own), own)],
            f1s.at[p],
            f1r.at[xl, p],
            home,
        )

    for p in range(2):
        launch(functools.partial(f1, p), away)

    def wz(j):
        return copy(wbuf.at[xl, xh, z, c], wbuf.at[xl, xh, z, c], wzs.at[j], wzr.at[j], z_peer(j))

    def wz_in(j):
        block = wbuf.at[xl, xh, (z + nz - j) % nz, c]
        return copy(block, block, wzs.at[j], wzr.at[j], z_peer(j))

    for j in range(1, nz):
        launch(functools.partial(wz, j))

    def meta_out(n):
        if n == 0:
            return copy(meta_nat, meta_own, ms.at[0], mr.at[0], sibling)
        return copy(meta_nat, meta_next, ms.at[n], mr.at[1], at_slab(before, n - 1))

    for n in range(3):
        launch(functools.partial(meta_out, n), diag)

    def f1_in(h, p):
        rows = pl.ds(pl.multiple_of((y % nyh) * blk + h * own, own), own)
        return copy(nrm.at[p], act.at[p, rows], f1s.at[p], f1r.at[h, p], sibling)

    def ring(i, p, way):
        rows = pl.ds(pl.multiple_of(i * blk, blk), blk)
        return copy(
            act.at[p, rows], act.at[p, rows], f2s.at[i, p, way], f2r.at[i, p], up if way == 0 else down
        )

    here = y % nyh
    for i in range(nyh):
        apart = (y + ny - i - nyh * c) % ny
        back = (ny - apart) % ny
        pending.append((functools.partial(ring, i, 0, 0), apart < nyh))
        pending.append((functools.partial(ring, i, 1, 0), apart < nyh - 1))
        pending.append((functools.partial(ring, i, 1, 1), back < nyh))
        pending.append((functools.partial(ring, i, 0, 1), back < nyh - 1))

    for p in range(2):
        for h in range(2):

            @pl.when(jnp.logical_and(half == c, jnp.logical_or(away, h != xl)))
            def _():
                f1_in(h, p).wait_recv()

        @pl.when(half == c)
        def _():
            ring(here, p, p).start()

    if nyh > 1:

        @pl.when(half == c)
        def _():
            ring(here, 1, 0).start()
            ring(here, 0, 1).start()

    def turn(i):
        rows = pl.ds(pl.multiple_of(i * blk, blk), blk)
        for p in range(2):
            cols = pl.ds(pl.multiple_of(p * win + i * blk, blk), blk)
            xt[:, cols] = act[p, rows, :].T

    def project(i):
        rows = pl.ds(pl.multiple_of(i * blk, blk), blk)
        lane = lax.broadcasted_iota(jnp.int32, (blk, 2 * HD), 1)
        row = lax.broadcasted_iota(jnp.int32, (blk, 2 * HD), 0) + i * blk
        live = row < jnp.where(c == 0, meta_own[2:3, :], meta_own[3:4, :])
        for h in range(2):
            w = wbuf[h].reshape(d_model, 4 * HD)
            from_normed = dot(act[0, rows, :], w)
            from_upstream = dot(act[1, rows, :], w[:, 2 * HD :])
            kv[h, rows, :] = from_normed[:, : 2 * HD].astype(BF16)
            query = from_normed[:, 2 * HD :].astype(BF16).astype(F32) * (HD**-0.5)
            qa[h, 0, rows, :] = jnp.where(lane < HD, query, 0.0).astype(BF16)
            qa[h, 1, rows, :] = jnp.where(
                jnp.logical_and(lane >= HD, live), from_upstream, 0.0
            ).astype(BF16)

    @pl.when(half == c)
    def _():
        turn(here)

    def wx(j):
        block = wbuf.at[xl, xh, :, c]
        return copy(block, block, wxs.at[j], wxr.at[j], x_peer(j))

    def wx_in(j):
        xx = (x + nxx - j) % nxx
        block = wbuf.at[xx % 2, xx // 2, :, c]
        return copy(block, block, wxs.at[j], wxr.at[j], x_peer(j))

    def wc(k):
        block = wbuf.at[:, :, :, k]
        return copy(block, block, wcs, wcr, sibling)

    def weights_x():
        for j in range(1, nz):
            wz_in(j).wait_recv()
        for j in range(1, nxx):
            launch(functools.partial(wx, j))

    def weights_core():
        for j in range(1, nxx):
            wx_in(j).wait_recv()
        launch(functools.partial(wc, c))

    def weights_done():
        wc(1 - c).wait_recv()

        @pl.when(jnp.logical_not(diag))
        def _():
            meta_out(0).wait_recv()

        meta_out(1).wait_recv()

    def far(i):
        return (y + ny - i - nyh * c) % ny == nyh

    stages = [weights_x, weights_core, weights_done]
    for t in range(1, nyh + 1):
        if t == nyh:
            for stage in stages:
                stage()
            stages = []

            @pl.loop(0, nyh)
            def _(i):
                @pl.when(jnp.logical_not(far(i)))
                def _():
                    project(i)

        elif stages:
            stages.pop(0)()
        from_below = (y + 2 * ny - t - nyh * c) % ny
        from_above = (y + 2 * ny + t - nyh * c) % ny
        has_below = from_below < nyh
        has_above = from_above < nyh

        @pl.when(has_below)
        def _():
            ring(from_below, 0, 0).wait_recv()
            if t < nyh:
                ring(from_below, 0, 0).start()

        @pl.when(has_above)
        def _():
            ring(from_above, 1, 1).wait_recv()
            if t < nyh:
                ring(from_above, 1, 1).start()

        if t < nyh:

            @pl.when(has_below)
            def _():
                ring(from_below, 1, 0).wait_recv()
                if t < nyh - 1:
                    ring(from_below, 1, 0).start()

            @pl.when(has_above)
            def _():
                ring(from_above, 0, 1).wait_recv()
                if t < nyh - 1:
                    ring(from_above, 0, 1).start()

            @pl.when(has_above)
            def _():
                turn(from_above)

        @pl.when(has_below)
        def _():
            turn(from_below)
            if t == nyh:
                project(from_below)

    row_id = lax.broadcasted_iota(jnp.int32, (win, edge), 0) + c * win
    for k in range(2):
        oh[:, k * edge : (k + 1) * edge] = (row_id == meta_next[k : k + 1, :]).astype(F32).astype(BF16)
    for h in range(2):
        kvt[h, :, :win] = kv[h, :win, :].T
    for h in range(2):
        picked = dot(kvt[h, :, :win], oh[...]).astype(BF16)
        for k in range(2):
            e_send[k, h] = picked[:, k * edge : (k + 1) * edge]

    def edge_out(k):
        return copy(e_send.at[k], e_recv.at[c], es.at[k], er.at[c], at_slab(after, k))

    def edge_in(k):
        return copy(e_send.at[k], e_recv.at[k], es.at[k], er.at[k], sibling)

    for k in range(2):
        launch(functools.partial(edge_out, k))
    keys = win + edge
    step = 256 if win % 256 == 0 else win
    has_edge = mine > 0
    count = jnp.where(c == 0, meta_own[2:3, :], meta_own[3:4, :])
    limit = jnp.concatenate([count] * (step // edge), 1)

    for h in range(2):

        @pl.loop(0, win // step)
        def _(n):
            q_rows = pl.ds(pl.multiple_of(n * step, step), step)
            key_live = lax.broadcasted_iota(jnp.int32, (win, step), 0) < limit
            scores = dot(kv[h, :win, :], qa[h, 0, q_rows, :], ((1,), (1,)))
            scores = jnp.where(key_live, scores, NEG)
            largest = jnp.max(scores, 0, keepdims=True)
            exponent = jnp.exp(scores - largest)
            g_prob = dot(kv[h, :win, :], qa[h, 1, q_rows, :], ((1,), (1,)))
            part_e[h, :, q_rows] = exponent
            part_g[h, :, q_rows] = g_prob
            stat[h, 0:1, q_rows] = largest
            stat[h, 1:2, q_rows] = jnp.sum(exponent, 0, keepdims=True)
            stat[h, 2:3, q_rows] = jnp.sum(exponent * g_prob, 0, keepdims=True)

    for k in range(2):
        edge_in(k).wait_recv()
    for h in range(2):
        arrived = e_recv[0, h].astype(F32) + e_recv[1, h].astype(F32)
        kvt[h, :, win:] = arrived.astype(BF16)
        kv[h, win:, :] = arrived.T.astype(BF16)

    def scores_of(h):
        @pl.loop(0, win // step)
        def _(n):
            q_rows = pl.ds(pl.multiple_of(n * step, step), step)
            scores = dot(kv[h, win:, :], qa[h, 0, q_rows, :], ((1,), (1,)))
            scores = jnp.where(has_edge, scores, NEG)
            own_largest = stat[h, 0:1, q_rows]
            largest = jnp.maximum(own_largest, jnp.max(scores, 0, keepdims=True))
            exponent = jnp.exp(scores - largest)
            g_prob = dot(kv[h, win:, :], qa[h, 1, q_rows, :], ((1,), (1,)))
            shrink = jnp.exp(own_largest - largest)
            norm = 1.0 / (shrink * stat[h, 1:2, q_rows] + jnp.sum(exponent, 0, keepdims=True))
            centre = norm * (
                shrink * stat[h, 2:3, q_rows] + jnp.sum(exponent * g_prob, 0, keepdims=True)
            )
            probs = exponent * norm
            wts[h, win:, q_rows] = probs.astype(BF16)
            gsc[h, win:, q_rows] = (probs * (g_prob - centre)).astype(BF16)
            own_probs = part_e[h, :, q_rows] * (shrink * norm)
            wts[h, :win, q_rows] = own_probs.astype(BF16)
            gsc[h, :win, q_rows] = (own_probs * (part_g[h, :, q_rows] - centre)).astype(BF16)

        g_send[h] = (dot(gsc[h, win:, :], qa[h, 0]) + dot(wts[h, win:, :], qa[h, 1])).astype(BF16)

    def grad_out(h, k):
        return copy(g_send.at[h], g_recv.at[h, c], gs.at[h, k], gr.at[h, c], at_slab(before, k))

    def grad_in(h, k):
        return copy(g_send.at[h], g_recv.at[h, k], gs.at[h, k], gr.at[h, k], sibling)

    for h in range(2):
        scores_of(h)
        for k in range(2):
            launch(functools.partial(grad_out, h, k))

    row_limit = jnp.concatenate([count] * (win // edge), 1)
    lane = lax.broadcasted_iota(jnp.int32, (HD, win), 1)
    side = lax.broadcasted_iota(jnp.int32, (win, 2 * HD), 1)
    for h in range(2):
        cols = pl.ds(h * 2 * HD, 2 * HD)
        attended = jnp.where(lane < row_limit, dot(kvt[h, HD:, :], wts[h]), 0.0)
        g_query = dot(kvt[h, :HD, :], gsc[h]) * (HD**-0.5)
        pair = jnp.concatenate([g_query, attended], 0).T
        qab[:win, cols] = jnp.where(side < HD, pair, 0.0).astype(BF16)
        qab[win:, cols] = jnp.where(side >= HD, pair, 0.0).astype(BF16)

    def dc(q, k):
        return copy(dwb.at[q, :, :, :, k], r1.at[q], dcs.at[q], dcr.at[q], sibling)

    def dx(q, j):
        xx = (x + j) % nxx
        return copy(
            s2.at[q, xx % 2, xx // 2], r2.at[q, j], dxs.at[q, j], dxr.at[q, j], x_peer(j)
        )

    def dz(j):
        return copy(s3.at[(z + j) % nz], r3.at[j], dzs.at[j], dzr.at[j], z_peer(j))

    def weights_start(q, grad_w):
        blocks = grad_w.reshape(nxh, nz, 2, wr, 4 * HD)
        for h in range(2):
            block = blocks[:, :, :, :, h * 2 * HD : (h + 1) * 2 * HD]
            dwf[q, h] = block
            dwb[q, h] = block.astype(BF16)
        launch(functools.partial(dc, q, 1 - c))

    def weights_cross(q):
        dc(q, 1 - c).wait_recv()
        for h in range(2):
            s2[q, h] = (dwf[q, h, :, :, c] + r1[q, h].astype(F32)).astype(BF16)
        for j in range(1, nxx):
            launch(functools.partial(dx, q, j))

    def weights_spread():
        for q in (1, 0):
            total = dwf[q, xl, xh, :, c] + r1[q, xl, xh].astype(F32)
            for j in range(1, nxx):
                dx(q, j).wait_recv()
                total += r2[q, j].astype(F32)
            tot[:, q] = total
            s3[:, q] = total.astype(BF16)
        for j in range(1, nz):
            launch(functools.partial(dz, j))

    weights_start(1, dot(xt[...], qab[...]))

    for h in range(2):
        cols = pl.ds(h * 2 * HD, 2 * HD)
        own_pair = dot(gsc[h, :win, :], qa[h, 0]) + dot(wts[h, :win, :], qa[h, 1])
        for k in range(2):
            grad_in(h, k).wait_recv()
        returned = dot(oh[...], g_recv[h].reshape(2 * edge, 2 * HD))
        gkvb[:, cols] = (own_pair + returned).astype(BF16)

    weights_cross(1)

    def hops(way, part):
        return nyh if way == part else nyh - 1

    def chain_link(way, part, i, h):
        return copy(
            csd.at[way, part, i, h], crv.at[way, part, i, h],
            ccs.at[way, part, i, h], ccr.at[way, part, i, h], up if way == 0 else down,
        )

    def chain_end(way, part, i, h, yy):
        return copy(
            csd.at[way, part, i, h], orv.at[way, part],
            ows.at[way, part, h], owr.at[way, part], at(yy, h, xh, z, xl),
        )

    def own_out(h):
        return copy(osd.at[h], oself, oss.at[h], osr, at(y, h, xh, z, xl))

    def chain_part(way, part, r):
        yy = (y + (r if way == 0 else ny - r)) % ny
        i = (yy + ny - nyh * c) % ny
        held = i < nyh
        for h in range(2):

            @pl.when(held)
            def _():
                total = pvf[i, h * own : (h + 1) * own, part * halfcol : (part + 1) * halfcol]
                if r < hops(way, part):
                    chain_link(way, part, i, h).wait_recv()
                    total += crv[way, part, i, h].astype(F32)
                csd[way, part, i, h] = total.astype(BF16)

            if r > 1:
                launch(functools.partial(chain_link, way, part, i, h), held)
            else:
                launch(functools.partial(chain_end, way, part, i, h, yy), held)

    def chain(r):
        for way in range(2):
            chain_part(way, way, r)
        if r > 1:
            for way in range(2):
                chain_part(way, 1 - way, r - 1)

    for b in range(nyh):
        rows = pl.ds(b * blk, blk)
        total = jnp.zeros((blk, d_model), F32)
        for h in range(2):
            cols = pl.ds(h * 2 * HD, 2 * HD)
            both = jnp.concatenate([gkvb[rows, cols], qab[rows, cols]], 1)
            total += dot(both, wbuf[h].reshape(d_model, 4 * HD), ((1,), (1,)))
        pvf[b] = total

    chain(nyh)

    @pl.when(half == c)
    def _():
        for h in range(2):
            osd[h] = pvf[here, h * own : (h + 1) * own, :].astype(BF16)

    for h in range(2):
        launch(
            functools.partial(own_out, h),
            jnp.logical_and(half == c, jnp.logical_or(xl != c, h != xl)),
        )

    @pl.when(at_home)
    def _():
        oself[...] = osd[xl]

    weights_start(0, dot(xt[:, :win], gkvb[...]))
    for r in range(nyh - 1, 0, -1):
        if r == 1:
            weights_spread()
        chain(r)
        if r == nyh - 1:
            weights_cross(0)

    def owner_in(way, part):
        return copy(
            csd.at[way, part, 0, 0], orv.at[way, part],
            ows.at[way, part, 0], owr.at[way, part], sibling,
        )

    for way in range(2):
        for part in range(2):
            owner_in(way, part).wait_recv()

    @pl.when(away)
    def _():
        own_out_arrived = copy(osd.at[0], oself, oss.at[0], osr, sibling)
        own_out_arrived.wait_recv()

    mine_sum = oself[...].astype(F32) + jnp.concatenate(
        [orv[0, part].astype(F32) + orv[1, part].astype(F32) for part in range(2)], 1
    )
    g_hat = mine_sum * gain
    normal_own = nx[...]
    g_tok = cot[...].astype(F32) + inv[:, 0:1] * (
        g_hat
        - jnp.mean(g_hat, 1, keepdims=True)
        - normal_own * jnp.mean(g_hat * normal_own, 1, keepdims=True)
    )
    out_tok[...] = g_tok.astype(BF16)

    final = tot[z]
    for j in range(1, nz):
        dz(j).wait_recv()
        final += r3[j].astype(F32)
    out_qkv[...] = jnp.concatenate([final[1, :, :HD], final[0]], 1)
    out_o[...] = final[1, :, HD:]

    drain()


def on_device(nxh, tokens, cotangent, w_qkv, w_out, mod_scale, mod_shift, mod_gate, counts, edge_index):
    ny = lax.axis_size("enc") // 2
    nz = lax.axis_size("slab") // (2 * nxh)
    own, d_model = tokens.shape
    edge = edge_index.shape[1]
    win = own * ny
    wr = w_qkv.shape[0]
    nyh, nxx = ny // 2, 2 * nxh
    wide = 4 * HD
    dma = pltpu.SemaphoreType.DMA
    vmem = pl.BlockSpec(memory_space=pltpu.VMEM)
    anywhere = pl.BlockSpec(memory_space=pl.ANY)
    keys = win + edge
    blk = 2 * own
    scratch = [
        pltpu.VMEM((own, d_model), BF16),
        pltpu.VMEM((own, d_model), BF16),
        pltpu.VMEM((wr, 3 * HD), BF16),
        pltpu.VMEM((wr, HD), BF16),
        pltpu.VMEM((1, d_model), F32),
        pltpu.VMEM((1, d_model), F32),
        pltpu.VMEM((1, d_model), F32),
        pltpu.SMEM((2,), jnp.int32),
        pltpu.VMEM((2, edge), jnp.int32),
        pltpu.VMEM((2, own, d_model), BF16),
        pltpu.VMEM((own, d_model), F32),
        pltpu.VMEM((own, 128), F32),
        pltpu.VMEM((2, win, d_model), BF16),
        pltpu.VMEM((d_model, 2 * win), BF16),
        pltpu.VMEM((2, nxh, nz, 2, wr, wide), BF16),
        pltpu.VMEM((8, edge), jnp.int32),
        pltpu.VMEM((8, edge), jnp.int32),
        pltpu.VMEM((8, edge), jnp.int32),
        pltpu.VMEM((2, keys, 2 * HD), BF16),
        pltpu.VMEM((2, 2 * HD, keys), BF16),
        pltpu.VMEM((2, 2, win, 2 * HD), BF16),
        pltpu.VMEM((win, 2 * edge), BF16),
        pltpu.VMEM((2, 2, 2 * HD, edge), BF16),
        pltpu.VMEM((2, 2, 2 * HD, edge), BF16),
        pltpu.VMEM((2, edge, 2 * HD), BF16),
        pltpu.VMEM((2, 2, edge, 2 * HD), BF16),
        pltpu.VMEM((2, keys, win), BF16),
        pltpu.VMEM((2, keys, win), BF16),
        pltpu.VMEM((2, win, win), F32),
        pltpu.VMEM((2, win, win), F32),
        pltpu.VMEM((2, 8, win), F32),
        pltpu.VMEM((win, wide), BF16),
        pltpu.VMEM((2 * win, wide), BF16),
        pltpu.VMEM((nyh, blk, d_model), F32),
        pltpu.VMEM((2, 2, nyh, 2, own, d_model // 2), BF16),
        pltpu.VMEM((2, 2, nyh, 2, own, d_model // 2), BF16),
        pltpu.VMEM((2, own, d_model), BF16),
        pltpu.VMEM((own, d_model), BF16),
        pltpu.VMEM((2, 2, own, d_model // 2), BF16),
        pltpu.VMEM((2, 2, nxh, nz, 2, wr, 2 * HD), F32),
        pltpu.VMEM((2, 2, nxh, nz, 2, wr, 2 * HD), BF16),
        pltpu.VMEM((2, 2, nxh, nz, wr, 2 * HD), BF16),
        pltpu.VMEM((2, 2, nxh, nz, wr, 2 * HD), BF16),
        pltpu.VMEM((2, nxx, nz, wr, 2 * HD), BF16),
        pltpu.VMEM((nz, 2, wr, 2 * HD), F32),
        pltpu.VMEM((nz, 2, wr, 2 * HD), BF16),
        pltpu.VMEM((nz, 2, wr, 2 * HD), BF16),
        dma((9,)),
        dma((2,)), dma((2, 2)), dma((nyh, 2, 2)), dma((nyh, 2)),
        dma((nz,)), dma((nz,)), dma((nxx,)), dma((nxx,)), dma, dma,
        dma((3,)), dma((2,)), dma((2,)), dma((2,)), dma((2, 2)), dma((2, 2)),
        dma((2,)), dma((2,)), dma((2, nxx)), dma((2, nxx)), dma((nz,)), dma((nz,)),
        dma((2, 2, nyh, 2)), dma((2, 2, nyh, 2)), dma((2, 2, 2)), dma((2, 2)), dma((2,)), dma,
    ]
    grad_tokens, grad_qkv, grad_out = pl.pallas_call(
        functools.partial(kernel, ny, nxh, nz, win, edge),
        out_shape=(
            jax.ShapeDtypeStruct((own, d_model), BF16),
            jax.ShapeDtypeStruct((wr, 3 * HD), F32),
            jax.ShapeDtypeStruct((wr, HD), F32),
        ),
        in_specs=[anywhere] * 9,
        out_specs=(vmem, vmem, vmem),
        scratch_shapes=scratch,
        compiler_params=pltpu.CompilerParams(collective_id=0, has_side_effects=True),
    )(
        tokens, cotangent, w_qkv, w_out.T,
        mod_scale[None, :], mod_shift[None, :], mod_gate[None, :], counts, edge_index,
    )
    return (grad_tokens, grad_qkv, grad_out.T)


def solution(mesh, nxh=2):
    placed = (
        P(("slab", "enc"), None),
        P(("slab", "enc"), None),
        P("slab", "enc"),
        P("enc", "slab"),
        P(),
        P(),
        P(),
        P("slab"),
        P("slab", None),
    )
    return jax.shard_map(
        functools.partial(on_device, nxh),
        mesh=mesh,
        in_specs=placed,
        out_specs=(P(("slab", "enc"), None), P("slab", "enc"), P("enc", "slab")),
        check_vma=False,
    )
```

```python
import functools

import jax
import jax.numpy as jnp
from jax import lax
from jax.experimental import pallas as pl
from jax.experimental.pallas import tpu as pltpu
from jax.sharding import PartitionSpec as P

HD = 64
EPS = 1e-06
NEG = -1000000000.0
MESH = pl.DeviceIdType.MESH
F32 = jnp.float32
BF16 = jnp.bfloat16


def dot(a, b, dims=((1,), (0,))):
    return lax.dot_general(a, b, (dims, ((), ())), preferred_element_type=F32)


def kernel(
    ny, nxh, nz, win, edge,
    tok_in, cot_in, wq_in, wo_in, scale_in, shift_in, gate_in, counts_in, edges_in,
    out_tok, out_qkv, out_o,
    tok, cot, wq, wo, scale, shift, gate, counts, edges,
    nrm, nx, inv, act, xt, wbuf, meta_nat, meta_own, meta_next,
    kv, kvt, qa, oh, e_send, e_recv, g_send, g_recv, wts, gsc, part_e, part_g, stat, gkvb, qab,
    pvf, csd, crv, osd, oself, orv, dwf, dwb, r1, s2, r2, tot, s3, r3,
    ins, f1s, f1r, f2s, f2r, wzs, wzr, wxs, wxr, wcs, wcr,
    ms, mr, es, er, gs, gr, dcs, dcr, dxs, dxr, dzs, dzr, ccs, ccr, ows, owr, oss, osr,
):
    ns = nxh * nz * 2
    nyh = ny // 2
    nxx = 2 * nxh
    own = tok.shape[0]
    blk = 2 * own
    d_model = tok.shape[1]
    wr = wq.shape[0]
    halfcol = d_model // 2

    enc = lax.axis_index("enc")
    slab = lax.axis_index("slab")
    y, xl = enc // 2, enc % 2
    xh, z, c = slab // (2 * nz), (slab // 2) % nz, slab % 2
    x = xh * 2 + xl
    mine = xh * 2 * nz + z * 2 + xl
    after = (mine + 1) % ns
    before = (mine + ns - 1) % ns
    half = y // nyh

    def at(y_, xl_, xh_, z_, c_):
        return {"enc": y_ * 2 + xl_, "slab": xh_ * (2 * nz) + z_ * 2 + c_}

    def at_slab(s_, c_):
        return {"enc": y * 2 + s_ % 2, "slab": (s_ // 2) * 2 + c_}

    sibling = at(y, xl, xh, z, 1 - c)
    up = at((y + 1) % ny, xl, xh, z, c)
    down = at((y + ny - 1) % ny, xl, xh, z, c)

    def z_peer(j):
        return at(y, xl, xh, (z + j) % nz, c)

    def x_peer(j):
        xx = (x + j) % nxx
        return at(y, xx % 2, xx // 2, z, c)

    def copy(src, dst, send, recv, to):
        return pltpu.make_async_remote_copy(
            src_ref=src, dst_ref=dst, send_sem=send, recv_sem=recv, device_id=to, device_id_type=MESH
        )

    at_home = jnp.logical_and(c == xl, half == c)
    away = jnp.logical_not(at_home)
    diag = c == xl

    pending = []

    def launch(make, when=None):
        if when is None:
            make().start()
            pending.append((make, None))
        else:

            @pl.when(when)
            def _():
                make().start()

            pending.append((make, when))

    def drain():
        for make, when in pending:
            if when is None:
                make().wait_send()
            else:

                @pl.when(when)
                def _():
                    make().wait_send()

    barrier = pltpu.get_barrier_semaphore()

    def greet(to):
        pl.semaphore_signal(barrier, inc=1, device_id=to, device_id_type=MESH)

    greet(sibling)
    greet(up)
    greet(down)
    for j in range(1, nz):
        greet(z_peer(j))
    for j in range(1, nxx):
        greet(x_peer(j))
    for k in range(2):
        greet(at_slab(after, k))
        greet(at_slab(before, k))

    @pl.when(half == c)
    def _():
        greet(at(y, 1 - xl, xh, z, xl))

    @pl.when(jnp.logical_and(half == c, xl != c))
    def _():
        greet(at(y, xl, xh, z, xl))

    above, below = (y + 1) % ny, (y + ny - 1) % ny
    greet(at(above, c, xh, z, half))
    greet(at(below, c, xh, z, half))

    @pl.when(away)
    def _():
        greet(at(y, c, xh, z, half))

    def count_of(flag):
        return flag.astype(jnp.int32)

    greeted = (
        3 + (nz - 1) + (nxx - 1) + 4 + 1
        - 2 * count_of(at_home)
        + 2 * count_of(half == c)
        + 2 * count_of(above // nyh == c)
        + 2 * count_of(below // nyh == c)
    )

    arrivals = [
        pltpu.make_async_copy(src, dst, ins.at[n])
        for n, (src, dst) in enumerate(
            (
                (tok_in, tok), (cot_in, cot), (wq_in, wq), (wo_in, wo), (scale_in, scale),
                (shift_in, shift), (gate_in, gate), (counts_in, counts), (edges_in, edges),
            )
        )
    ]
    for arrival in arrivals:
        arrival.start()
    for arrival in arrivals:
        arrival.wait()

    widened = tok[...].astype(F32)
    average = jnp.mean(widened, 1, keepdims=True)
    centred = widened - average
    variance = jnp.mean(centred * centred, 1, keepdims=True)
    inv_std = lax.rsqrt(variance + EPS)
    normal = centred * inv_std
    gain = 1.0 + scale[...]
    nx[...] = normal
    inv[...] = jnp.broadcast_to(inv_std, inv.shape)
    nrm[0] = (normal * gain + shift[...]).astype(BF16)
    nrm[1] = (cot[...].astype(F32) * gate[...]).astype(BF16)

    hd = HD
    wq_here = wq[...]
    wbuf[xl, xh, z, c] = jnp.concatenate([wq_here[:, hd : 3 * hd], wq_here[:, :hd], wo[...]], 1)

    meta_nat[...] = jnp.zeros(meta_nat.shape, jnp.int32)
    meta_nat[0:2, :] = edges[...]
    meta_nat[2:3, :] = jnp.full((1, edge), counts[0], jnp.int32)
    meta_nat[3:4, :] = jnp.full((1, edge), counts[1], jnp.int32)

    @pl.when(diag)
    def _():
        meta_own[...] = meta_nat[...]

    r_own = (y % nyh) * blk + xl * own
    home = at(y, c, xh, z, half)

    @pl.when(at_home)
    def _():
        for p in range(2):
            act[p, pl.ds(pl.multiple_of(r_own, own), own), :] = nrm[p]

    pl.semaphore_wait(barrier, greeted)

    def f1(p):
        return copy(
            nrm.at[p],
            act.at[p, pl.ds(pl.multiple_of(r_own, own), own)],
            f1s.at[p],
            f1r.at[xl, p],
            home,
        )

    for p in range(2):
        launch(functools.partial(f1, p), away)

    def wz(j):
        return copy(wbuf.at[xl, xh, z, c], wbuf.at[xl, xh, z, c], wzs.at[j], wzr.at[j], z_peer(j))

    def wz_in(j):
        block = wbuf.at[xl, xh, (z + nz - j) % nz, c]
        return copy(block, block, wzs.at[j], wzr.at[j], z_peer(j))

    for j in range(1, nz):
        launch(functools.partial(wz, j))

    def meta_out(n):
        if n == 0:
            return copy(meta_nat, meta_own, ms.at[0], mr.at[0], sibling)
        return copy(meta_nat, meta_next, ms.at[n], mr.at[1], at_slab(before, n - 1))

    for n in range(3):
        launch(functools.partial(meta_out, n), diag)

    def f1_in(h, p):
        rows = pl.ds(pl.multiple_of((y % nyh) * blk + h * own, own), own)
        return copy(nrm.at[p], act.at[p, rows], f1s.at[p], f1r.at[h, p], sibling)

    def ring(i, p, h, way):
        rows = pl.ds(pl.multiple_of(i * blk + h * own, own), own)
        return copy(
            act.at[p, rows], act.at[p, rows], f2s.at[i, p, h, way], f2r.at[i, p, h],
            up if way == 0 else down,
        )

    here = y % nyh
    for i in range(nyh):
        apart = (y + ny - i - nyh * c) % ny
        back = (ny - apart) % ny
        for h in range(2):
            pending.append((functools.partial(ring, i, 0, h, 0), apart < nyh))
            pending.append((functools.partial(ring, i, 1, h, 0), apart < nyh - 1))
            pending.append((functools.partial(ring, i, 1, h, 1), back < nyh))
            pending.append((functools.partial(ring, i, 0, h, 1), back < nyh - 1))

    for h in (xl, 1 - xl):
        for p in range(2):
            if h is xl:

                @pl.when(jnp.logical_and(half == c, away))
                def _():
                    f1_in(h, p).wait_recv()

            else:

                @pl.when(half == c)
                def _():
                    f1_in(h, p).wait_recv()

            @pl.when(half == c)
            def _():
                ring(here, p, h, p).start()
                if nyh > 1:
                    ring(here, p, h, 1 - p).start()

    def turn(i):
        rows = pl.ds(pl.multiple_of(i * blk, blk), blk)
        for p in range(2):
            cols = pl.ds(pl.multiple_of(p * win + i * blk, blk), blk)
            xt[:, cols] = act[p, rows, :].T

    def project(i):
        rows = pl.ds(pl.multiple_of(i * blk, blk), blk)
        lane = lax.broadcasted_iota(jnp.int32, (blk, 2 * HD), 1)
        row = lax.broadcasted_iota(jnp.int32, (blk, 2 * HD), 0) + i * blk
        live = row < jnp.where(c == 0, meta_own[2:3, :], meta_own[3:4, :])
        for h in range(2):
            w = wbuf[h].reshape(d_model, 4 * HD)
            from_normed = dot(act[0, rows, :], w)
            from_upstream = dot(act[1, rows, :], w[:, 2 * HD :])
            kv[h, rows, :] = from_normed[:, : 2 * HD].astype(BF16)
            query = from_normed[:, 2 * HD :].astype(BF16).astype(F32) * (HD**-0.5)
            qa[h, 0, rows, :] = jnp.where(lane < HD, query, 0.0).astype(BF16)
            qa[h, 1, rows, :] = jnp.where(
                jnp.logical_and(lane >= HD, live), from_upstream, 0.0
            ).astype(BF16)

    @pl.when(half == c)
    def _():
        turn(here)

    def wx(j):
        block = wbuf.at[xl, xh, :, c]
        return copy(block, block, wxs.at[j], wxr.at[j], x_peer(j))

    def wx_in(j):
        xx = (x + nxx - j) % nxx
        block = wbuf.at[xx % 2, xx // 2, :, c]
        return copy(block, block, wxs.at[j], wxr.at[j], x_peer(j))

    def wc(k):
        block = wbuf.at[:, :, :, k]
        return copy(block, block, wcs, wcr, sibling)

    def weights_x():
        for j in range(1, nz):
            wz_in(j).wait_recv()
        for j in range(1, nxx):
            launch(functools.partial(wx, j))

    def weights_core():
        for j in range(1, nxx):
            wx_in(j).wait_recv()
        launch(functools.partial(wc, c))

    def weights_done():
        wc(1 - c).wait_recv()

        @pl.when(jnp.logical_not(diag))
        def _():
            meta_out(0).wait_recv()

        meta_out(1).wait_recv()

    def far(i):
        return (y + ny - i - nyh * c) % ny == nyh

    stages = [weights_x, weights_core, weights_done]
    for t in range(1, nyh + 1):
        if t == nyh:
            for stage in stages:
                stage()
            stages = []

            @pl.loop(0, nyh)
            def _(i):
                @pl.when(jnp.logical_not(far(i)))
                def _():
                    project(i)

        elif stages:
            stages.pop(0)()
        from_below = (y + 2 * ny - t - nyh * c) % ny
        from_above = (y + 2 * ny + t - nyh * c) % ny
        has_below = from_below < nyh
        has_above = from_above < nyh

        def relay(i, p, h, way):
            ring(i, p, h, way).wait_recv()
            if t < (nyh if p == way else nyh - 1):
                ring(i, p, h, way).start()

        for h in (xl, 1 - xl):
            for way_first in (True, False):
                if t == nyh and not way_first:
                    continue

                @pl.when(has_below)
                def _():
                    relay(from_below, 0 if way_first else 1, h, 0)

                @pl.when(has_above)
                def _():
                    relay(from_above, 1 if way_first else 0, h, 1)

        if t < nyh:

            @pl.when(has_above)
            def _():
                turn(from_above)

        @pl.when(has_below)
        def _():
            turn(from_below)
            if t == nyh:
                project(from_below)

    row_id = lax.broadcasted_iota(jnp.int32, (win, edge), 0) + c * win
    for k in range(2):
        oh[:, k * edge : (k + 1) * edge] = (row_id == meta_next[k : k + 1, :]).astype(F32).astype(BF16)
    for h in range(2):
        kvt[h, :, :win] = kv[h, :win, :].T
    for h in range(2):
        picked = dot(kvt[h, :, :win], oh[...]).astype(BF16)
        for k in range(2):
            e_send[k, h] = picked[:, k * edge : (k + 1) * edge]

    def edge_out(k):
        return copy(e_send.at[k], e_recv.at[c], es.at[k], er.at[c], at_slab(after, k))

    def edge_in(k):
        return copy(e_send.at[k], e_recv.at[k], es.at[k], er.at[k], sibling)

    for k in range(2):
        launch(functools.partial(edge_out, k))
    keys = win + edge
    step = 256 if win % 256 == 0 else win
    has_edge = mine > 0
    count = jnp.where(c == 0, meta_own[2:3, :], meta_own[3:4, :])
    limit = jnp.concatenate([count] * (step // edge), 1)

    for h in range(2):

        @pl.loop(0, win // step)
        def _(n):
            q_rows = pl.ds(pl.multiple_of(n * step, step), step)
            key_live = lax.broadcasted_iota(jnp.int32, (win, step), 0) < limit
            scores = dot(kv[h, :win, :], qa[h, 0, q_rows, :], ((1,), (1,)))
            scores = jnp.where(key_live, scores, NEG)
            largest = jnp.max(scores, 0, keepdims=True)
            exponent = jnp.exp(scores - largest)
            g_prob = dot(kv[h, :win, :], qa[h, 1, q_rows, :], ((1,), (1,)))
            part_e[h, :, q_rows] = exponent
            part_g[h, :, q_rows] = g_prob
            stat[h, 0:1, q_rows] = largest
            stat[h, 1:2, q_rows] = jnp.sum(exponent, 0, keepdims=True)
            stat[h, 2:3, q_rows] = jnp.sum(exponent * g_prob, 0, keepdims=True)

    for k in range(2):
        edge_in(k).wait_recv()
    for h in range(2):
        arrived = e_recv[0, h].astype(F32) + e_recv[1, h].astype(F32)
        kvt[h, :, win:] = arrived.astype(BF16)
        kv[h, win:, :] = arrived.T.astype(BF16)

    def scores_of(h):
        @pl.loop(0, win // step)
        def _(n):
            q_rows = pl.ds(pl.multiple_of(n * step, step), step)
            scores = dot(kv[h, win:, :], qa[h, 0, q_rows, :], ((1,), (1,)))
            scores = jnp.where(has_edge, scores, NEG)
            own_largest = stat[h, 0:1, q_rows]
            largest = jnp.maximum(own_largest, jnp.max(scores, 0, keepdims=True))
            exponent = jnp.exp(scores - largest)
            g_prob = dot(kv[h, win:, :], qa[h, 1, q_rows, :], ((1,), (1,)))
            shrink = jnp.exp(own_largest - largest)
            norm = 1.0 / (shrink * stat[h, 1:2, q_rows] + jnp.sum(exponent, 0, keepdims=True))
            centre = norm * (
                shrink * stat[h, 2:3, q_rows] + jnp.sum(exponent * g_prob, 0, keepdims=True)
            )
            probs = exponent * norm
            wts[h, win:, q_rows] = probs.astype(BF16)
            gsc[h, win:, q_rows] = (probs * (g_prob - centre)).astype(BF16)
            own_probs = part_e[h, :, q_rows] * (shrink * norm)
            wts[h, :win, q_rows] = own_probs.astype(BF16)
            gsc[h, :win, q_rows] = (own_probs * (part_g[h, :, q_rows] - centre)).astype(BF16)

        g_send[h] = (dot(gsc[h, win:, :], qa[h, 0]) + dot(wts[h, win:, :], qa[h, 1])).astype(BF16)

    def grad_out(h, k):
        return copy(g_send.at[h], g_recv.at[h, c], gs.at[h, k], gr.at[h, c], at_slab(before, k))

    def grad_in(h, k):
        return copy(g_send.at[h], g_recv.at[h, k], gs.at[h, k], gr.at[h, k], sibling)

    for h in range(2):
        scores_of(h)
        for k in range(2):
            launch(functools.partial(grad_out, h, k))

    row_limit = jnp.concatenate([count] * (win // edge), 1)
    lane = lax.broadcasted_iota(jnp.int32, (HD, win), 1)
    side = lax.broadcasted_iota(jnp.int32, (win, 2 * HD), 1)
    for h in range(2):
        cols = pl.ds(h * 2 * HD, 2 * HD)
        attended = jnp.where(lane < row_limit, dot(kvt[h, HD:, :], wts[h]), 0.0)
        g_query = dot(kvt[h, :HD, :], gsc[h]) * (HD**-0.5)
        pair = jnp.concatenate([g_query, attended], 0).T
        qab[:win, cols] = jnp.where(side < HD, pair, 0.0).astype(BF16)
        qab[win:, cols] = jnp.where(side >= HD, pair, 0.0).astype(BF16)

    def dc(q, k):
        return copy(dwb.at[q, :, :, :, k], r1.at[q], dcs.at[q], dcr.at[q], sibling)

    def dx(q, j):
        xx = (x + j) % nxx
        return copy(
            s2.at[q, xx % 2, xx // 2], r2.at[q, j], dxs.at[q, j], dxr.at[q, j], x_peer(j)
        )

    def dz(j):
        return copy(s3.at[(z + j) % nz], r3.at[j], dzs.at[j], dzr.at[j], z_peer(j))

    def weights_start(q, grad_w):
        blocks = grad_w.reshape(nxh, nz, 2, wr, 4 * HD)
        for h in range(2):
            block = blocks[:, :, :, :, h * 2 * HD : (h + 1) * 2 * HD]
            dwf[q, h] = block
            dwb[q, h] = block.astype(BF16)
        launch(functools.partial(dc, q, 1 - c))

    def weights_cross(q):
        dc(q, 1 - c).wait_recv()
        for h in range(2):
            s2[q, h] = (dwf[q, h, :, :, c] + r1[q, h].astype(F32)).astype(BF16)
        for j in range(1, nxx):
            launch(functools.partial(dx, q, j))

    def weights_spread():
        for q in (1, 0):
            total = dwf[q, xl, xh, :, c] + r1[q, xl, xh].astype(F32)
            for j in range(1, nxx):
                dx(q, j).wait_recv()
                total += r2[q, j].astype(F32)
            tot[:, q] = total
            s3[:, q] = total.astype(BF16)
        for j in range(1, nz):
            launch(functools.partial(dz, j))

    weights_start(1, dot(xt[...], qab[...]))

    for h in range(2):
        cols = pl.ds(h * 2 * HD, 2 * HD)
        own_pair = dot(gsc[h, :win, :], qa[h, 0]) + dot(wts[h, :win, :], qa[h, 1])
        for k in range(2):
            grad_in(h, k).wait_recv()
        returned = dot(oh[...], g_recv[h].reshape(2 * edge, 2 * HD))
        gkvb[:, cols] = (own_pair + returned).astype(BF16)

    weights_cross(1)

    def hops(way, part):
        return nyh if way == part else nyh - 1

    def chain_link(way, part, i, h):
        return copy(
            csd.at[way, part, i, h], crv.at[way, part, i, h],
            ccs.at[way, part, i, h], ccr.at[way, part, i, h], up if way == 0 else down,
        )

    def chain_end(way, part, i, h, yy):
        return copy(
            csd.at[way, part, i, h], orv.at[way, part],
            ows.at[way, part, h], owr.at[way, part], at(yy, h, xh, z, xl),
        )

    def own_out(h):
        return copy(osd.at[h], oself, oss.at[h], osr, at(y, h, xh, z, xl))

    def chain_part(way, part, r):
        yy = (y + (r if way == 0 else ny - r)) % ny
        i = (yy + ny - nyh * c) % ny
        held = i < nyh
        for h in range(2):

            @pl.when(held)
            def _():
                total = pvf[i, h * own : (h + 1) * own, part * halfcol : (part + 1) * halfcol]
                if r < hops(way, part):
                    chain_link(way, part, i, h).wait_recv()
                    total += crv[way, part, i, h].astype(F32)
                csd[way, part, i, h] = total.astype(BF16)

            if r > 1:
                launch(functools.partial(chain_link, way, part, i, h), held)
            else:
                launch(functools.partial(chain_end, way, part, i, h, yy), held)

    def chain(r):
        for way in range(2):
            chain_part(way, way, r)
        if r > 1:
            for way in range(2):
                chain_part(way, 1 - way, r - 1)

    for b in range(nyh):
        rows = pl.ds(b * blk, blk)
        total = jnp.zeros((blk, d_model), F32)
        for h in range(2):
            cols = pl.ds(h * 2 * HD, 2 * HD)
            both = jnp.concatenate([gkvb[rows, cols], qab[rows, cols]], 1)
            total += dot(both, wbuf[h].reshape(d_model, 4 * HD), ((1,), (1,)))
        pvf[b] = total

    chain(nyh)

    @pl.when(half == c)
    def _():
        for h in range(2):
            osd[h] = pvf[here, h * own : (h + 1) * own, :].astype(BF16)

    for h in range(2):
        launch(
            functools.partial(own_out, h),
            jnp.logical_and(half == c, jnp.logical_or(xl != c, h != xl)),
        )

    @pl.when(at_home)
    def _():
        oself[...] = osd[xl]

    weights_start(0, dot(xt[:, :win], gkvb[...]))
    for r in range(nyh - 1, 0, -1):
        if r == 1:
            weights_spread()
        chain(r)
        if r == nyh - 1:
            weights_cross(0)

    def owner_in(way, part):
        return copy(
            csd.at[way, part, 0, 0], orv.at[way, part],
            ows.at[way, part, 0], owr.at[way, part], sibling,
        )

    for way in range(2):
        for part in range(2):
            owner_in(way, part).wait_recv()

    @pl.when(away)
    def _():
        own_out_arrived = copy(osd.at[0], oself, oss.at[0], osr, sibling)
        own_out_arrived.wait_recv()

    mine_sum = oself[...].astype(F32) + jnp.concatenate(
        [orv[0, part].astype(F32) + orv[1, part].astype(F32) for part in range(2)], 1
    )
    g_hat = mine_sum * gain
    normal_own = nx[...]
    g_tok = cot[...].astype(F32) + inv[:, 0:1] * (
        g_hat
        - jnp.mean(g_hat, 1, keepdims=True)
        - normal_own * jnp.mean(g_hat * normal_own, 1, keepdims=True)
    )
    out_tok[...] = g_tok.astype(BF16)

    final = tot[z]
    for j in range(1, nz):
        dz(j).wait_recv()
        final += r3[j].astype(F32)
    out_qkv[...] = jnp.concatenate([final[1, :, :HD], final[0]], 1)
    out_o[...] = final[1, :, HD:]

    drain()


def on_device(nxh, tokens, cotangent, w_qkv, w_out, mod_scale, mod_shift, mod_gate, counts, edge_index):
    ny = lax.axis_size("enc") // 2
    nz = lax.axis_size("slab") // (2 * nxh)
    own, d_model = tokens.shape
    edge = edge_index.shape[1]
    win = own * ny
    wr = w_qkv.shape[0]
    nyh, nxx = ny // 2, 2 * nxh
    wide = 4 * HD
    dma = pltpu.SemaphoreType.DMA
    vmem = pl.BlockSpec(memory_space=pltpu.VMEM)
    anywhere = pl.BlockSpec(memory_space=pl.ANY)
    keys = win + edge
    blk = 2 * own
    scratch = [
        pltpu.VMEM((own, d_model), BF16),
        pltpu.VMEM((own, d_model), BF16),
        pltpu.VMEM((wr, 3 * HD), BF16),
        pltpu.VMEM((wr, HD), BF16),
        pltpu.VMEM((1, d_model), F32),
        pltpu.VMEM((1, d_model), F32),
        pltpu.VMEM((1, d_model), F32),
        pltpu.SMEM((2,), jnp.int32),
        pltpu.VMEM((2, edge), jnp.int32),
        pltpu.VMEM((2, own, d_model), BF16),
        pltpu.VMEM((own, d_model), F32),
        pltpu.VMEM((own, 128), F32),
        pltpu.VMEM((2, win, d_model), BF16),
        pltpu.VMEM((d_model, 2 * win), BF16),
        pltpu.VMEM((2, nxh, nz, 2, wr, wide), BF16),
        pltpu.VMEM((8, edge), jnp.int32),
        pltpu.VMEM((8, edge), jnp.int32),
        pltpu.VMEM((8, edge), jnp.int32),
        pltpu.VMEM((2, keys, 2 * HD), BF16),
        pltpu.VMEM((2, 2 * HD, keys), BF16),
        pltpu.VMEM((2, 2, win, 2 * HD), BF16),
        pltpu.VMEM((win, 2 * edge), BF16),
        pltpu.VMEM((2, 2, 2 * HD, edge), BF16),
        pltpu.VMEM((2, 2, 2 * HD, edge), BF16),
        pltpu.VMEM((2, edge, 2 * HD), BF16),
        pltpu.VMEM((2, 2, edge, 2 * HD), BF16),
        pltpu.VMEM((2, keys, win), BF16),
        pltpu.VMEM((2, keys, win), BF16),
        pltpu.VMEM((2, win, win), F32),
        pltpu.VMEM((2, win, win), F32),
        pltpu.VMEM((2, 8, win), F32),
        pltpu.VMEM((win, wide), BF16),
        pltpu.VMEM((2 * win, wide), BF16),
        pltpu.VMEM((nyh, blk, d_model), F32),
        pltpu.VMEM((2, 2, nyh, 2, own, d_model // 2), BF16),
        pltpu.VMEM((2, 2, nyh, 2, own, d_model // 2), BF16),
        pltpu.VMEM((2, own, d_model), BF16),
        pltpu.VMEM((own, d_model), BF16),
        pltpu.VMEM((2, 2, own, d_model // 2), BF16),
        pltpu.VMEM((2, 2, nxh, nz, 2, wr, 2 * HD), F32),
        pltpu.VMEM((2, 2, nxh, nz, 2, wr, 2 * HD), BF16),
        pltpu.VMEM((2, 2, nxh, nz, wr, 2 * HD), BF16),
        pltpu.VMEM((2, 2, nxh, nz, wr, 2 * HD), BF16),
        pltpu.VMEM((2, nxx, nz, wr, 2 * HD), BF16),
        pltpu.VMEM((nz, 2, wr, 2 * HD), F32),
        pltpu.VMEM((nz, 2, wr, 2 * HD), BF16),
        pltpu.VMEM((nz, 2, wr, 2 * HD), BF16),
        dma((9,)),
        dma((2,)), dma((2, 2)), dma((nyh, 2, 2, 2)), dma((nyh, 2, 2)),
        dma((nz,)), dma((nz,)), dma((nxx,)), dma((nxx,)), dma, dma,
        dma((3,)), dma((2,)), dma((2,)), dma((2,)), dma((2, 2)), dma((2, 2)),
        dma((2,)), dma((2,)), dma((2, nxx)), dma((2, nxx)), dma((nz,)), dma((nz,)),
        dma((2, 2, nyh, 2)), dma((2, 2, nyh, 2)), dma((2, 2, 2)), dma((2, 2)), dma((2,)), dma,
    ]
    grad_tokens, grad_qkv, grad_out = pl.pallas_call(
        functools.partial(kernel, ny, nxh, nz, win, edge),
        out_shape=(
            jax.ShapeDtypeStruct((own, d_model), BF16),
            jax.ShapeDtypeStruct((wr, 3 * HD), F32),
            jax.ShapeDtypeStruct((wr, HD), F32),
        ),
        in_specs=[anywhere] * 9,
        out_specs=(vmem, vmem, vmem),
        scratch_shapes=scratch,
        compiler_params=pltpu.CompilerParams(collective_id=0, has_side_effects=True),
    )(
        tokens, cotangent, w_qkv, w_out.T,
        mod_scale[None, :], mod_shift[None, :], mod_gate[None, :], counts, edge_index,
    )
    return (grad_tokens, grad_qkv, grad_out.T)


def solution(mesh, nxh=2):
    placed = (
        P(("slab", "enc"), None),
        P(("slab", "enc"), None),
        P("slab", "enc"),
        P("enc", "slab"),
        P(),
        P(),
        P(),
        P("slab"),
        P("slab", None),
    )
    return jax.shard_map(
        functools.partial(on_device, nxh),
        mesh=mesh,
        in_specs=placed,
        out_specs=(P(("slab", "enc"), None), P("slab", "enc"), P("enc", "slab")),
        check_vma=False,
    )
```

```python
import functools

import jax
import jax.numpy as jnp
from jax import lax
from jax.experimental import pallas as pl
from jax.experimental.pallas import tpu as pltpu
from jax.sharding import PartitionSpec as P

HD = 64
EPS = 1e-06
NEG = -1000000000.0
MESH = pl.DeviceIdType.MESH
F32 = jnp.float32
BF16 = jnp.bfloat16


def dot(a, b, dims=((1,), (0,))):
    return lax.dot_general(a, b, (dims, ((), ())), preferred_element_type=F32)


def kernel(
    ny, nxh, nz, win, edge,
    tok_in, cot_in, wq_in, wo_in, scale_in, shift_in, gate_in, counts_in, edges_in,
    out_tok, out_qkv, out_o,
    tok, cot, wq, wo, scale, shift, gate, counts, edges,
    nrm, nx, inv, act, xt, wbuf, meta_nat, meta_own, meta_next,
    kv, kvt, qa, oh, e_send, e_recv, g_send, g_recv, wts, gsc, part_e, part_g, stat, gkvb, qab,
    pvf, csd, crv, osd, oself, orv, dwf, dwb, r1, s2, r2, tot, s3, r3,
    ins, f1s, f1r, f2s, f2r, wzs, wzr, wxs, wxr, wcs, wcr,
    ms, mr, es, er, gs, gr, dcs, dcr, dxs, dxr, dzs, dzr, ccs, ccr, ows, owr, oss, osr,
):
    ns = nxh * nz * 2
    nyh = ny // 2
    nxx = 2 * nxh
    z_far = sorted(range(1, nz), key=lambda j: -min(j, nz - j))
    x_far = sorted(range(1, nxx), key=lambda j: -min(j, nxx - j))
    own = tok.shape[0]
    blk = 2 * own
    d_model = tok.shape[1]
    wr = wq.shape[0]
    halfcol = d_model // 2

    enc = lax.axis_index("enc")
    slab = lax.axis_index("slab")
    y, xl = enc // 2, enc % 2
    xh, z, c = slab // (2 * nz), (slab // 2) % nz, slab % 2
    x = xh * 2 + xl
    mine = xh * 2 * nz + z * 2 + xl
    after = (mine + 1) % ns
    before = (mine + ns - 1) % ns
    half = y // nyh

    def at(y_, xl_, xh_, z_, c_):
        return {"enc": y_ * 2 + xl_, "slab": xh_ * (2 * nz) + z_ * 2 + c_}

    def at_slab(s_, c_):
        return {"enc": y * 2 + s_ % 2, "slab": (s_ // 2) * 2 + c_}

    sibling = at(y, xl, xh, z, 1 - c)
    up = at((y + 1) % ny, xl, xh, z, c)
    down = at((y + ny - 1) % ny, xl, xh, z, c)

    def z_peer(j):
        return at(y, xl, xh, (z + j) % nz, c)

    def x_peer(j):
        xx = (x + j) % nxx
        return at(y, xx % 2, xx // 2, z, c)

    def copy(src, dst, send, recv, to):
        return pltpu.make_async_remote_copy(
            src_ref=src, dst_ref=dst, send_sem=send, recv_sem=recv, device_id=to, device_id_type=MESH
        )

    at_home = jnp.logical_and(c == xl, half == c)
    away = jnp.logical_not(at_home)
    diag = c == xl

    pending = []

    def launch(make, when=None):
        if when is None:
            make().start()
            pending.append((make, None))
        else:

            @pl.when(when)
            def _():
                make().start()

            pending.append((make, when))

    def drain():
        for make, when in pending:
            if when is None:
                make().wait_send()
            else:

                @pl.when(when)
                def _():
                    make().wait_send()

    barrier = pltpu.get_barrier_semaphore()

    def greet(to):
        pl.semaphore_signal(barrier, inc=1, device_id=to, device_id_type=MESH)

    greet(sibling)
    greet(up)
    greet(down)
    for j in range(1, nz):
        greet(z_peer(j))
    for j in range(1, nxx):
        greet(x_peer(j))
    for k in range(2):
        greet(at_slab(after, k))
        greet(at_slab(before, k))

    @pl.when(half == c)
    def _():
        greet(at(y, 1 - xl, xh, z, xl))

    @pl.when(jnp.logical_and(half == c, xl != c))
    def _():
        greet(at(y, xl, xh, z, xl))

    above, below = (y + 1) % ny, (y + ny - 1) % ny
    greet(at(above, c, xh, z, half))
    greet(at(below, c, xh, z, half))

    @pl.when(away)
    def _():
        greet(at(y, c, xh, z, half))

    def count_of(flag):
        return flag.astype(jnp.int32)

    greeted = (
        3 + (nz - 1) + (nxx - 1) + 4 + 1
        - 2 * count_of(at_home)
        + 2 * count_of(half == c)
        + 2 * count_of(above // nyh == c)
        + 2 * count_of(below // nyh == c)
    )

    arrivals = [
        pltpu.make_async_copy(src, dst, ins.at[n])
        for n, (src, dst) in enumerate(
            (
                (tok_in, tok), (cot_in, cot), (wq_in, wq), (wo_in, wo), (scale_in, scale),
                (shift_in, shift), (gate_in, gate), (counts_in, counts), (edges_in, edges),
            )
        )
    ]
    for arrival in arrivals:
        arrival.start()
    for arrival in arrivals:
        arrival.wait()

    widened = tok[...].astype(F32)
    average = jnp.mean(widened, 1, keepdims=True)
    centred = widened - average
    variance = jnp.mean(centred * centred, 1, keepdims=True)
    inv_std = lax.rsqrt(variance + EPS)
    normal = centred * inv_std
    gain = 1.0 + scale[...]
    nx[...] = normal
    inv[...] = jnp.broadcast_to(inv_std, inv.shape)
    nrm[0] = (normal * gain + shift[...]).astype(BF16)
    nrm[1] = (cot[...].astype(F32) * gate[...]).astype(BF16)

    hd = HD
    wq_here = wq[...]
    wbuf[xl, xh, z, c] = jnp.concatenate([wq_here[:, hd : 3 * hd], wq_here[:, :hd], wo[...]], 1)

    meta_nat[...] = jnp.zeros(meta_nat.shape, jnp.int32)
    meta_nat[0:2, :] = edges[...]
    meta_nat[2:3, :] = jnp.full((1, edge), counts[0], jnp.int32)
    meta_nat[3:4, :] = jnp.full((1, edge), counts[1], jnp.int32)

    @pl.when(diag)
    def _():
        meta_own[...] = meta_nat[...]

    r_own = (y % nyh) * blk + xl * own
    home = at(y, c, xh, z, half)

    @pl.when(at_home)
    def _():
        for p in range(2):
            act[p, pl.ds(pl.multiple_of(r_own, own), own), :] = nrm[p]

    pl.semaphore_wait(barrier, greeted)

    def f1(p):
        return copy(
            nrm.at[p],
            act.at[p, pl.ds(pl.multiple_of(r_own, own), own)],
            f1s.at[p],
            f1r.at[xl, p],
            home,
        )

    for p in range(2):
        launch(functools.partial(f1, p), away)

    def wz(j):
        return copy(wbuf.at[xl, xh, z, c], wbuf.at[xl, xh, z, c], wzs.at[j], wzr.at[j], z_peer(j))

    def wz_in(j):
        block = wbuf.at[xl, xh, (z + nz - j) % nz, c]
        return copy(block, block, wzs.at[j], wzr.at[j], z_peer(j))

    for j in z_far:
        launch(functools.partial(wz, j))

    def meta_out(n):
        if n == 0:
            return copy(meta_nat, meta_own, ms.at[0], mr.at[0], sibling)
        return copy(meta_nat, meta_next, ms.at[n], mr.at[1], at_slab(before, n - 1))

    for n in range(3):
        launch(functools.partial(meta_out, n), diag)

    def f1_in(h, p):
        rows = pl.ds(pl.multiple_of((y % nyh) * blk + h * own, own), own)
        return copy(nrm.at[p], act.at[p, rows], f1s.at[p], f1r.at[h, p], sibling)

    def ring(i, p, h, way):
        rows = pl.ds(pl.multiple_of(i * blk + h * own, own), own)
        return copy(
            act.at[p, rows], act.at[p, rows], f2s.at[i, p, h, way], f2r.at[i, p, h],
            up if way == 0 else down,
        )

    here = y % nyh
    for i in range(nyh):
        apart = (y + ny - i - nyh * c) % ny
        back = (ny - apart) % ny
        for h in range(2):
            pending.append((functools.partial(ring, i, 0, h, 0), apart < nyh))
            pending.append((functools.partial(ring, i, 1, h, 0), apart < nyh - 1))
            pending.append((functools.partial(ring, i, 1, h, 1), back < nyh))
            pending.append((functools.partial(ring, i, 0, h, 1), back < nyh - 1))

    for h in (xl, 1 - xl):
        for p in range(2):
            if h is xl:

                @pl.when(jnp.logical_and(half == c, away))
                def _():
                    f1_in(h, p).wait_recv()

            else:

                @pl.when(half == c)
                def _():
                    f1_in(h, p).wait_recv()

            @pl.when(half == c)
            def _():
                ring(here, p, h, p).start()
                if nyh > 1:
                    ring(here, p, h, 1 - p).start()

    def turn(i):
        rows = pl.ds(pl.multiple_of(i * blk, blk), blk)
        for p in range(2):
            cols = pl.ds(pl.multiple_of(p * win + i * blk, blk), blk)
            xt[:, cols] = act[p, rows, :].T

    def project(i):
        rows = pl.ds(pl.multiple_of(i * blk, blk), blk)
        lane = lax.broadcasted_iota(jnp.int32, (blk, 2 * HD), 1)
        row = lax.broadcasted_iota(jnp.int32, (blk, 2 * HD), 0) + i * blk
        live = row < jnp.where(c == 0, meta_own[2:3, :], meta_own[3:4, :])
        for h in range(2):
            w = wbuf[h].reshape(d_model, 4 * HD)
            from_normed = dot(act[0, rows, :], w)
            from_upstream = dot(act[1, rows, :], w[:, 2 * HD :])
            kv[h, rows, :] = from_normed[:, : 2 * HD].astype(BF16)
            query = from_normed[:, 2 * HD :].astype(BF16).astype(F32) * (HD**-0.5)
            qa[h, 0, rows, :] = jnp.where(lane < HD, query, 0.0).astype(BF16)
            qa[h, 1, rows, :] = jnp.where(
                jnp.logical_and(lane >= HD, live), from_upstream, 0.0
            ).astype(BF16)

    @pl.when(half == c)
    def _():
        turn(here)

    def wx(j):
        block = wbuf.at[xl, xh, :, c]
        return copy(block, block, wxs.at[j], wxr.at[j], x_peer(j))

    def wx_in(j):
        xx = (x + nxx - j) % nxx
        block = wbuf.at[xx % 2, xx // 2, :, c]
        return copy(block, block, wxs.at[j], wxr.at[j], x_peer(j))

    def wc(k):
        block = wbuf.at[:, :, :, k]
        return copy(block, block, wcs, wcr, sibling)

    def weights_x():
        for j in range(1, nz):
            wz_in(j).wait_recv()
        for j in x_far:
            launch(functools.partial(wx, j))

    def weights_core():
        for j in range(1, nxx):
            wx_in(j).wait_recv()
        launch(functools.partial(wc, c))

    def weights_done():
        wc(1 - c).wait_recv()

        @pl.when(jnp.logical_not(diag))
        def _():
            meta_out(0).wait_recv()

        meta_out(1).wait_recv()

    def far(i):
        return (y + ny - i - nyh * c) % ny == nyh

    stages = [weights_x, weights_core, weights_done]
    for t in range(1, nyh + 1):
        if t == nyh:
            for stage in stages:
                stage()
            stages = []

            @pl.loop(0, nyh)
            def _(i):
                @pl.when(jnp.logical_not(far(i)))
                def _():
                    project(i)

        elif stages:
            stages.pop(0)()
        from_below = (y + 2 * ny - t - nyh * c) % ny
        from_above = (y + 2 * ny + t - nyh * c) % ny
        has_below = from_below < nyh
        has_above = from_above < nyh

        def relay(i, p, h, way):
            ring(i, p, h, way).wait_recv()
            if t < (nyh if p == way else nyh - 1):
                ring(i, p, h, way).start()

        for h in (xl, 1 - xl):
            for way_first in (True, False):
                if t == nyh and not way_first:
                    continue

                @pl.when(has_below)
                def _():
                    relay(from_below, 0 if way_first else 1, h, 0)

                @pl.when(has_above)
                def _():
                    relay(from_above, 1 if way_first else 0, h, 1)

        if t < nyh:

            @pl.when(has_above)
            def _():
                turn(from_above)

        @pl.when(has_below)
        def _():
            turn(from_below)
            if t == nyh:
                project(from_below)

    row_id = lax.broadcasted_iota(jnp.int32, (win, edge), 0) + c * win
    for k in range(2):
        oh[:, k * edge : (k + 1) * edge] = (row_id == meta_next[k : k + 1, :]).astype(F32).astype(BF16)
    for h in range(2):
        kvt[h, :, :win] = kv[h, :win, :].T
    for h in range(2):
        picked = dot(kvt[h, :, :win], oh[...]).astype(BF16)
        for k in range(2):
            e_send[k, h] = picked[:, k * edge : (k + 1) * edge]

    def edge_out(k):
        return copy(e_send.at[k], e_recv.at[c], es.at[k], er.at[c], at_slab(after, k))

    def edge_in(k):
        return copy(e_send.at[k], e_recv.at[k], es.at[k], er.at[k], sibling)

    for k in range(2):
        launch(functools.partial(edge_out, k))
    keys = win + edge
    step = 256 if win % 256 == 0 else win
    has_edge = mine > 0
    count = jnp.where(c == 0, meta_own[2:3, :], meta_own[3:4, :])
    limit = jnp.concatenate([count] * (step // edge), 1)

    for h in range(2):

        @pl.loop(0, win // step)
        def _(n):
            q_rows = pl.ds(pl.multiple_of(n * step, step), step)
            key_live = lax.broadcasted_iota(jnp.int32, (win, step), 0) < limit
            scores = dot(kv[h, :win, :], qa[h, 0, q_rows, :], ((1,), (1,)))
            scores = jnp.where(key_live, scores, NEG)
            largest = jnp.max(scores, 0, keepdims=True)
            exponent = jnp.exp(scores - largest)
            g_prob = dot(kv[h, :win, :], qa[h, 1, q_rows, :], ((1,), (1,)))
            part_e[h, :, q_rows] = exponent
            part_g[h, :, q_rows] = g_prob
            stat[h, 0:1, q_rows] = largest
            stat[h, 1:2, q_rows] = jnp.sum(exponent, 0, keepdims=True)
            stat[h, 2:3, q_rows] = jnp.sum(exponent * g_prob, 0, keepdims=True)

    for k in range(2):
        edge_in(k).wait_recv()
    for h in range(2):
        arrived = e_recv[0, h].astype(F32) + e_recv[1, h].astype(F32)
        kvt[h, :, win:] = arrived.astype(BF16)
        kv[h, win:, :] = arrived.T.astype(BF16)

    def scores_of(h):
        @pl.loop(0, win // step)
        def _(n):
            q_rows = pl.ds(pl.multiple_of(n * step, step), step)
            scores = dot(kv[h, win:, :], qa[h, 0, q_rows, :], ((1,), (1,)))
            scores = jnp.where(has_edge, scores, NEG)
            own_largest = stat[h, 0:1, q_rows]
            largest = jnp.maximum(own_largest, jnp.max(scores, 0, keepdims=True))
            exponent = jnp.exp(scores - largest)
            g_prob = dot(kv[h, win:, :], qa[h, 1, q_rows, :], ((1,), (1,)))
            shrink = jnp.exp(own_largest - largest)
            norm = 1.0 / (shrink * stat[h, 1:2, q_rows] + jnp.sum(exponent, 0, keepdims=True))
            centre = norm * (
                shrink * stat[h, 2:3, q_rows] + jnp.sum(exponent * g_prob, 0, keepdims=True)
            )
            probs = exponent * norm
            wts[h, win:, q_rows] = probs.astype(BF16)
            gsc[h, win:, q_rows] = (probs * (g_prob - centre)).astype(BF16)
            own_probs = part_e[h, :, q_rows] * (shrink * norm)
            wts[h, :win, q_rows] = own_probs.astype(BF16)
            gsc[h, :win, q_rows] = (own_probs * (part_g[h, :, q_rows] - centre)).astype(BF16)

        g_send[h] = (dot(gsc[h, win:, :], qa[h, 0]) + dot(wts[h, win:, :], qa[h, 1])).astype(BF16)

    def grad_out(h, k):
        return copy(g_send.at[h], g_recv.at[h, c], gs.at[h, k], gr.at[h, c], at_slab(before, k))

    def grad_in(h, k):
        return copy(g_send.at[h], g_recv.at[h, k], gs.at[h, k], gr.at[h, k], sibling)

    for h in range(2):
        scores_of(h)
        for k in range(2):
            launch(functools.partial(grad_out, h, k))

    row_limit = jnp.concatenate([count] * (win // edge), 1)
    lane = lax.broadcasted_iota(jnp.int32, (HD, win), 1)
    side = lax.broadcasted_iota(jnp.int32, (win, 2 * HD), 1)
    for h in range(2):
        cols = pl.ds(h * 2 * HD, 2 * HD)
        attended = jnp.where(lane < row_limit, dot(kvt[h, HD:, :], wts[h]), 0.0)
        g_query = dot(kvt[h, :HD, :], gsc[h]) * (HD**-0.5)
        pair = jnp.concatenate([g_query, attended], 0).T
        qab[:win, cols] = jnp.where(side < HD, pair, 0.0).astype(BF16)
        qab[win:, cols] = jnp.where(side >= HD, pair, 0.0).astype(BF16)

    def dc(q, k):
        return copy(dwb.at[q, :, :, :, k], r1.at[q], dcs.at[q], dcr.at[q], sibling)

    def dx(q, j):
        xx = (x + j) % nxx
        return copy(
            s2.at[q, xx % 2, xx // 2], r2.at[q, j], dxs.at[q, j], dxr.at[q, j], x_peer(j)
        )

    def dz(j):
        return copy(s3.at[(z + j) % nz], r3.at[j], dzs.at[j], dzr.at[j], z_peer(j))

    def weights_start(q, grad_w):
        blocks = grad_w.reshape(nxh, nz, 2, wr, 4 * HD)
        for h in range(2):
            block = blocks[:, :, :, :, h * 2 * HD : (h + 1) * 2 * HD]
            dwf[q, h] = block
            dwb[q, h] = block.astype(BF16)
        launch(functools.partial(dc, q, 1 - c))

    def weights_cross(q):
        dc(q, 1 - c).wait_recv()
        for h in range(2):
            s2[q, h] = (dwf[q, h, :, :, c] + r1[q, h].astype(F32)).astype(BF16)
        for j in x_far:
            launch(functools.partial(dx, q, j))

    def weights_total(q):
        total = dwf[q, xl, xh, :, c] + r1[q, xl, xh].astype(F32)
        for j in range(1, nxx):
            dx(q, j).wait_recv()
            total += r2[q, j].astype(F32)
        tot[:, q] = total
        s3[:, q] = total.astype(BF16)

    def weights_spread():
        for j in z_far:
            launch(functools.partial(dz, j))

    weights_start(1, dot(xt[...], qab[...]))

    for h in range(2):
        cols = pl.ds(h * 2 * HD, 2 * HD)
        own_pair = dot(gsc[h, :win, :], qa[h, 0]) + dot(wts[h, :win, :], qa[h, 1])
        for k in range(2):
            grad_in(h, k).wait_recv()
        returned = dot(oh[...], g_recv[h].reshape(2 * edge, 2 * HD))
        gkvb[:, cols] = (own_pair + returned).astype(BF16)

    weights_cross(1)

    def hops(way, part):
        return nyh if way == part else nyh - 1

    def chain_link(way, part, i, h):
        return copy(
            csd.at[way, part, i, h], crv.at[way, part, i, h],
            ccs.at[way, part, i, h], ccr.at[way, part, i, h], up if way == 0 else down,
        )

    def chain_end(way, part, i, h, yy):
        return copy(
            csd.at[way, part, i, h], orv.at[way, part],
            ows.at[way, part, h], owr.at[way, part], at(yy, h, xh, z, xl),
        )

    def own_out(h):
        return copy(osd.at[h], oself, oss.at[h], osr, at(y, h, xh, z, xl))

    def chain_piece(way, part, r, h):
        yy = (y + (r if way == 0 else ny - r)) % ny
        i = (yy + ny - nyh * c) % ny
        held = i < nyh

        @pl.when(held)
        def _():
            total = pvf[i, h * own : (h + 1) * own, part * halfcol : (part + 1) * halfcol]
            if r < hops(way, part):
                chain_link(way, part, i, h).wait_recv()
                total += crv[way, part, i, h].astype(F32)
            csd[way, part, i, h] = total.astype(BF16)

        if r > 1:
            launch(functools.partial(chain_link, way, part, i, h), held)
        else:
            launch(functools.partial(chain_end, way, part, i, h, yy), held)

    def chain(r):
        for h in range(2):
            for way in range(2):
                chain_piece(way, way, r, h)
        if r > 1:
            for h in range(2):
                for way in range(2):
                    chain_piece(way, 1 - way, r - 1, h)

    for b in range(nyh):
        rows = pl.ds(b * blk, blk)
        total = jnp.zeros((blk, d_model), F32)
        for h in range(2):
            cols = pl.ds(h * 2 * HD, 2 * HD)
            both = jnp.concatenate([gkvb[rows, cols], qab[rows, cols]], 1)
            total += dot(both, wbuf[h].reshape(d_model, 4 * HD), ((1,), (1,)))
        pvf[b] = total

    chain(nyh)

    @pl.when(half == c)
    def _():
        for h in range(2):
            osd[h] = pvf[here, h * own : (h + 1) * own, :].astype(BF16)

    for h in range(2):
        launch(
            functools.partial(own_out, h),
            jnp.logical_and(half == c, jnp.logical_or(xl != c, h != xl)),
        )

    @pl.when(at_home)
    def _():
        oself[...] = osd[xl]

    weights_start(0, dot(xt[:, :win], gkvb[...]))
    weights_cross(0)
    for r in range(nyh - 1, 0, -1):
        if r == 1:
            weights_total(0)
            weights_spread()
        chain(r)
        if r == nyh - 1:
            weights_total(1)

    def owner_in(way, part):
        return copy(
            csd.at[way, part, 0, 0], orv.at[way, part],
            ows.at[way, part, 0], owr.at[way, part], sibling,
        )

    for way in range(2):
        for part in range(2):
            owner_in(way, part).wait_recv()

    @pl.when(away)
    def _():
        own_out_arrived = copy(osd.at[0], oself, oss.at[0], osr, sibling)
        own_out_arrived.wait_recv()

    mine_sum = oself[...].astype(F32) + jnp.concatenate(
        [orv[0, part].astype(F32) + orv[1, part].astype(F32) for part in range(2)], 1
    )
    g_hat = mine_sum * gain
    normal_own = nx[...]
    g_tok = cot[...].astype(F32) + inv[:, 0:1] * (
        g_hat
        - jnp.mean(g_hat, 1, keepdims=True)
        - normal_own * jnp.mean(g_hat * normal_own, 1, keepdims=True)
    )
    out_tok[...] = g_tok.astype(BF16)

    final = tot[z]
    for j in range(1, nz):
        dz(j).wait_recv()
        final += r3[j].astype(F32)
    out_qkv[...] = jnp.concatenate([final[1, :, :HD], final[0]], 1)
    out_o[...] = final[1, :, HD:]

    drain()


def on_device(nxh, tokens, cotangent, w_qkv, w_out, mod_scale, mod_shift, mod_gate, counts, edge_index):
    ny = lax.axis_size("enc") // 2
    nz = lax.axis_size("slab") // (2 * nxh)
    own, d_model = tokens.shape
    edge = edge_index.shape[1]
    win = own * ny
    wr = w_qkv.shape[0]
    nyh, nxx = ny // 2, 2 * nxh
    wide = 4 * HD
    dma = pltpu.SemaphoreType.DMA
    vmem = pl.BlockSpec(memory_space=pltpu.VMEM)
    anywhere = pl.BlockSpec(memory_space=pltpu.MemorySpace.HBM)
    keys = win + edge
    blk = 2 * own
    scratch = [
        pltpu.VMEM((own, d_model), BF16),
        pltpu.VMEM((own, d_model), BF16),
        pltpu.VMEM((wr, 3 * HD), BF16),
        pltpu.VMEM((wr, HD), BF16),
        pltpu.VMEM((1, d_model), F32),
        pltpu.VMEM((1, d_model), F32),
        pltpu.VMEM((1, d_model), F32),
        pltpu.SMEM((2,), jnp.int32),
        pltpu.VMEM((2, edge), jnp.int32),
        pltpu.VMEM((2, own, d_model), BF16),
        pltpu.VMEM((own, d_model), F32),
        pltpu.VMEM((own, 128), F32),
        pltpu.VMEM((2, win, d_model), BF16),
        pltpu.VMEM((d_model, 2 * win), BF16),
        pltpu.VMEM((2, nxh, nz, 2, wr, wide), BF16),
        pltpu.VMEM((8, edge), jnp.int32),
        pltpu.VMEM((8, edge), jnp.int32),
        pltpu.VMEM((8, edge), jnp.int32),
        pltpu.VMEM((2, keys, 2 * HD), BF16),
        pltpu.VMEM((2, 2 * HD, keys), BF16),
        pltpu.VMEM((2, 2, win, 2 * HD), BF16),
        pltpu.VMEM((win, 2 * edge), BF16),
        pltpu.VMEM((2, 2, 2 * HD, edge), BF16),
        pltpu.VMEM((2, 2, 2 * HD, edge), BF16),
        pltpu.VMEM((2, edge, 2 * HD), BF16),
        pltpu.VMEM((2, 2, edge, 2 * HD), BF16),
        pltpu.VMEM((2, keys, win), BF16),
        pltpu.VMEM((2, keys, win), BF16),
        pltpu.VMEM((2, win, win), F32),
        pltpu.VMEM((2, win, win), F32),
        pltpu.VMEM((2, 8, win), F32),
        pltpu.VMEM((win, wide), BF16),
        pltpu.VMEM((2 * win, wide), BF16),
        pltpu.VMEM((nyh, blk, d_model), F32),
        pltpu.VMEM((2, 2, nyh, 2, own, d_model // 2), BF16),
        pltpu.VMEM((2, 2, nyh, 2, own, d_model // 2), BF16),
        pltpu.VMEM((2, own, d_model), BF16),
        pltpu.VMEM((own, d_model), BF16),
        pltpu.VMEM((2, 2, own, d_model // 2), BF16),
        pltpu.VMEM((2, 2, nxh, nz, 2, wr, 2 * HD), F32),
        pltpu.VMEM((2, 2, nxh, nz, 2, wr, 2 * HD), BF16),
        pltpu.VMEM((2, 2, nxh, nz, wr, 2 * HD), BF16),
        pltpu.VMEM((2, 2, nxh, nz, wr, 2 * HD), BF16),
        pltpu.VMEM((2, nxx, nz, wr, 2 * HD), BF16),
        pltpu.VMEM((nz, 2, wr, 2 * HD), F32),
        pltpu.VMEM((nz, 2, wr, 2 * HD), BF16),
        pltpu.VMEM((nz, 2, wr, 2 * HD), BF16),
        dma((9,)),
        dma((2,)), dma((2, 2)), dma((nyh, 2, 2, 2)), dma((nyh, 2, 2)),
        dma((nz,)), dma((nz,)), dma((nxx,)), dma((nxx,)), dma, dma,
        dma((3,)), dma((2,)), dma((2,)), dma((2,)), dma((2, 2)), dma((2, 2)),
        dma((2,)), dma((2,)), dma((2, nxx)), dma((2, nxx)), dma((nz,)), dma((nz,)),
        dma((2, 2, nyh, 2)), dma((2, 2, nyh, 2)), dma((2, 2, 2)), dma((2, 2)), dma((2,)), dma,
    ]
    grad_tokens, grad_qkv, grad_out = pl.pallas_call(
        functools.partial(kernel, ny, nxh, nz, win, edge),
        out_shape=(
            jax.ShapeDtypeStruct((own, d_model), BF16),
            jax.ShapeDtypeStruct((wr, 3 * HD), F32),
            jax.ShapeDtypeStruct((wr, HD), F32),
        ),
        in_specs=[anywhere] * 9,
        out_specs=(vmem, vmem, vmem),
        scratch_shapes=scratch,
        compiler_params=pltpu.CompilerParams(collective_id=0, has_side_effects=True, vmem_limit_bytes=36 * 1024 * 1024),
    )(
        *(
            pltpu.with_memory_space_constraint(a, pltpu.MemorySpace.HBM)
            for a in (
                tokens, cotangent, w_qkv, w_out.T,
                mod_scale[None, :], mod_shift[None, :], mod_gate[None, :], counts, edge_index,
            )
        )
    )
    return (grad_tokens, grad_qkv, grad_out.T)


def solution(mesh, nxh=2):
    placed = (
        P(("slab", "enc"), None),
        P(("slab", "enc"), None),
        P("slab", "enc"),
        P("enc", "slab"),
        P(),
        P(),
        P(),
        P("slab"),
        P("slab", None),
    )
    return jax.shard_map(
        functools.partial(on_device, nxh),
        mesh=mesh,
        in_specs=placed,
        out_specs=(P(("slab", "enc"), None), P("slab", "enc"), P("enc", "slab")),
        check_vma=False,
    )
```

```python
import functools

import jax
import jax.numpy as jnp
from jax import lax
from jax.experimental import pallas as pl
from jax.experimental.pallas import tpu as pltpu
from jax.sharding import PartitionSpec as P

HD = 64
EPS = 1e-06
NEG = -1000000000.0
MESH = pl.DeviceIdType.MESH
F32 = jnp.float32
BF16 = jnp.bfloat16


def dot(a, b, dims=((1,), (0,))):
    return lax.dot_general(a, b, (dims, ((), ())), preferred_element_type=F32)


def kernel(
    ny, nxh, nz, win, edge,
    tok_in, cot_in, wq_in, wo_in, scale_in, shift_in, gate_in, counts_in, edges_in,
    out_tok, out_qkv, out_o,
    tok, cot, wq, wo, scale, shift, gate, counts, edges,
    nrm, nx, inv, act, xt, wbuf, meta_nat, meta_own, meta_next,
    kv, kvt, qa, oh, e_send, e_recv, g_send, g_recv, wts, gsc, part_e, part_g, stat, gkvb, qab,
    pvf, csd, crv, osd, oself, orv, dwf, dwb, r1, s2, r2, tot, s3, r3,
    ins, f1s, f1r, f2s, f2r, wzs, wzr, wxs, wxr, wcs, wcr,
    ms, mr, es, er, gs, gr, dcs, dcr, dxs, dxr, dzs, dzr, ccs, ccr, ows, owr, oss, osr,
):
    ns = nxh * nz * 2
    nyh = ny // 2
    nxx = 2 * nxh
    z_far = sorted(range(1, nz), key=lambda j: -min(j, nz - j))
    x_far = sorted(range(1, nxx), key=lambda j: -min(j, nxx - j))
    own = tok.shape[0]
    blk = 2 * own
    d_model = tok.shape[1]
    wr = wq.shape[0]
    halfcol = d_model // 2

    enc = lax.axis_index("enc")
    slab = lax.axis_index("slab")
    y, xl = enc // 2, enc % 2
    xh, z, c = slab // (2 * nz), (slab // 2) % nz, slab % 2
    x = xh * 2 + xl
    mine = xh * 2 * nz + z * 2 + xl
    after = (mine + 1) % ns
    before = (mine + ns - 1) % ns
    half = y // nyh

    def at(y_, xl_, xh_, z_, c_):
        return {"enc": y_ * 2 + xl_, "slab": xh_ * (2 * nz) + z_ * 2 + c_}

    def at_slab(s_, c_):
        return {"enc": y * 2 + s_ % 2, "slab": (s_ // 2) * 2 + c_}

    sibling = at(y, xl, xh, z, 1 - c)
    up = at((y + 1) % ny, xl, xh, z, c)
    down = at((y + ny - 1) % ny, xl, xh, z, c)

    def z_peer(j):
        return at(y, xl, xh, (z + j) % nz, c)

    def x_peer(j):
        xx = (x + j) % nxx
        return at(y, xx % 2, xx // 2, z, c)

    def copy(src, dst, send, recv, to):
        return pltpu.make_async_remote_copy(
            src_ref=src, dst_ref=dst, send_sem=send, recv_sem=recv, device_id=to, device_id_type=MESH
        )

    at_home = jnp.logical_and(c == xl, half == c)
    away = jnp.logical_not(at_home)
    diag = c == xl

    pending = []

    def launch(make, when=None):
        if when is None:
            make().start()
            pending.append((make, None))
        else:

            @pl.when(when)
            def _():
                make().start()

            pending.append((make, when))

    def drain():
        for make, when in pending:
            if when is None:
                make().wait_send()
            else:

                @pl.when(when)
                def _():
                    make().wait_send()

    barrier = pltpu.get_barrier_semaphore()

    def greet(to):
        pl.semaphore_signal(barrier, inc=1, device_id=to, device_id_type=MESH)

    greet(sibling)
    greet(up)
    greet(down)
    for j in range(1, nz):
        greet(z_peer(j))
    for j in range(1, nxx):
        greet(x_peer(j))
    for k in range(2):
        greet(at_slab(after, k))
        greet(at_slab(before, k))

    @pl.when(half == c)
    def _():
        greet(at(y, 1 - xl, xh, z, xl))

    @pl.when(jnp.logical_and(half == c, xl != c))
    def _():
        greet(at(y, xl, xh, z, xl))

    above, below = (y + 1) % ny, (y + ny - 1) % ny
    greet(at(above, c, xh, z, half))
    greet(at(below, c, xh, z, half))

    @pl.when(away)
    def _():
        greet(at(y, c, xh, z, half))

    def count_of(flag):
        return flag.astype(jnp.int32)

    greeted = (
        3 + (nz - 1) + (nxx - 1) + 4 + 1
        - 2 * count_of(at_home)
        + 2 * count_of(half == c)
        + 2 * count_of(above // nyh == c)
        + 2 * count_of(below // nyh == c)
    )

    arrivals = [
        pltpu.make_async_copy(src, dst, ins.at[n])
        for n, (src, dst) in enumerate(
            (
                (tok_in, tok), (cot_in, cot), (wq_in, wq), (wo_in, wo), (scale_in, scale),
                (shift_in, shift), (gate_in, gate), (counts_in, counts), (edges_in, edges),
            )
        )
    ]
    for arrival in arrivals:
        arrival.start()
    for arrival in arrivals:
        arrival.wait()

    widened = tok[...].astype(F32)
    average = jnp.mean(widened, 1, keepdims=True)
    centred = widened - average
    variance = jnp.mean(centred * centred, 1, keepdims=True)
    inv_std = lax.rsqrt(variance + EPS)
    normal = centred * inv_std
    gain = 1.0 + scale[...]
    nx[...] = normal
    inv[...] = jnp.broadcast_to(inv_std, inv.shape)
    nrm[0] = (normal * gain + shift[...]).astype(BF16)
    nrm[1] = (cot[...].astype(F32) * gate[...]).astype(BF16)

    hd = HD
    wq_here = wq[...]
    wbuf[xl, xh, z, c] = jnp.concatenate([wq_here[:, hd : 3 * hd], wq_here[:, :hd], wo[...]], 1)

    meta_nat[...] = jnp.zeros(meta_nat.shape, jnp.int32)
    meta_nat[0:2, :] = edges[...]
    meta_nat[2:3, :] = jnp.full((1, edge), counts[0], jnp.int32)
    meta_nat[3:4, :] = jnp.full((1, edge), counts[1], jnp.int32)

    @pl.when(diag)
    def _():
        meta_own[...] = meta_nat[...]

    r_own = (y % nyh) * blk + xl * own
    home = at(y, c, xh, z, half)

    @pl.when(at_home)
    def _():
        for p in range(2):
            act[p, pl.ds(pl.multiple_of(r_own, own), own), :] = nrm[p]

    pl.semaphore_wait(barrier, greeted)

    def f1(p):
        return copy(
            nrm.at[p],
            act.at[p, pl.ds(pl.multiple_of(r_own, own), own)],
            f1s.at[p],
            f1r.at[xl, p],
            home,
        )

    for p in range(2):
        launch(functools.partial(f1, p), away)

    def wz(j):
        return copy(wbuf.at[xl, xh, z, c], wbuf.at[xl, xh, z, c], wzs.at[j], wzr.at[j], z_peer(j))

    def wz_in(j):
        block = wbuf.at[xl, xh, (z + nz - j) % nz, c]
        return copy(block, block, wzs.at[j], wzr.at[j], z_peer(j))

    for j in z_far:
        launch(functools.partial(wz, j))

    def meta_out(n):
        if n == 0:
            return copy(meta_nat, meta_own, ms.at[0], mr.at[0], sibling)
        return copy(meta_nat, meta_next, ms.at[n], mr.at[1], at_slab(before, n - 1))

    for n in range(3):
        launch(functools.partial(meta_out, n), diag)

    def f1_in(h, p):
        rows = pl.ds(pl.multiple_of((y % nyh) * blk + h * own, own), own)
        return copy(nrm.at[p], act.at[p, rows], f1s.at[p], f1r.at[h, p], sibling)

    def ring(i, p, h, way):
        rows = pl.ds(pl.multiple_of(i * blk + h * own, own), own)
        return copy(
            act.at[p, rows], act.at[p, rows], f2s.at[i, p, h, way], f2r.at[i, p, h],
            up if way == 0 else down,
        )

    here = y % nyh
    for i in range(nyh):
        apart = (y + ny - i - nyh * c) % ny
        back = (ny - apart) % ny
        for h in range(2):
            pending.append((functools.partial(ring, i, 0, h, 0), apart < nyh))
            pending.append((functools.partial(ring, i, 1, h, 0), apart < nyh - 1))
            pending.append((functools.partial(ring, i, 1, h, 1), back < nyh))
            pending.append((functools.partial(ring, i, 0, h, 1), back < nyh - 1))

    for h in (xl, 1 - xl):
        for p in range(2):
            if h is xl:

                @pl.when(jnp.logical_and(half == c, away))
                def _():
                    f1_in(h, p).wait_recv()

            else:

                @pl.when(half == c)
                def _():
                    f1_in(h, p).wait_recv()

            @pl.when(half == c)
            def _():
                ring(here, p, h, p).start()
                if nyh > 1:
                    ring(here, p, h, 1 - p).start()

    def turn(i):
        rows = pl.ds(pl.multiple_of(i * blk, blk), blk)
        for p in range(2):
            cols = pl.ds(pl.multiple_of(p * win + i * blk, blk), blk)
            xt[:, cols] = act[p, rows, :].T

    def project(i):
        rows = pl.ds(pl.multiple_of(i * blk, blk), blk)
        lane = lax.broadcasted_iota(jnp.int32, (blk, 2 * HD), 1)
        row = lax.broadcasted_iota(jnp.int32, (blk, 2 * HD), 0) + i * blk
        live = row < jnp.where(c == 0, meta_own[2:3, :], meta_own[3:4, :])
        for h in range(2):
            w = wbuf[h].reshape(d_model, 4 * HD)
            from_normed = dot(act[0, rows, :], w)
            from_upstream = dot(act[1, rows, :], w[:, 2 * HD :])
            pair = from_normed[:, : 2 * HD].astype(BF16)
            kv[h, rows, :] = pair
            kvt[h, :, rows] = pair.T
            query = from_normed[:, 2 * HD :].astype(BF16).astype(F32) * (HD**-0.5)
            qa[h, 0, rows, :] = jnp.where(lane < HD, query, 0.0).astype(BF16)
            qa[h, 1, rows, :] = jnp.where(
                jnp.logical_and(lane >= HD, live), from_upstream, 0.0
            ).astype(BF16)

    @pl.when(half == c)
    def _():
        turn(here)

    def wx(j):
        block = wbuf.at[xl, xh, :, c]
        return copy(block, block, wxs.at[j], wxr.at[j], x_peer(j))

    def wx_in(j):
        xx = (x + nxx - j) % nxx
        block = wbuf.at[xx % 2, xx // 2, :, c]
        return copy(block, block, wxs.at[j], wxr.at[j], x_peer(j))

    def wc(k):
        block = wbuf.at[:, :, :, k]
        return copy(block, block, wcs, wcr, sibling)

    def weights_x():
        for j in range(1, nz):
            wz_in(j).wait_recv()
        for j in x_far:
            launch(functools.partial(wx, j))

    def weights_core():
        for j in range(1, nxx):
            wx_in(j).wait_recv()
        launch(functools.partial(wc, c))

    def weights_done():
        wc(1 - c).wait_recv()

        @pl.when(jnp.logical_not(diag))
        def _():
            meta_out(0).wait_recv()

        meta_out(1).wait_recv()

    def hot():
        row_id = lax.broadcasted_iota(jnp.int32, (win, edge), 0) + c * win
        for k in range(2):
            hit = row_id == meta_next[k : k + 1, :]
            oh[:, k * edge : (k + 1) * edge] = hit.astype(F32).astype(BF16)

    def project_near(t):
        @pl.loop(0, nyh)
        def _(i):
            apart = (y + ny - i - nyh * c) % ny

            @pl.when(jnp.minimum(apart, ny - apart) < t)
            def _():
                project(i)

    stages = [weights_x, weights_core, weights_done]
    ready = False
    for t in range(1, nyh + 1):
        if stages:
            stages.pop(0)()
            if t == nyh:
                for stage in stages:
                    stage()
                stages = []
            if not stages:
                hot()
                project_near(t)
                ready = True
        from_below = (y + 2 * ny - t - nyh * c) % ny
        from_above = (y + 2 * ny + t - nyh * c) % ny
        has_below = from_below < nyh
        has_above = from_above < nyh

        def relay(i, p, h, way):
            ring(i, p, h, way).wait_recv()
            if t < (nyh if p == way else nyh - 1):
                ring(i, p, h, way).start()

        for h in (xl, 1 - xl):
            for way_first in (True, False):
                if t == nyh and not way_first:
                    continue

                @pl.when(has_below)
                def _():
                    relay(from_below, 0 if way_first else 1, h, 0)

                @pl.when(has_above)
                def _():
                    relay(from_above, 1 if way_first else 0, h, 1)

        if t < nyh:

            @pl.when(has_above)
            def _():
                if ready:
                    project(from_above)
                turn(from_above)

        @pl.when(has_below)
        def _():
            if ready:
                project(from_below)
            if t < nyh:
                turn(from_below)

    def edge_out(h, k):
        return copy(e_send.at[h, k], e_recv.at[h, c], es.at[h, k], er.at[h, c], at_slab(after, k))

    def edge_in(h, k):
        return copy(e_send.at[h, k], e_recv.at[h, k], es.at[h, k], er.at[h, k], sibling)

    for h in range(2):
        picked = dot(kvt[h, :, :win], oh[...]).astype(BF16)
        for k in range(2):
            e_send[h, k] = picked[:, k * edge : (k + 1) * edge]
            launch(functools.partial(edge_out, h, k))

    last = (y + ny - nyh - nyh * c) % ny

    @pl.when(last < nyh)
    def _():
        turn(last)

    keys = win + edge
    step = 256 if win % 256 == 0 else win
    has_edge = mine > 0
    count = jnp.where(c == 0, meta_own[2:3, :], meta_own[3:4, :])
    limit = jnp.concatenate([count] * (step // edge), 1)

    for h in range(2):

        @pl.loop(0, win // step)
        def _(n):
            q_rows = pl.ds(pl.multiple_of(n * step, step), step)
            key_live = lax.broadcasted_iota(jnp.int32, (win, step), 0) < limit
            scores = dot(kv[h, :win, :], qa[h, 0, q_rows, :], ((1,), (1,)))
            scores = jnp.where(key_live, scores, NEG)
            largest = jnp.max(scores, 0, keepdims=True)
            exponent = jnp.exp(scores - largest)
            g_prob = dot(kv[h, :win, :], qa[h, 1, q_rows, :], ((1,), (1,)))
            part_e[h, :, q_rows] = exponent
            part_g[h, :, q_rows] = g_prob
            stat[h, 0:1, q_rows] = largest
            stat[h, 1:2, q_rows] = jnp.sum(exponent, 0, keepdims=True)
            stat[h, 2:3, q_rows] = jnp.sum(exponent * g_prob, 0, keepdims=True)

    def scores_of(h):
        for k in range(2):
            edge_in(h, k).wait_recv()
        arrived = e_recv[h, 0].astype(F32) + e_recv[h, 1].astype(F32)
        kvt[h, :, win:] = arrived.astype(BF16)
        kv[h, win:, :] = arrived.T.astype(BF16)

        @pl.loop(0, win // step)
        def _(n):
            q_rows = pl.ds(pl.multiple_of(n * step, step), step)
            scores = dot(kv[h, win:, :], qa[h, 0, q_rows, :], ((1,), (1,)))
            scores = jnp.where(has_edge, scores, NEG)
            own_largest = stat[h, 0:1, q_rows]
            largest = jnp.maximum(own_largest, jnp.max(scores, 0, keepdims=True))
            exponent = jnp.exp(scores - largest)
            g_prob = dot(kv[h, win:, :], qa[h, 1, q_rows, :], ((1,), (1,)))
            shrink = jnp.exp(own_largest - largest)
            norm = 1.0 / (shrink * stat[h, 1:2, q_rows] + jnp.sum(exponent, 0, keepdims=True))
            centre = norm * (
                shrink * stat[h, 2:3, q_rows] + jnp.sum(exponent * g_prob, 0, keepdims=True)
            )
            probs = exponent * norm
            wts[h, win:, q_rows] = probs.astype(BF16)
            gsc[h, win:, q_rows] = (probs * (g_prob - centre)).astype(BF16)
            own_probs = part_e[h, :, q_rows] * (shrink * norm)
            wts[h, :win, q_rows] = own_probs.astype(BF16)
            gsc[h, :win, q_rows] = (own_probs * (part_g[h, :, q_rows] - centre)).astype(BF16)

        g_send[h] = (dot(gsc[h, win:, :], qa[h, 0]) + dot(wts[h, win:, :], qa[h, 1])).astype(BF16)

    def grad_out(h, k):
        return copy(g_send.at[h], g_recv.at[h, c], gs.at[h, k], gr.at[h, c], at_slab(before, k))

    def grad_in(h, k):
        return copy(g_send.at[h], g_recv.at[h, k], gs.at[h, k], gr.at[h, k], sibling)

    for h in range(2):
        scores_of(h)
        for k in range(2):
            launch(functools.partial(grad_out, h, k))

    row_limit = jnp.concatenate([count] * (win // edge), 1)
    lane = lax.broadcasted_iota(jnp.int32, (HD, win), 1)
    side = lax.broadcasted_iota(jnp.int32, (win, 2 * HD), 1)
    for h in range(2):
        cols = pl.ds(h * 2 * HD, 2 * HD)
        attended = jnp.where(lane < row_limit, dot(kvt[h, HD:, :], wts[h]), 0.0)
        g_query = dot(kvt[h, :HD, :], gsc[h]) * (HD**-0.5)
        pair = jnp.concatenate([g_query, attended], 0).T
        qab[:win, cols] = jnp.where(side < HD, pair, 0.0).astype(BF16)
        qab[win:, cols] = jnp.where(side >= HD, pair, 0.0).astype(BF16)

    def dc(q, k):
        return copy(dwb.at[q, :, :, :, k], r1.at[q], dcs.at[q], dcr.at[q], sibling)

    def dx(q, j):
        xx = (x + j) % nxx
        return copy(
            s2.at[q, xx % 2, xx // 2], r2.at[q, j], dxs.at[q, j], dxr.at[q, j], x_peer(j)
        )

    def dz(j):
        return copy(s3.at[(z + j) % nz], r3.at[j], dzs.at[j], dzr.at[j], z_peer(j))

    def weights_start(q, grad_w):
        blocks = grad_w.reshape(nxh, nz, 2, wr, 4 * HD)
        for h in range(2):
            block = blocks[:, :, :, :, h * 2 * HD : (h + 1) * 2 * HD]
            dwf[q, h] = block
            dwb[q, h] = block.astype(BF16)
        launch(functools.partial(dc, q, 1 - c))

    def weights_cross(q):
        dc(q, 1 - c).wait_recv()
        for h in range(2):
            s2[q, h] = (dwf[q, h, :, :, c] + r1[q, h].astype(F32)).astype(BF16)
        for j in x_far:
            launch(functools.partial(dx, q, j))

    def weights_total(q):
        total = dwf[q, xl, xh, :, c] + r1[q, xl, xh].astype(F32)
        for j in range(1, nxx):
            dx(q, j).wait_recv()
            total += r2[q, j].astype(F32)
        tot[:, q] = total
        s3[:, q] = total.astype(BF16)

    def weights_spread():
        for j in z_far:
            launch(functools.partial(dz, j))

    weights_start(1, dot(xt[...], qab[...]))

    for h in range(2):
        cols = pl.ds(h * 2 * HD, 2 * HD)
        own_pair = dot(gsc[h, :win, :], qa[h, 0]) + dot(wts[h, :win, :], qa[h, 1])
        for k in range(2):
            grad_in(h, k).wait_recv()
        returned = dot(oh[...], g_recv[h].reshape(2 * edge, 2 * HD))
        gkvb[:, cols] = (own_pair + returned).astype(BF16)

    weights_cross(1)

    def hops(way, part):
        return nyh if way == part else nyh - 1

    def chain_link(way, part, i, h):
        return copy(
            csd.at[way, part, i, h], crv.at[way, part, i, h],
            ccs.at[way, part, i, h], ccr.at[way, part, i, h], up if way == 0 else down,
        )

    def chain_end(way, part, i, h, yy):
        return copy(
            csd.at[way, part, i, h], orv.at[way, part],
            ows.at[way, part, h], owr.at[way, part], at(yy, h, xh, z, xl),
        )

    def own_out(h):
        return copy(osd.at[h], oself, oss.at[h], osr, at(y, h, xh, z, xl))

    def chain_piece(way, part, r, h):
        yy = (y + (r if way == 0 else ny - r)) % ny
        i = (yy + ny - nyh * c) % ny
        held = i < nyh

        @pl.when(held)
        def _():
            total = pvf[i, h * own : (h + 1) * own, part * halfcol : (part + 1) * halfcol]
            if r < hops(way, part):
                chain_link(way, part, i, h).wait_recv()
                total += crv[way, part, i, h].astype(F32)
            csd[way, part, i, h] = total.astype(BF16)

        if r > 1:
            launch(functools.partial(chain_link, way, part, i, h), held)
        else:
            launch(functools.partial(chain_end, way, part, i, h, yy), held)

    def chain(r):
        for h in range(2):
            for way in range(2):
                chain_piece(way, way, r, h)
        if r > 1:
            for h in range(2):
                for way in range(2):
                    chain_piece(way, 1 - way, r - 1, h)

    for b in range(nyh):
        rows = pl.ds(b * blk, blk)
        total = jnp.zeros((blk, d_model), F32)
        for h in range(2):
            cols = pl.ds(h * 2 * HD, 2 * HD)
            both = jnp.concatenate([gkvb[rows, cols], qab[rows, cols]], 1)
            total += dot(both, wbuf[h].reshape(d_model, 4 * HD), ((1,), (1,)))
        pvf[b] = total

    chain(nyh)

    @pl.when(half == c)
    def _():
        for h in range(2):
            osd[h] = pvf[here, h * own : (h + 1) * own, :].astype(BF16)

    for h in range(2):
        launch(
            functools.partial(own_out, h),
            jnp.logical_and(half == c, jnp.logical_or(xl != c, h != xl)),
        )

    @pl.when(at_home)
    def _():
        oself[...] = osd[xl]

    weights_start(0, dot(xt[:, :win], gkvb[...]))
    weights_cross(0)
    for r in range(nyh - 1, 0, -1):
        if r == 1:
            weights_total(0)
            weights_spread()
        chain(r)
        if r == nyh - 1:
            weights_total(1)

    def owner_in(way, part):
        return copy(
            csd.at[way, part, 0, 0], orv.at[way, part],
            ows.at[way, part, 0], owr.at[way, part], sibling,
        )

    for way in range(2):
        for part in range(2):
            owner_in(way, part).wait_recv()

    @pl.when(away)
    def _():
        own_out_arrived = copy(osd.at[0], oself, oss.at[0], osr, sibling)
        own_out_arrived.wait_recv()

    mine_sum = oself[...].astype(F32) + jnp.concatenate(
        [orv[0, part].astype(F32) + orv[1, part].astype(F32) for part in range(2)], 1
    )
    g_hat = mine_sum * gain
    normal_own = nx[...]
    g_tok = cot[...].astype(F32) + inv[:, 0:1] * (
        g_hat
        - jnp.mean(g_hat, 1, keepdims=True)
        - normal_own * jnp.mean(g_hat * normal_own, 1, keepdims=True)
    )
    out_tok[...] = g_tok.astype(BF16)

    final = tot[z]
    for j in range(1, nz):
        dz(j).wait_recv()
        final += r3[j].astype(F32)
    out_qkv[...] = jnp.concatenate([final[1, :, :HD], final[0]], 1)
    out_o[...] = final[1, :, HD:]

    drain()


def write_out(tok, qkv, o, out_tok, out_qkv, out_o, sems):
    moves = [
        pltpu.make_async_copy(src, dst, sems.at[n])
        for n, (src, dst) in enumerate(((tok, out_tok), (qkv, out_qkv), (o, out_o)))
    ]
    for move in moves:
        move.start()
    for move in moves:
        move.wait()


def on_device(nxh, tokens, cotangent, w_qkv, w_out, mod_scale, mod_shift, mod_gate, counts, edge_index):
    ny = lax.axis_size("enc") // 2
    nz = lax.axis_size("slab") // (2 * nxh)
    own, d_model = tokens.shape
    edge = edge_index.shape[1]
    win = own * ny
    wr = w_qkv.shape[0]
    nyh, nxx = ny // 2, 2 * nxh
    wide = 4 * HD
    dma = pltpu.SemaphoreType.DMA
    vmem = pl.BlockSpec(memory_space=pltpu.VMEM)
    anywhere = pl.BlockSpec(memory_space=pltpu.MemorySpace.HBM)
    keys = win + edge
    blk = 2 * own
    scratch = [
        pltpu.VMEM((own, d_model), BF16),
        pltpu.VMEM((own, d_model), BF16),
        pltpu.VMEM((wr, 3 * HD), BF16),
        pltpu.VMEM((wr, HD), BF16),
        pltpu.VMEM((1, d_model), F32),
        pltpu.VMEM((1, d_model), F32),
        pltpu.VMEM((1, d_model), F32),
        pltpu.SMEM((2,), jnp.int32),
        pltpu.VMEM((2, edge), jnp.int32),
        pltpu.VMEM((2, own, d_model), BF16),
        pltpu.VMEM((own, d_model), F32),
        pltpu.VMEM((own, 128), F32),
        pltpu.VMEM((2, win, d_model), BF16),
        pltpu.VMEM((d_model, 2 * win), BF16),
        pltpu.VMEM((2, nxh, nz, 2, wr, wide), BF16),
        pltpu.VMEM((8, edge), jnp.int32),
        pltpu.VMEM((8, edge), jnp.int32),
        pltpu.VMEM((8, edge), jnp.int32),
        pltpu.VMEM((2, keys, 2 * HD), BF16),
        pltpu.VMEM((2, 2 * HD, keys), BF16),
        pltpu.VMEM((2, 2, win, 2 * HD), BF16),
        pltpu.VMEM((win, 2 * edge), BF16),
        pltpu.VMEM((2, 2, 2 * HD, edge), BF16),
        pltpu.VMEM((2, 2, 2 * HD, edge), BF16),
        pltpu.VMEM((2, edge, 2 * HD), BF16),
        pltpu.VMEM((2, 2, edge, 2 * HD), BF16),
        pltpu.VMEM((2, keys, win), BF16),
        pltpu.VMEM((2, keys, win), BF16),
        pltpu.VMEM((2, win, win), F32),
        pltpu.VMEM((2, win, win), F32),
        pltpu.VMEM((2, 8, win), F32),
        pltpu.VMEM((win, wide), BF16),
        pltpu.VMEM((2 * win, wide), BF16),
        pltpu.VMEM((nyh, blk, d_model), F32),
        pltpu.VMEM((2, 2, nyh, 2, own, d_model // 2), BF16),
        pltpu.VMEM((2, 2, nyh, 2, own, d_model // 2), BF16),
        pltpu.VMEM((2, own, d_model), BF16),
        pltpu.VMEM((own, d_model), BF16),
        pltpu.VMEM((2, 2, own, d_model // 2), BF16),
        pltpu.VMEM((2, 2, nxh, nz, 2, wr, 2 * HD), F32),
        pltpu.VMEM((2, 2, nxh, nz, 2, wr, 2 * HD), BF16),
        pltpu.VMEM((2, 2, nxh, nz, wr, 2 * HD), BF16),
        pltpu.VMEM((2, 2, nxh, nz, wr, 2 * HD), BF16),
        pltpu.VMEM((2, nxx, nz, wr, 2 * HD), BF16),
        pltpu.VMEM((nz, 2, wr, 2 * HD), F32),
        pltpu.VMEM((nz, 2, wr, 2 * HD), BF16),
        pltpu.VMEM((nz, 2, wr, 2 * HD), BF16),
        dma((9,)),
        dma((2,)), dma((2, 2)), dma((nyh, 2, 2, 2)), dma((nyh, 2, 2)),
        dma((nz,)), dma((nz,)), dma((nxx,)), dma((nxx,)), dma, dma,
        dma((3,)), dma((2,)), dma((2, 2)), dma((2, 2)), dma((2, 2)), dma((2, 2)),
        dma((2,)), dma((2,)), dma((2, nxx)), dma((2, nxx)), dma((nz,)), dma((nz,)),
        dma((2, 2, nyh, 2)), dma((2, 2, nyh, 2)), dma((2, 2, 2)), dma((2, 2)), dma((2,)), dma,
    ]
    grad_tokens, grad_qkv, grad_out = pl.pallas_call(
        functools.partial(kernel, ny, nxh, nz, win, edge),
        out_shape=(
            jax.ShapeDtypeStruct((own, d_model), BF16),
            jax.ShapeDtypeStruct((wr, 3 * HD), F32),
            jax.ShapeDtypeStruct((wr, HD), F32),
        ),
        in_specs=[anywhere] * 9,
        out_specs=(vmem, vmem, vmem),
        scratch_shapes=scratch,
        compiler_params=pltpu.CompilerParams(collective_id=0, has_side_effects=True, vmem_limit_bytes=36 * 1024 * 1024),
    )(
        *(
            pltpu.with_memory_space_constraint(a, pltpu.MemorySpace.HBM)
            for a in (
                tokens, cotangent, w_qkv, w_out.T,
                mod_scale[None, :], mod_shift[None, :], mod_gate[None, :], counts, edge_index,
            )
        )
    )
    grad_tokens, grad_qkv, grad_out = pl.pallas_call(
        write_out,
        out_shape=tuple(jax.ShapeDtypeStruct(a.shape, a.dtype) for a in (grad_tokens, grad_qkv, grad_out)),
        in_specs=[vmem] * 3,
        out_specs=(anywhere,) * 3,
        scratch_shapes=[dma((3,))],
        compiler_params=pltpu.CompilerParams(vmem_limit_bytes=4 * 1024 * 1024),
    )(grad_tokens, grad_qkv, grad_out)
    return (grad_tokens, grad_qkv, grad_out.T)


def solution(mesh, nxh=2):
    placed = (
        P(("slab", "enc"), None),
        P(("slab", "enc"), None),
        P("slab", "enc"),
        P("enc", "slab"),
        P(),
        P(),
        P(),
        P("slab"),
        P("slab", None),
    )
    return jax.shard_map(
        functools.partial(on_device, nxh),
        mesh=mesh,
        in_specs=placed,
        out_specs=(P(("slab", "enc"), None), P("slab", "enc"), P("enc", "slab")),
        check_vma=False,
    )
```

```python
import functools

import jax
import jax.numpy as jnp
from jax import lax
from jax.experimental import pallas as pl
from jax.experimental.pallas import tpu as pltpu
from jax.sharding import PartitionSpec as P

HD = 64
EPS = 1e-06
NEG = -1000000000.0
MESH = pl.DeviceIdType.MESH
F32 = jnp.float32
BF16 = jnp.bfloat16


def dot(a, b, dims=((1,), (0,))):
    return lax.dot_general(a, b, (dims, ((), ())), preferred_element_type=F32)


def kernel(
    ny, nxh, nz, win, edge,
    tok_in, cot_in, wq_in, wo_in, scale_in, shift_in, gate_in, counts_in, edges_in,
    out_tok, out_qkv, out_o,
    tok, cot, wq, wo, scale, shift, gate, counts, edges,
    nrm, nx, inv, act, xt, wbuf, meta_nat, meta_own, meta_next,
    kv, kvt, qa, oh, e_send, e_recv, g_send, g_recv, wts, gsc, part_e, part_g, stat, gkvb, qab,
    pvf, csd, crv, osd, oself, orv, dwf, dwb, r1, s2, r2, tot, s3, r3,
    ins, f1s, f1r, f2s, f2r, wzs, wzr, wxs, wxr, wcs, wcr,
    ms, mr, es, er, gs, gr, dcs, dcr, dxs, dxr, dzs, dzr, ccs, ccr, ows, owr, oss, osr,
):
    ns = nxh * nz * 2
    nyh = ny // 2
    nxx = 2 * nxh
    z_far = sorted(range(1, nz), key=lambda j: -min(j, nz - j))
    x_far = sorted(range(1, nxx), key=lambda j: -min(j, nxx - j))
    own = tok.shape[0]
    blk = 2 * own
    d_model = tok.shape[1]
    wr = wq.shape[0]
    halfcol = d_model // 2

    enc = lax.axis_index("enc")
    slab = lax.axis_index("slab")
    y, xl = enc // 2, enc % 2
    xh, z, c = slab // (2 * nz), (slab // 2) % nz, slab % 2
    x = xh * 2 + xl
    mine = xh * 2 * nz + z * 2 + xl
    after = (mine + 1) % ns
    before = (mine + ns - 1) % ns
    half = y // nyh

    def at(y_, xl_, xh_, z_, c_):
        return {"enc": y_ * 2 + xl_, "slab": xh_ * (2 * nz) + z_ * 2 + c_}

    def at_slab(s_, c_):
        return {"enc": y * 2 + s_ % 2, "slab": (s_ // 2) * 2 + c_}

    sibling = at(y, xl, xh, z, 1 - c)
    up = at((y + 1) % ny, xl, xh, z, c)
    down = at((y + ny - 1) % ny, xl, xh, z, c)

    def z_peer(j):
        return at(y, xl, xh, (z + j) % nz, c)

    def x_peer(j):
        xx = (x + j) % nxx
        return at(y, xx % 2, xx // 2, z, c)

    def copy(src, dst, send, recv, to):
        return pltpu.make_async_remote_copy(
            src_ref=src, dst_ref=dst, send_sem=send, recv_sem=recv, device_id=to, device_id_type=MESH
        )

    at_home = jnp.logical_and(c == xl, half == c)
    away = jnp.logical_not(at_home)
    diag = c == xl

    pending = []

    def launch(make, when=None):
        if when is None:
            make().start()
            pending.append((make, None))
        else:

            @pl.when(when)
            def _():
                make().start()

            pending.append((make, when))

    def drain():
        for make, when in pending:
            if when is None:
                make().wait_send()
            else:

                @pl.when(when)
                def _():
                    make().wait_send()

    barrier = pltpu.get_barrier_semaphore()

    def greet(to):
        pl.semaphore_signal(barrier, inc=1, device_id=to, device_id_type=MESH)

    greet(sibling)
    greet(up)
    greet(down)
    for j in range(1, nz):
        greet(z_peer(j))
    for j in range(1, nxx):
        greet(x_peer(j))
    for k in range(2):
        greet(at_slab(after, k))
        greet(at_slab(before, k))

    @pl.when(half == c)
    def _():
        greet(at(y, 1 - xl, xh, z, xl))

    @pl.when(jnp.logical_and(half == c, xl != c))
    def _():
        greet(at(y, xl, xh, z, xl))

    above, below = (y + 1) % ny, (y + ny - 1) % ny
    greet(at(above, c, xh, z, half))
    greet(at(below, c, xh, z, half))

    @pl.when(away)
    def _():
        greet(at(y, c, xh, z, half))

    def count_of(flag):
        return flag.astype(jnp.int32)

    greeted = (
        3 + (nz - 1) + (nxx - 1) + 4 + 1
        - 2 * count_of(at_home)
        + 2 * count_of(half == c)
        + 2 * count_of(above // nyh == c)
        + 2 * count_of(below // nyh == c)
    )

    arrivals = [
        pltpu.make_async_copy(src, dst, ins.at[n])
        for n, (src, dst) in enumerate(
            (
                (tok_in, tok), (cot_in, cot), (wq_in, wq), (wo_in, wo), (scale_in, scale),
                (shift_in, shift), (gate_in, gate), (counts_in, counts), (edges_in, edges),
            )
        )
    ]
    for arrival in arrivals:
        arrival.start()
    for arrival in arrivals:
        arrival.wait()

    widened = tok[...].astype(F32)
    average = jnp.mean(widened, 1, keepdims=True)
    centred = widened - average
    variance = jnp.mean(centred * centred, 1, keepdims=True)
    inv_std = lax.rsqrt(variance + EPS)
    normal = centred * inv_std
    gain = 1.0 + scale[...]
    nx[...] = normal
    inv[...] = jnp.broadcast_to(inv_std, inv.shape)
    nrm[0] = (normal * gain + shift[...]).astype(BF16)
    nrm[1] = (cot[...].astype(F32) * gate[...]).astype(BF16)

    hd = HD
    wq_here = wq[...]
    wbuf[xl, xh, z, c] = jnp.concatenate([wq_here[:, hd : 3 * hd], wq_here[:, :hd], wo[...]], 1)

    meta_nat[...] = jnp.zeros(meta_nat.shape, jnp.int32)
    meta_nat[0:2, :] = edges[...]
    meta_nat[2:3, :] = jnp.full((1, edge), counts[0], jnp.int32)
    meta_nat[3:4, :] = jnp.full((1, edge), counts[1], jnp.int32)

    @pl.when(diag)
    def _():
        meta_own[...] = meta_nat[...]

    r_own = (y % nyh) * blk + xl * own
    home = at(y, c, xh, z, half)

    @pl.when(at_home)
    def _():
        for p in range(2):
            act[p, pl.ds(pl.multiple_of(r_own, own), own), :] = nrm[p]

    pl.semaphore_wait(barrier, greeted)

    def f1(p):
        return copy(
            nrm.at[p],
            act.at[p, pl.ds(pl.multiple_of(r_own, own), own)],
            f1s.at[p],
            f1r.at[xl, p],
            home,
        )

    for p in range(2):
        launch(functools.partial(f1, p), away)

    def wz(j):
        return copy(wbuf.at[xl, xh, z, c], wbuf.at[xl, xh, z, c], wzs.at[j], wzr.at[j], z_peer(j))

    def wz_in(j):
        block = wbuf.at[xl, xh, (z + nz - j) % nz, c]
        return copy(block, block, wzs.at[j], wzr.at[j], z_peer(j))

    for j in z_far:
        launch(functools.partial(wz, j))

    def meta_out(n):
        if n == 0:
            return copy(meta_nat, meta_own, ms.at[0], mr.at[0], sibling)
        return copy(meta_nat, meta_next, ms.at[n], mr.at[1], at_slab(before, n - 1))

    for n in range(3):
        launch(functools.partial(meta_out, n), diag)

    def f1_in(h, p):
        rows = pl.ds(pl.multiple_of((y % nyh) * blk + h * own, own), own)
        return copy(nrm.at[p], act.at[p, rows], f1s.at[p], f1r.at[h, p], sibling)

    def ring(i, p, h, way):
        rows = pl.ds(pl.multiple_of(i * blk + h * own, own), own)
        return copy(
            act.at[p, rows], act.at[p, rows], f2s.at[i, p, h, way], f2r.at[i, p, h],
            up if way == 0 else down,
        )

    here = y % nyh
    for i in range(nyh):
        apart = (y + ny - i - nyh * c) % ny
        back = (ny - apart) % ny
        for h in range(2):
            pending.append((functools.partial(ring, i, 0, h, 0), apart < nyh))
            pending.append((functools.partial(ring, i, 1, h, 0), apart < nyh - 1))
            pending.append((functools.partial(ring, i, 1, h, 1), back < nyh))
            pending.append((functools.partial(ring, i, 0, h, 1), back < nyh - 1))

    for h in (xl, 1 - xl):
        for p in range(2):
            if h is xl:

                @pl.when(jnp.logical_and(half == c, away))
                def _():
                    f1_in(h, p).wait_recv()

            else:

                @pl.when(half == c)
                def _():
                    f1_in(h, p).wait_recv()

            @pl.when(half == c)
            def _():
                ring(here, p, h, p).start()
                if nyh > 1:
                    ring(here, p, h, 1 - p).start()

    def turn(i):
        rows = pl.ds(pl.multiple_of(i * blk, blk), blk)
        for p in range(2):
            cols = pl.ds(pl.multiple_of(p * win + i * blk, blk), blk)
            xt[:, cols] = act[p, rows, :].T

    def project(i):
        rows = pl.ds(pl.multiple_of(i * blk, blk), blk)
        lane = lax.broadcasted_iota(jnp.int32, (blk, 2 * HD), 1)
        row = lax.broadcasted_iota(jnp.int32, (blk, 2 * HD), 0) + i * blk
        live = row < jnp.where(c == 0, meta_own[2:3, :], meta_own[3:4, :])
        for h in range(2):
            w = wbuf[h].reshape(d_model, 4 * HD)
            from_normed = dot(act[0, rows, :], w)
            from_upstream = dot(act[1, rows, :], w[:, 2 * HD :])
            pair = from_normed[:, : 2 * HD].astype(BF16)
            kv[h, rows, :] = pair
            kvt[h, :, rows] = pair.T
            query = from_normed[:, 2 * HD :].astype(BF16).astype(F32) * (HD**-0.5)
            qa[h, 0, rows, :] = jnp.where(lane < HD, query, 0.0).astype(BF16)
            qa[h, 1, rows, :] = jnp.where(
                jnp.logical_and(lane >= HD, live), from_upstream, 0.0
            ).astype(BF16)

    @pl.when(half == c)
    def _():
        turn(here)

    def wx(j):
        block = wbuf.at[xl, xh, :, c]
        return copy(block, block, wxs.at[j], wxr.at[j], x_peer(j))

    def wx_in(j):
        xx = (x + nxx - j) % nxx
        block = wbuf.at[xx % 2, xx // 2, :, c]
        return copy(block, block, wxs.at[j], wxr.at[j], x_peer(j))

    def wc(k):
        block = wbuf.at[:, :, :, k]
        return copy(block, block, wcs, wcr, sibling)

    def weights_x():
        for j in range(1, nz):
            wz_in(j).wait_recv()
        for j in x_far:
            launch(functools.partial(wx, j))

    def weights_core():
        for j in range(1, nxx):
            wx_in(j).wait_recv()
        launch(functools.partial(wc, c))

    def weights_done():
        wc(1 - c).wait_recv()

        @pl.when(jnp.logical_not(diag))
        def _():
            meta_out(0).wait_recv()

        meta_out(1).wait_recv()

    def hot():
        row_id = lax.broadcasted_iota(jnp.int32, (win, edge), 0) + c * win
        for k in range(2):
            hit = row_id == meta_next[k : k + 1, :]
            oh[:, k * edge : (k + 1) * edge] = hit.astype(F32).astype(BF16)

    def project_near(t):
        @pl.loop(0, nyh)
        def _(i):
            apart = (y + ny - i - nyh * c) % ny

            @pl.when(jnp.minimum(apart, ny - apart) < t)
            def _():
                project(i)

    stages = [weights_x, weights_core, weights_done]
    ready = False
    for t in range(1, nyh + 1):
        if stages:
            stages.pop(0)()
            if t == nyh:
                for stage in stages:
                    stage()
                stages = []
            if not stages:
                hot()
                project_near(t)
                ready = True
        from_below = (y + 2 * ny - t - nyh * c) % ny
        from_above = (y + 2 * ny + t - nyh * c) % ny
        has_below = from_below < nyh
        has_above = from_above < nyh

        def relay(i, p, h, way):
            ring(i, p, h, way).wait_recv()
            if t < (nyh if p == way else nyh - 1):
                ring(i, p, h, way).start()

        for h in (xl, 1 - xl):
            for way_first in (True, False):
                if t == nyh and not way_first:
                    continue

                @pl.when(has_below)
                def _():
                    relay(from_below, 0 if way_first else 1, h, 0)

                @pl.when(has_above)
                def _():
                    relay(from_above, 1 if way_first else 0, h, 1)

        if t < nyh:

            @pl.when(has_above)
            def _():
                if ready:
                    project(from_above)
                turn(from_above)

        @pl.when(has_below)
        def _():
            if ready:
                project(from_below)
            if t < nyh:
                turn(from_below)

    def edge_out(h, k):
        return copy(e_send.at[h, k], e_recv.at[h, c], es.at[h, k], er.at[h, c], at_slab(after, k))

    def edge_in(h, k):
        return copy(e_send.at[h, k], e_recv.at[h, k], es.at[h, k], er.at[h, k], sibling)

    for h in range(2):
        picked = dot(kvt[h, :, :win], oh[...]).astype(BF16)
        for k in range(2):
            e_send[h, k] = picked[:, k * edge : (k + 1) * edge]
            launch(functools.partial(edge_out, h, k))

    last = (y + ny - nyh - nyh * c) % ny

    @pl.when(last < nyh)
    def _():
        turn(last)

    keys = win + edge
    step = 256 if win % 256 == 0 else win
    has_edge = mine > 0
    count = jnp.where(c == 0, meta_own[2:3, :], meta_own[3:4, :])
    limit = jnp.concatenate([count] * (step // edge), 1)

    for h in range(2):

        @pl.loop(0, win // step)
        def _(n):
            q_rows = pl.ds(pl.multiple_of(n * step, step), step)
            key_live = lax.broadcasted_iota(jnp.int32, (win, step), 0) < limit
            scores = dot(kv[h, :win, :], qa[h, 0, q_rows, :], ((1,), (1,)))
            scores = jnp.where(key_live, scores, NEG)
            largest = jnp.max(scores, 0, keepdims=True)
            exponent = jnp.exp(scores - largest)
            g_prob = dot(kv[h, :win, :], qa[h, 1, q_rows, :], ((1,), (1,)))
            part_e[h, :, q_rows] = exponent
            part_g[h, :, q_rows] = g_prob
            stat[h, 0:1, q_rows] = largest
            stat[h, 1:2, q_rows] = jnp.sum(exponent, 0, keepdims=True)
            stat[h, 2:3, q_rows] = jnp.sum(exponent * g_prob, 0, keepdims=True)

    def scores_of(h):
        for k in range(2):
            edge_in(h, k).wait_recv()
        arrived = e_recv[h, 0].astype(F32) + e_recv[h, 1].astype(F32)
        kvt[h, :, win:] = arrived.astype(BF16)
        kv[h, win:, :] = arrived.T.astype(BF16)

        @pl.loop(0, win // step)
        def _(n):
            q_rows = pl.ds(pl.multiple_of(n * step, step), step)
            scores = dot(kv[h, win:, :], qa[h, 0, q_rows, :], ((1,), (1,)))
            scores = jnp.where(has_edge, scores, NEG)
            own_largest = stat[h, 0:1, q_rows]
            largest = jnp.maximum(own_largest, jnp.max(scores, 0, keepdims=True))
            exponent = jnp.exp(scores - largest)
            g_prob = dot(kv[h, win:, :], qa[h, 1, q_rows, :], ((1,), (1,)))
            shrink = jnp.exp(own_largest - largest)
            norm = 1.0 / (shrink * stat[h, 1:2, q_rows] + jnp.sum(exponent, 0, keepdims=True))
            centre = norm * (
                shrink * stat[h, 2:3, q_rows] + jnp.sum(exponent * g_prob, 0, keepdims=True)
            )
            probs = exponent * norm
            wts[h, win:, q_rows] = probs.astype(BF16)
            gsc[h, win:, q_rows] = (probs * (g_prob - centre)).astype(BF16)
            own_probs = part_e[h, :, q_rows] * (shrink * norm)
            wts[h, :win, q_rows] = own_probs.astype(BF16)
            gsc[h, :win, q_rows] = (own_probs * (part_g[h, :, q_rows] - centre)).astype(BF16)

        g_send[h] = (dot(gsc[h, win:, :], qa[h, 0]) + dot(wts[h, win:, :], qa[h, 1])).astype(BF16)

    def grad_out(h, k):
        return copy(g_send.at[h], g_recv.at[h, c], gs.at[h, k], gr.at[h, c], at_slab(before, k))

    def grad_in(h, k):
        return copy(g_send.at[h], g_recv.at[h, k], gs.at[h, k], gr.at[h, k], sibling)

    for h in range(2):
        scores_of(h)
        for k in range(2):
            launch(functools.partial(grad_out, h, k))

    row_limit = jnp.concatenate([count] * (win // edge), 1)
    lane = lax.broadcasted_iota(jnp.int32, (HD, win), 1)
    side = lax.broadcasted_iota(jnp.int32, (win, 2 * HD), 1)
    for h in range(2):
        cols = pl.ds(h * 2 * HD, 2 * HD)
        attended = jnp.where(lane < row_limit, dot(kvt[h, HD:, :], wts[h]), 0.0)
        g_query = dot(kvt[h, :HD, :], gsc[h]) * (HD**-0.5)
        pair = jnp.concatenate([g_query, attended], 0).T
        qab[:win, cols] = jnp.where(side < HD, pair, 0.0).astype(BF16)
        qab[win:, cols] = jnp.where(side >= HD, pair, 0.0).astype(BF16)

    def dc(q, k):
        return copy(dwb.at[q, :, :, :, k], r1.at[q], dcs.at[q], dcr.at[q], sibling)

    def dx(q, j):
        xx = (x + j) % nxx
        return copy(
            s2.at[q, xx % 2, xx // 2], r2.at[q, j], dxs.at[q, j], dxr.at[q, j], x_peer(j)
        )

    def dz(j):
        return copy(s3.at[(z + j) % nz], r3.at[j], dzs.at[j], dzr.at[j], z_peer(j))

    def weights_start(q, grad_w):
        blocks = grad_w.reshape(nxh, nz, 2, wr, 4 * HD)
        for h in range(2):
            block = blocks[:, :, :, :, h * 2 * HD : (h + 1) * 2 * HD]
            dwf[q, h] = block
            dwb[q, h] = block.astype(BF16)
        launch(functools.partial(dc, q, 1 - c))

    def weights_cross(q):
        dc(q, 1 - c).wait_recv()
        for h in range(2):
            s2[q, h] = (dwf[q, h, :, :, c] + r1[q, h].astype(F32)).astype(BF16)
        for j in x_far:
            launch(functools.partial(dx, q, j))

    def weights_total(q):
        total = dwf[q, xl, xh, :, c] + r1[q, xl, xh].astype(F32)
        for j in range(1, nxx):
            dx(q, j).wait_recv()
            total += r2[q, j].astype(F32)
        tot[:, q] = total
        s3[:, q] = total.astype(BF16)

    def weights_spread():
        for j in z_far:
            launch(functools.partial(dz, j))

    weights_start(1, dot(xt[...], qab[...]))

    for h in range(2):
        cols = pl.ds(h * 2 * HD, 2 * HD)
        own_pair = dot(gsc[h, :win, :], qa[h, 0]) + dot(wts[h, :win, :], qa[h, 1])
        for k in range(2):
            grad_in(h, k).wait_recv()
        returned = dot(oh[...], g_recv[h].reshape(2 * edge, 2 * HD))
        gkvb[:, cols] = (own_pair + returned).astype(BF16)


    def hops(way, part):
        return nyh if way == part else nyh - 1

    def chain_link(way, part, i, h):
        return copy(
            csd.at[way, part, i, h], crv.at[way, part, i, h],
            ccs.at[way, part, i, h], ccr.at[way, part, i, h], up if way == 0 else down,
        )

    def chain_end(way, part, i, h, yy):
        return copy(
            csd.at[way, part, i, h], orv.at[way, part],
            ows.at[way, part, h], owr.at[way, part], at(yy, h, xh, z, xl),
        )

    def own_out(h):
        return copy(osd.at[h], oself, oss.at[h], osr, at(y, h, xh, z, xl))

    def chain_piece(way, part, r, h):
        yy = (y + (r if way == 0 else ny - r)) % ny
        i = (yy + ny - nyh * c) % ny
        held = i < nyh

        @pl.when(held)
        def _():
            total = pvf[i, h * own : (h + 1) * own, part * halfcol : (part + 1) * halfcol]
            if r < hops(way, part):
                chain_link(way, part, i, h).wait_recv()
                total += crv[way, part, i, h].astype(F32)
            csd[way, part, i, h] = total.astype(BF16)

        if r > 1:
            launch(functools.partial(chain_link, way, part, i, h), held)
        else:
            launch(functools.partial(chain_end, way, part, i, h, yy), held)

    def chain(r):
        for h in range(2):
            for way in range(2):
                chain_piece(way, way, r, h)
        if r > 1:
            for h in range(2):
                for way in range(2):
                    chain_piece(way, 1 - way, r - 1, h)

    grads = jnp.concatenate(
        [gkvb[:, : 2 * HD], qab[:win, : 2 * HD], gkvb[:, 2 * HD :], qab[:win, 2 * HD :]], 1
    )
    flat = [wbuf[h].reshape(d_model, 4 * HD) for h in range(2)]
    width = halfcol // 2
    for n in range(4):
        cols = slice(n * width, (n + 1) * width)
        both = jnp.concatenate([w[cols, :] for w in flat], 1)
        pvf[:, :, cols] = dot(grads, both, ((1,), (1,))).reshape(nyh, blk, width)

    chain(nyh)

    @pl.when(half == c)
    def _():
        for h in range(2):
            osd[h] = pvf[here, h * own : (h + 1) * own, :].astype(BF16)

    for h in range(2):
        launch(
            functools.partial(own_out, h),
            jnp.logical_and(half == c, jnp.logical_or(xl != c, h != xl)),
        )

    @pl.when(at_home)
    def _():
        oself[...] = osd[xl]

    weights_start(0, dot(xt[:, :win], gkvb[...]))
    weights_cross(1)
    weights_cross(0)
    for r in range(nyh - 1, 0, -1):
        if r == 1:
            weights_total(0)
            weights_spread()
        chain(r)
        if r == nyh - 1:
            weights_total(1)

    def owner_in(way, part):
        return copy(
            csd.at[way, part, 0, 0], orv.at[way, part],
            ows.at[way, part, 0], owr.at[way, part], sibling,
        )

    for way in range(2):
        for part in range(2):
            owner_in(way, part).wait_recv()

    @pl.when(away)
    def _():
        own_out_arrived = copy(osd.at[0], oself, oss.at[0], osr, sibling)
        own_out_arrived.wait_recv()

    mine_sum = oself[...].astype(F32) + jnp.concatenate(
        [orv[0, part].astype(F32) + orv[1, part].astype(F32) for part in range(2)], 1
    )
    g_hat = mine_sum * gain
    normal_own = nx[...]
    g_tok = cot[...].astype(F32) + inv[:, 0:1] * (
        g_hat
        - jnp.mean(g_hat, 1, keepdims=True)
        - normal_own * jnp.mean(g_hat * normal_own, 1, keepdims=True)
    )
    out_tok[...] = g_tok.astype(BF16)

    final = tot[z]
    for j in range(1, nz):
        dz(j).wait_recv()
        final += r3[j].astype(F32)
    out_qkv[...] = jnp.concatenate([final[1, :, :HD], final[0]], 1)
    out_o[...] = final[1, :, HD:]

    drain()


def write_out(tok, qkv, o, out_tok, out_qkv, out_o, sems):
    moves = [
        pltpu.make_async_copy(src, dst, sems.at[n])
        for n, (src, dst) in enumerate(((tok, out_tok), (qkv, out_qkv), (o, out_o)))
    ]
    for move in moves:
        move.start()
    for move in moves:
        move.wait()


def on_device(nxh, tokens, cotangent, w_qkv, w_out, mod_scale, mod_shift, mod_gate, counts, edge_index):
    ny = lax.axis_size("enc") // 2
    nz = lax.axis_size("slab") // (2 * nxh)
    own, d_model = tokens.shape
    edge = edge_index.shape[1]
    win = own * ny
    wr = w_qkv.shape[0]
    nyh, nxx = ny // 2, 2 * nxh
    wide = 4 * HD
    dma = pltpu.SemaphoreType.DMA
    vmem = pl.BlockSpec(memory_space=pltpu.VMEM)
    anywhere = pl.BlockSpec(memory_space=pltpu.MemorySpace.HBM)
    keys = win + edge
    blk = 2 * own
    scratch = [
        pltpu.VMEM((own, d_model), BF16),
        pltpu.VMEM((own, d_model), BF16),
        pltpu.VMEM((wr, 3 * HD), BF16),
        pltpu.VMEM((wr, HD), BF16),
        pltpu.VMEM((1, d_model), F32),
        pltpu.VMEM((1, d_model), F32),
        pltpu.VMEM((1, d_model), F32),
        pltpu.SMEM((2,), jnp.int32),
        pltpu.VMEM((2, edge), jnp.int32),
        pltpu.VMEM((2, own, d_model), BF16),
        pltpu.VMEM((own, d_model), F32),
        pltpu.VMEM((own, 128), F32),
        pltpu.VMEM((2, win, d_model), BF16),
        pltpu.VMEM((d_model, 2 * win), BF16),
        pltpu.VMEM((2, nxh, nz, 2, wr, wide), BF16),
        pltpu.VMEM((8, edge), jnp.int32),
        pltpu.VMEM((8, edge), jnp.int32),
        pltpu.VMEM((8, edge), jnp.int32),
        pltpu.VMEM((2, keys, 2 * HD), BF16),
        pltpu.VMEM((2, 2 * HD, keys), BF16),
        pltpu.VMEM((2, 2, win, 2 * HD), BF16),
        pltpu.VMEM((win, 2 * edge), BF16),
        pltpu.VMEM((2, 2, 2 * HD, edge), BF16),
        pltpu.VMEM((2, 2, 2 * HD, edge), BF16),
        pltpu.VMEM((2, edge, 2 * HD), BF16),
        pltpu.VMEM((2, 2, edge, 2 * HD), BF16),
        pltpu.VMEM((2, keys, win), BF16),
        pltpu.VMEM((2, keys, win), BF16),
        pltpu.VMEM((2, win, win), F32),
        pltpu.VMEM((2, win, win), F32),
        pltpu.VMEM((2, 8, win), F32),
        pltpu.VMEM((win, wide), BF16),
        pltpu.VMEM((2 * win, wide), BF16),
        pltpu.VMEM((nyh, blk, d_model), F32),
        pltpu.VMEM((2, 2, nyh, 2, own, d_model // 2), BF16),
        pltpu.VMEM((2, 2, nyh, 2, own, d_model // 2), BF16),
        pltpu.VMEM((2, own, d_model), BF16),
        pltpu.VMEM((own, d_model), BF16),
        pltpu.VMEM((2, 2, own, d_model // 2), BF16),
        pltpu.VMEM((2, 2, nxh, nz, 2, wr, 2 * HD), F32),
        pltpu.VMEM((2, 2, nxh, nz, 2, wr, 2 * HD), BF16),
        pltpu.VMEM((2, 2, nxh, nz, wr, 2 * HD), BF16),
        pltpu.VMEM((2, 2, nxh, nz, wr, 2 * HD), BF16),
        pltpu.VMEM((2, nxx, nz, wr, 2 * HD), BF16),
        pltpu.VMEM((nz, 2, wr, 2 * HD), F32),
        pltpu.VMEM((nz, 2, wr, 2 * HD), BF16),
        pltpu.VMEM((nz, 2, wr, 2 * HD), BF16),
        dma((9,)),
        dma((2,)), dma((2, 2)), dma((nyh, 2, 2, 2)), dma((nyh, 2, 2)),
        dma((nz,)), dma((nz,)), dma((nxx,)), dma((nxx,)), dma, dma,
        dma((3,)), dma((2,)), dma((2, 2)), dma((2, 2)), dma((2, 2)), dma((2, 2)),
        dma((2,)), dma((2,)), dma((2, nxx)), dma((2, nxx)), dma((nz,)), dma((nz,)),
        dma((2, 2, nyh, 2)), dma((2, 2, nyh, 2)), dma((2, 2, 2)), dma((2, 2)), dma((2,)), dma,
    ]
    grad_tokens, grad_qkv, grad_out = pl.pallas_call(
        functools.partial(kernel, ny, nxh, nz, win, edge),
        out_shape=(
            jax.ShapeDtypeStruct((own, d_model), BF16),
            jax.ShapeDtypeStruct((wr, 3 * HD), F32),
            jax.ShapeDtypeStruct((wr, HD), F32),
        ),
        in_specs=[anywhere] * 9,
        out_specs=(vmem, vmem, vmem),
        scratch_shapes=scratch,
        compiler_params=pltpu.CompilerParams(collective_id=0, has_side_effects=True, vmem_limit_bytes=36 * 1024 * 1024),
    )(
        *(
            pltpu.with_memory_space_constraint(a, pltpu.MemorySpace.HBM)
            for a in (
                tokens, cotangent, w_qkv, w_out.T,
                mod_scale[None, :], mod_shift[None, :], mod_gate[None, :], counts, edge_index,
            )
        )
    )
    grad_tokens, grad_qkv, grad_out = pl.pallas_call(
        write_out,
        out_shape=tuple(jax.ShapeDtypeStruct(a.shape, a.dtype) for a in (grad_tokens, grad_qkv, grad_out)),
        in_specs=[vmem] * 3,
        out_specs=(anywhere,) * 3,
        scratch_shapes=[dma((3,))],
        compiler_params=pltpu.CompilerParams(vmem_limit_bytes=4 * 1024 * 1024),
    )(grad_tokens, grad_qkv, grad_out)
    return (grad_tokens, grad_qkv, grad_out.T)


def solution(mesh, nxh=2):
    placed = (
        P(("slab", "enc"), None),
        P(("slab", "enc"), None),
        P("slab", "enc"),
        P("enc", "slab"),
        P(),
        P(),
        P(),
        P("slab"),
        P("slab", None),
    )
    return jax.shard_map(
        functools.partial(on_device, nxh),
        mesh=mesh,
        in_specs=placed,
        out_specs=(P(("slab", "enc"), None), P("slab", "enc"), P("enc", "slab")),
        check_vma=False,
    )
```

```python
import functools

import jax
import jax.numpy as jnp
from jax import lax
from jax.experimental import pallas as pl
from jax.experimental.pallas import tpu as pltpu
from jax.sharding import PartitionSpec as P

HD = 64
EPS = 1e-06
NEG = -1000000000.0
MESH = pl.DeviceIdType.MESH
F32 = jnp.float32
BF16 = jnp.bfloat16


def dot(a, b, dims=((1,), (0,))):
    return lax.dot_general(a, b, (dims, ((), ())), preferred_element_type=F32)


def kernel(
    ny, nxh, nz, win, edge,
    tok_in, cot_in, wq_in, wo_in, scale_in, shift_in, gate_in, counts_in, edges_in,
    out_tok, out_qkv, out_o,
    tok, cot, wq, wo, scale, shift, gate, counts, edges,
    nrm, nx, inv, act, xt, wbuf, meta_nat, meta_own, meta_next,
    kv, kvt, qa, oh, e_send, e_recv, g_send, g_recv, wts, gsc, part_e, part_g, stat, gkvb, qab,
    pvf, csd, crv, osd, oself, orv, dwf, dwb, r1, s2, r2, tot, s3, r3,
    ins, f1s, f1r, f2s, f2r, wzs, wzr, wxs, wxr, wcs, wcr,
    ms, mr, es, er, gs, gr, dcs, dcr, dxs, dxr, dzs, dzr, ccs, ccr, ows, owr, oss, osr,
):
    ns = nxh * nz * 2
    nyh = ny // 2
    nxx = 2 * nxh
    z_far = sorted(range(1, nz), key=lambda j: -min(j, nz - j))
    x_far = sorted(range(1, nxx), key=lambda j: -min(j, nxx - j))
    own = tok.shape[0]
    blk = 2 * own
    d_model = tok.shape[1]
    wr = wq.shape[0]
    halfcol = d_model // 2

    enc = lax.axis_index("enc")
    slab = lax.axis_index("slab")
    y, xl = enc // 2, enc % 2
    xh, z, c = slab // (2 * nz), (slab // 2) % nz, slab % 2
    x = xh * 2 + xl
    mine = xh * 2 * nz + z * 2 + xl
    after = (mine + 1) % ns
    before = (mine + ns - 1) % ns
    half = y // nyh

    def at(y_, xl_, xh_, z_, c_):
        return {"enc": y_ * 2 + xl_, "slab": xh_ * (2 * nz) + z_ * 2 + c_}

    def at_slab(s_, c_):
        return {"enc": y * 2 + s_ % 2, "slab": (s_ // 2) * 2 + c_}

    sibling = at(y, xl, xh, z, 1 - c)
    up = at((y + 1) % ny, xl, xh, z, c)
    down = at((y + ny - 1) % ny, xl, xh, z, c)

    def z_peer(j):
        return at(y, xl, xh, (z + j) % nz, c)

    def x_peer(j):
        xx = (x + j) % nxx
        return at(y, xx % 2, xx // 2, z, c)

    def copy(src, dst, send, recv, to):
        return pltpu.make_async_remote_copy(
            src_ref=src, dst_ref=dst, send_sem=send, recv_sem=recv, device_id=to, device_id_type=MESH
        )

    at_home = jnp.logical_and(c == xl, half == c)
    away = jnp.logical_not(at_home)
    diag = c == xl

    pending = []

    def launch(make, when=None):
        if when is None:
            make().start()
            pending.append((make, None))
        else:

            @pl.when(when)
            def _():
                make().start()

            pending.append((make, when))

    def drain():
        for make, when in pending:
            if when is None:
                make().wait_send()
            else:

                @pl.when(when)
                def _():
                    make().wait_send()

    arrivals = [
        pltpu.make_async_copy(src, dst, ins.at[n])
        for n, (src, dst) in enumerate(
            (
                (tok_in, tok), (cot_in, cot), (wq_in, wq), (wo_in, wo), (scale_in, scale),
                (shift_in, shift), (gate_in, gate), (counts_in, counts), (edges_in, edges),
            )
        )
    ]
    for arrival in arrivals:
        arrival.start()

    barrier = pltpu.get_barrier_semaphore()

    def greet(to):
        pl.semaphore_signal(barrier, inc=1, device_id=to, device_id_type=MESH)

    for j in z_far:
        greet(z_peer(j))
    for j in x_far:
        greet(x_peer(j))
    greet(up)
    greet(down)
    greet(sibling)
    for k in range(2):
        greet(at_slab(after, k))
        greet(at_slab(before, k))

    @pl.when(half == c)
    def _():
        greet(at(y, 1 - xl, xh, z, xl))

    @pl.when(jnp.logical_and(half == c, xl != c))
    def _():
        greet(at(y, xl, xh, z, xl))

    above, below = (y + 1) % ny, (y + ny - 1) % ny
    greet(at(above, c, xh, z, half))
    greet(at(below, c, xh, z, half))

    @pl.when(away)
    def _():
        greet(at(y, c, xh, z, half))

    def count_of(flag):
        return flag.astype(jnp.int32)

    greeted = (
        3 + (nz - 1) + (nxx - 1) + 4 + 1
        - 2 * count_of(at_home)
        + 2 * count_of(half == c)
        + 2 * count_of(above // nyh == c)
        + 2 * count_of(below // nyh == c)
    )

    for arrival in arrivals:
        arrival.wait()

    widened = tok[...].astype(F32)
    average = jnp.mean(widened, 1, keepdims=True)
    centred = widened - average
    variance = jnp.mean(centred * centred, 1, keepdims=True)
    inv_std = lax.rsqrt(variance + EPS)
    normal = centred * inv_std
    gain = 1.0 + scale[...]
    nx[...] = normal
    inv[...] = jnp.broadcast_to(inv_std, inv.shape)
    nrm[0] = (normal * gain + shift[...]).astype(BF16)
    nrm[1] = (cot[...].astype(F32) * gate[...]).astype(BF16)

    hd = HD
    wq_here = wq[...]
    wbuf[xl, xh, z, c] = jnp.concatenate([wq_here[:, hd : 3 * hd], wq_here[:, :hd], wo[...]], 1)

    meta_nat[...] = jnp.zeros(meta_nat.shape, jnp.int32)
    meta_nat[0:2, :] = edges[...]
    meta_nat[2:3, :] = jnp.full((1, edge), counts[0], jnp.int32)
    meta_nat[3:4, :] = jnp.full((1, edge), counts[1], jnp.int32)

    @pl.when(diag)
    def _():
        meta_own[...] = meta_nat[...]

    r_own = (y % nyh) * blk + xl * own
    home = at(y, c, xh, z, half)

    @pl.when(at_home)
    def _():
        for p in range(2):
            act[p, pl.ds(pl.multiple_of(r_own, own), own), :] = nrm[p]

    pl.semaphore_wait(barrier, greeted)

    def f1(p):
        return copy(
            nrm.at[p],
            act.at[p, pl.ds(pl.multiple_of(r_own, own), own)],
            f1s.at[p],
            f1r.at[xl, p],
            home,
        )

    for p in range(2):
        launch(functools.partial(f1, p), away)

    def wz(j):
        return copy(wbuf.at[xl, xh, z, c], wbuf.at[xl, xh, z, c], wzs.at[j], wzr.at[j], z_peer(j))

    def wz_in(j):
        block = wbuf.at[xl, xh, (z + nz - j) % nz, c]
        return copy(block, block, wzs.at[j], wzr.at[j], z_peer(j))

    for j in z_far:
        launch(functools.partial(wz, j))

    def meta_out(n):
        if n == 0:
            return copy(meta_nat, meta_own, ms.at[0], mr.at[0], sibling)
        return copy(meta_nat, meta_next, ms.at[n], mr.at[1], at_slab(before, n - 1))

    for n in range(3):
        launch(functools.partial(meta_out, n), diag)

    def f1_in(h, p):
        rows = pl.ds(pl.multiple_of((y % nyh) * blk + h * own, own), own)
        return copy(nrm.at[p], act.at[p, rows], f1s.at[p], f1r.at[h, p], sibling)

    def ring(i, p, h, way):
        rows = pl.ds(pl.multiple_of(i * blk + h * own, own), own)
        return copy(
            act.at[p, rows], act.at[p, rows], f2s.at[i, p, h, way], f2r.at[i, p, h],
            up if way == 0 else down,
        )

    here = y % nyh
    for i in range(nyh):
        apart = (y + ny - i - nyh * c) % ny
        back = (ny - apart) % ny
        for h in range(2):
            pending.append((functools.partial(ring, i, 0, h, 0), apart < nyh))
            pending.append((functools.partial(ring, i, 1, h, 0), apart < nyh - 1))
            pending.append((functools.partial(ring, i, 1, h, 1), back < nyh))
            pending.append((functools.partial(ring, i, 0, h, 1), back < nyh - 1))

    for h in (xl, 1 - xl):
        for p in range(2):
            if h is xl:

                @pl.when(jnp.logical_and(half == c, away))
                def _():
                    f1_in(h, p).wait_recv()

            else:

                @pl.when(half == c)
                def _():
                    f1_in(h, p).wait_recv()

            @pl.when(half == c)
            def _():
                ring(here, p, h, p).start()
                if nyh > 1:
                    ring(here, p, h, 1 - p).start()

    def turn(i):
        rows = pl.ds(pl.multiple_of(i * blk, blk), blk)
        for p in range(2):
            cols = pl.ds(pl.multiple_of(p * win + i * blk, blk), blk)
            xt[:, cols] = act[p, rows, :].T

    def project(i):
        rows = pl.ds(pl.multiple_of(i * blk, blk), blk)
        lane = lax.broadcasted_iota(jnp.int32, (blk, 2 * HD), 1)
        row = lax.broadcasted_iota(jnp.int32, (blk, 2 * HD), 0) + i * blk
        live = row < jnp.where(c == 0, meta_own[2:3, :], meta_own[3:4, :])
        for h in range(2):
            w = wbuf[h].reshape(d_model, 4 * HD)
            from_normed = dot(act[0, rows, :], w)
            from_upstream = dot(act[1, rows, :], w[:, 2 * HD :])
            pair = from_normed[:, : 2 * HD].astype(BF16)
            kv[h, rows, :] = pair
            kvt[h, :, rows] = pair.T
            query = from_normed[:, 2 * HD :].astype(BF16).astype(F32) * (HD**-0.5)
            qa[h, 0, rows, :] = jnp.where(lane < HD, query, 0.0).astype(BF16)
            qa[h, 1, rows, :] = jnp.where(
                jnp.logical_and(lane >= HD, live), from_upstream, 0.0
            ).astype(BF16)

    @pl.when(half == c)
    def _():
        turn(here)

    def wx(j):
        block = wbuf.at[xl, xh, :, c]
        return copy(block, block, wxs.at[j], wxr.at[j], x_peer(j))

    def wx_in(j):
        xx = (x + nxx - j) % nxx
        block = wbuf.at[xx % 2, xx // 2, :, c]
        return copy(block, block, wxs.at[j], wxr.at[j], x_peer(j))

    def wc(k):
        block = wbuf.at[:, :, :, k]
        return copy(block, block, wcs, wcr, sibling)

    def weights_x():
        for j in range(1, nz):
            wz_in(j).wait_recv()
        for j in x_far:
            launch(functools.partial(wx, j))

    def weights_core():
        for j in range(1, nxx):
            wx_in(j).wait_recv()
        launch(functools.partial(wc, c))

    def weights_done():
        wc(1 - c).wait_recv()

        @pl.when(jnp.logical_not(diag))
        def _():
            meta_out(0).wait_recv()

        meta_out(1).wait_recv()

    def hot():
        row_id = lax.broadcasted_iota(jnp.int32, (win, edge), 0) + c * win
        for k in range(2):
            hit = row_id == meta_next[k : k + 1, :]
            oh[:, k * edge : (k + 1) * edge] = hit.astype(F32).astype(BF16)

    def project_near(t):
        @pl.loop(0, nyh)
        def _(i):
            apart = (y + ny - i - nyh * c) % ny

            @pl.when(jnp.minimum(apart, ny - apart) < t)
            def _():
                project(i)

    stages = [weights_x, weights_core, weights_done]
    ready = False
    for t in range(1, nyh + 1):
        if stages:
            stages.pop(0)()
            if t == nyh:
                for stage in stages:
                    stage()
                stages = []
            if not stages:
                hot()
                project_near(t)
                ready = True
        from_below = (y + 2 * ny - t - nyh * c) % ny
        from_above = (y + 2 * ny + t - nyh * c) % ny
        has_below = from_below < nyh
        has_above = from_above < nyh

        def relay(i, p, h, way):
            ring(i, p, h, way).wait_recv()
            if t < (nyh if p == way else nyh - 1):
                ring(i, p, h, way).start()

        for h in (xl, 1 - xl):
            for way_first in (True, False):
                if t == nyh and not way_first:
                    continue

                @pl.when(has_below)
                def _():
                    relay(from_below, 0 if way_first else 1, h, 0)

                @pl.when(has_above)
                def _():
                    relay(from_above, 1 if way_first else 0, h, 1)

        if t < nyh:

            @pl.when(has_above)
            def _():
                if ready:
                    project(from_above)
                turn(from_above)

        @pl.when(has_below)
        def _():
            if ready:
                project(from_below)
            if t < nyh:
                turn(from_below)

    def edge_out(h, k):
        return copy(e_send.at[h, k], e_recv.at[h, c], es.at[h, k], er.at[h, c], at_slab(after, k))

    def edge_in(h, k):
        return copy(e_send.at[h, k], e_recv.at[h, k], es.at[h, k], er.at[h, k], sibling)

    for h in range(2):
        picked = dot(kvt[h, :, :win], oh[...]).astype(BF16)
        for k in range(2):
            e_send[h, k] = picked[:, k * edge : (k + 1) * edge]
            launch(functools.partial(edge_out, h, k))

    last = (y + ny - nyh - nyh * c) % ny

    @pl.when(last < nyh)
    def _():
        turn(last)

    keys = win + edge
    step = 256 if win % 256 == 0 else win
    has_edge = mine > 0
    count = jnp.where(c == 0, meta_own[2:3, :], meta_own[3:4, :])
    limit = jnp.concatenate([count] * (step // edge), 1)

    for h in range(2):

        @pl.loop(0, win // step)
        def _(n):
            q_rows = pl.ds(pl.multiple_of(n * step, step), step)
            key_live = lax.broadcasted_iota(jnp.int32, (win, step), 0) < limit
            scores = dot(kv[h, :win, :], qa[h, 0, q_rows, :], ((1,), (1,)))
            scores = jnp.where(key_live, scores, NEG)
            largest = jnp.max(scores, 0, keepdims=True)
            exponent = jnp.exp(scores - largest)
            g_prob = dot(kv[h, :win, :], qa[h, 1, q_rows, :], ((1,), (1,)))
            part_e[h, :, q_rows] = exponent
            part_g[h, :, q_rows] = g_prob
            stat[h, 0:1, q_rows] = largest
            stat[h, 1:2, q_rows] = jnp.sum(exponent, 0, keepdims=True)
            stat[h, 2:3, q_rows] = jnp.sum(exponent * g_prob, 0, keepdims=True)

    def scores_of(h):
        for k in range(2):
            edge_in(h, k).wait_recv()
        arrived = e_recv[h, 0].astype(F32) + e_recv[h, 1].astype(F32)
        kvt[h, :, win:] = arrived.astype(BF16)
        kv[h, win:, :] = arrived.T.astype(BF16)

        @pl.loop(0, win // step)
        def _(n):
            q_rows = pl.ds(pl.multiple_of(n * step, step), step)
            scores = dot(kv[h, win:, :], qa[h, 0, q_rows, :], ((1,), (1,)))
            scores = jnp.where(has_edge, scores, NEG)
            own_largest = stat[h, 0:1, q_rows]
            largest = jnp.maximum(own_largest, jnp.max(scores, 0, keepdims=True))
            exponent = jnp.exp(scores - largest)
            g_prob = dot(kv[h, win:, :], qa[h, 1, q_rows, :], ((1,), (1,)))
            shrink = jnp.exp(own_largest - largest)
            norm = 1.0 / (shrink * stat[h, 1:2, q_rows] + jnp.sum(exponent, 0, keepdims=True))
            centre = norm * (
                shrink * stat[h, 2:3, q_rows] + jnp.sum(exponent * g_prob, 0, keepdims=True)
            )
            probs = exponent * norm
            wts[h, win:, q_rows] = probs.astype(BF16)
            gsc[h, win:, q_rows] = (probs * (g_prob - centre)).astype(BF16)
            own_probs = part_e[h, :, q_rows] * (shrink * norm)
            wts[h, :win, q_rows] = own_probs.astype(BF16)
            gsc[h, :win, q_rows] = (own_probs * (part_g[h, :, q_rows] - centre)).astype(BF16)

        g_send[h] = (dot(gsc[h, win:, :], qa[h, 0]) + dot(wts[h, win:, :], qa[h, 1])).astype(BF16)

    def grad_out(h, k):
        return copy(g_send.at[h], g_recv.at[h, c], gs.at[h, k], gr.at[h, c], at_slab(before, k))

    def grad_in(h, k):
        return copy(g_send.at[h], g_recv.at[h, k], gs.at[h, k], gr.at[h, k], sibling)

    for h in range(2):
        scores_of(h)
        for k in range(2):
            launch(functools.partial(grad_out, h, k))

    row_limit = jnp.concatenate([count] * (win // edge), 1)
    lane = lax.broadcasted_iota(jnp.int32, (HD, win), 1)
    side = lax.broadcasted_iota(jnp.int32, (win, 2 * HD), 1)
    for h in range(2):
        cols = pl.ds(h * 2 * HD, 2 * HD)
        attended = jnp.where(lane < row_limit, dot(kvt[h, HD:, :], wts[h]), 0.0)
        g_query = dot(kvt[h, :HD, :], gsc[h]) * (HD**-0.5)
        pair = jnp.concatenate([g_query, attended], 0).T
        qab[:win, cols] = jnp.where(side < HD, pair, 0.0).astype(BF16)
        qab[win:, cols] = jnp.where(side >= HD, pair, 0.0).astype(BF16)

    def dc(q, k):
        return copy(dwb.at[q, :, :, :, k], r1.at[q], dcs.at[q], dcr.at[q], sibling)

    def dx(q, j):
        xx = (x + j) % nxx
        return copy(
            s2.at[q, xx % 2, xx // 2], r2.at[q, j], dxs.at[q, j], dxr.at[q, j], x_peer(j)
        )

    def dz(j):
        return copy(s3.at[(z + j) % nz], r3.at[j], dzs.at[j], dzr.at[j], z_peer(j))

    def weights_start(q, grad_w):
        blocks = grad_w.reshape(nxh, nz, 2, wr, 4 * HD)
        for h in range(2):
            block = blocks[:, :, :, :, h * 2 * HD : (h + 1) * 2 * HD]
            dwf[q, h] = block
            dwb[q, h] = block.astype(BF16)
        launch(functools.partial(dc, q, 1 - c))

    def weights_cross(q):
        dc(q, 1 - c).wait_recv()
        for h in range(2):
            s2[q, h] = (dwf[q, h, :, :, c] + r1[q, h].astype(F32)).astype(BF16)
        for j in x_far:
            launch(functools.partial(dx, q, j))

    def weights_total(q):
        total = dwf[q, xl, xh, :, c] + r1[q, xl, xh].astype(F32)
        for j in range(1, nxx):
            dx(q, j).wait_recv()
            total += r2[q, j].astype(F32)
        tot[:, q] = total
        s3[:, q] = total.astype(BF16)

    def weights_spread():
        for j in z_far:
            launch(functools.partial(dz, j))

    weights_start(1, dot(xt[...], qab[...]))

    for h in range(2):
        cols = pl.ds(h * 2 * HD, 2 * HD)
        own_pair = dot(gsc[h, :win, :], qa[h, 0]) + dot(wts[h, :win, :], qa[h, 1])
        for k in range(2):
            grad_in(h, k).wait_recv()
        returned = dot(oh[...], g_recv[h].reshape(2 * edge, 2 * HD))
        gkvb[:, cols] = (own_pair + returned).astype(BF16)


    def hops(way, part):
        return nyh if way == part else nyh - 1

    def chain_link(way, part, i, h):
        return copy(
            csd.at[way, part, i, h], crv.at[way, part, i, h],
            ccs.at[way, part, i, h], ccr.at[way, part, i, h], up if way == 0 else down,
        )

    def chain_end(way, part, i, h, yy):
        return copy(
            csd.at[way, part, i, h], orv.at[way, part],
            ows.at[way, part, h], owr.at[way, part], at(yy, h, xh, z, xl),
        )

    def own_out(h):
        return copy(osd.at[h], oself, oss.at[h], osr, at(y, h, xh, z, xl))

    def chain_piece(way, part, r, h):
        yy = (y + (r if way == 0 else ny - r)) % ny
        i = (yy + ny - nyh * c) % ny
        held = i < nyh

        @pl.when(held)
        def _():
            total = pvf[i, h * own : (h + 1) * own, part * halfcol : (part + 1) * halfcol]
            if r < hops(way, part):
                chain_link(way, part, i, h).wait_recv()
                total += crv[way, part, i, h].astype(F32)
            csd[way, part, i, h] = total.astype(BF16)

        if r > 1:
            launch(functools.partial(chain_link, way, part, i, h), held)
        else:
            launch(functools.partial(chain_end, way, part, i, h, yy), held)

    def chain(r):
        for h in range(2):
            for way in range(2):
                chain_piece(way, way, r, h)
        if r > 1:
            for h in range(2):
                for way in range(2):
                    chain_piece(way, 1 - way, r - 1, h)

    grads = jnp.concatenate(
        [gkvb[:, : 2 * HD], qab[:win, : 2 * HD], gkvb[:, 2 * HD :], qab[:win, 2 * HD :]], 1
    )
    flat = [wbuf[h].reshape(d_model, 4 * HD) for h in range(2)]
    width = halfcol // 2
    for n in range(4):
        cols = slice(n * width, (n + 1) * width)
        both = jnp.concatenate([w[cols, :] for w in flat], 1)
        pvf[:, :, cols] = dot(grads, both, ((1,), (1,))).reshape(nyh, blk, width)

    chain(nyh)

    @pl.when(half == c)
    def _():
        for h in range(2):
            osd[h] = pvf[here, h * own : (h + 1) * own, :].astype(BF16)

    for h in range(2):
        launch(
            functools.partial(own_out, h),
            jnp.logical_and(half == c, jnp.logical_or(xl != c, h != xl)),
        )

    @pl.when(at_home)
    def _():
        oself[...] = osd[xl]

    weights_start(0, dot(xt[:, :win], gkvb[...]))
    weights_cross(1)
    weights_cross(0)
    for r in range(nyh - 1, 0, -1):
        if r == 1:
            weights_total(0)
            weights_spread()
        chain(r)
        if r == nyh - 1:
            weights_total(1)

    def owner_in(way, part):
        return copy(
            csd.at[way, part, 0, 0], orv.at[way, part],
            ows.at[way, part, 0], owr.at[way, part], sibling,
        )

    for way in range(2):
        for part in range(2):
            owner_in(way, part).wait_recv()

    @pl.when(away)
    def _():
        own_out_arrived = copy(osd.at[0], oself, oss.at[0], osr, sibling)
        own_out_arrived.wait_recv()

    mine_sum = oself[...].astype(F32) + jnp.concatenate(
        [orv[0, part].astype(F32) + orv[1, part].astype(F32) for part in range(2)], 1
    )
    g_hat = mine_sum * gain
    normal_own = nx[...]
    g_tok = cot[...].astype(F32) + inv[:, 0:1] * (
        g_hat
        - jnp.mean(g_hat, 1, keepdims=True)
        - normal_own * jnp.mean(g_hat * normal_own, 1, keepdims=True)
    )
    out_tok[...] = g_tok.astype(BF16)

    final = tot[z]
    for j in range(1, nz):
        dz(j).wait_recv()
        final += r3[j].astype(F32)
    out_qkv[...] = jnp.concatenate([final[1, :, :HD], final[0]], 1)
    out_o[...] = final[1, :, HD:]

    drain()


def write_out(tok, qkv, o, out_tok, out_qkv, out_o, sems):
    moves = [
        pltpu.make_async_copy(src, dst, sems.at[n])
        for n, (src, dst) in enumerate(((tok, out_tok), (qkv, out_qkv), (o, out_o)))
    ]
    for move in moves:
        move.start()
    for move in moves:
        move.wait()


def on_device(nxh, tokens, cotangent, w_qkv, w_out, mod_scale, mod_shift, mod_gate, counts, edge_index):
    ny = lax.axis_size("enc") // 2
    nz = lax.axis_size("slab") // (2 * nxh)
    own, d_model = tokens.shape
    edge = edge_index.shape[1]
    win = own * ny
    wr = w_qkv.shape[0]
    nyh, nxx = ny // 2, 2 * nxh
    wide = 4 * HD
    dma = pltpu.SemaphoreType.DMA
    vmem = pl.BlockSpec(memory_space=pltpu.VMEM)
    anywhere = pl.BlockSpec(memory_space=pltpu.MemorySpace.HBM)
    keys = win + edge
    blk = 2 * own
    scratch = [
        pltpu.VMEM((own, d_model), BF16),
        pltpu.VMEM((own, d_model), BF16),
        pltpu.VMEM((wr, 3 * HD), BF16),
        pltpu.VMEM((wr, HD), BF16),
        pltpu.VMEM((1, d_model), F32),
        pltpu.VMEM((1, d_model), F32),
        pltpu.VMEM((1, d_model), F32),
        pltpu.SMEM((2,), jnp.int32),
        pltpu.VMEM((2, edge), jnp.int32),
        pltpu.VMEM((2, own, d_model), BF16),
        pltpu.VMEM((own, d_model), F32),
        pltpu.VMEM((own, 128), F32),
        pltpu.VMEM((2, win, d_model), BF16),
        pltpu.VMEM((d_model, 2 * win), BF16),
        pltpu.VMEM((2, nxh, nz, 2, wr, wide), BF16),
        pltpu.VMEM((8, edge), jnp.int32),
        pltpu.VMEM((8, edge), jnp.int32),
        pltpu.VMEM((8, edge), jnp.int32),
        pltpu.VMEM((2, keys, 2 * HD), BF16),
        pltpu.VMEM((2, 2 * HD, keys), BF16),
        pltpu.VMEM((2, 2, win, 2 * HD), BF16),
        pltpu.VMEM((win, 2 * edge), BF16),
        pltpu.VMEM((2, 2, 2 * HD, edge), BF16),
        pltpu.VMEM((2, 2, 2 * HD, edge), BF16),
        pltpu.VMEM((2, edge, 2 * HD), BF16),
        pltpu.VMEM((2, 2, edge, 2 * HD), BF16),
        pltpu.VMEM((2, keys, win), BF16),
        pltpu.VMEM((2, keys, win), BF16),
        pltpu.VMEM((2, win, win), F32),
        pltpu.VMEM((2, win, win), F32),
        pltpu.VMEM((2, 8, win), F32),
        pltpu.VMEM((win, wide), BF16),
        pltpu.VMEM((2 * win, wide), BF16),
        pltpu.VMEM((nyh, blk, d_model), F32),
        pltpu.VMEM((2, 2, nyh, 2, own, d_model // 2), BF16),
        pltpu.VMEM((2, 2, nyh, 2, own, d_model // 2), BF16),
        pltpu.VMEM((2, own, d_model), BF16),
        pltpu.VMEM((own, d_model), BF16),
        pltpu.VMEM((2, 2, own, d_model // 2), BF16),
        pltpu.VMEM((2, 2, nxh, nz, 2, wr, 2 * HD), F32),
        pltpu.VMEM((2, 2, nxh, nz, 2, wr, 2 * HD), BF16),
        pltpu.VMEM((2, 2, nxh, nz, wr, 2 * HD), BF16),
        pltpu.VMEM((2, 2, nxh, nz, wr, 2 * HD), BF16),
        pltpu.VMEM((2, nxx, nz, wr, 2 * HD), BF16),
        pltpu.VMEM((nz, 2, wr, 2 * HD), F32),
        pltpu.VMEM((nz, 2, wr, 2 * HD), BF16),
        pltpu.VMEM((nz, 2, wr, 2 * HD), BF16),
        dma((9,)),
        dma((2,)), dma((2, 2)), dma((nyh, 2, 2, 2)), dma((nyh, 2, 2)),
        dma((nz,)), dma((nz,)), dma((nxx,)), dma((nxx,)), dma, dma,
        dma((3,)), dma((2,)), dma((2, 2)), dma((2, 2)), dma((2, 2)), dma((2, 2)),
        dma((2,)), dma((2,)), dma((2, nxx)), dma((2, nxx)), dma((nz,)), dma((nz,)),
        dma((2, 2, nyh, 2)), dma((2, 2, nyh, 2)), dma((2, 2, 2)), dma((2, 2)), dma((2,)), dma,
    ]
    grad_tokens, grad_qkv, grad_out = pl.pallas_call(
        functools.partial(kernel, ny, nxh, nz, win, edge),
        out_shape=(
            jax.ShapeDtypeStruct((own, d_model), BF16),
            jax.ShapeDtypeStruct((wr, 3 * HD), F32),
            jax.ShapeDtypeStruct((wr, HD), F32),
        ),
        in_specs=[anywhere] * 9,
        out_specs=(vmem, vmem, vmem),
        scratch_shapes=scratch,
        compiler_params=pltpu.CompilerParams(collective_id=0, has_side_effects=True, vmem_limit_bytes=36 * 1024 * 1024),
    )(
        *(
            pltpu.with_memory_space_constraint(a, pltpu.MemorySpace.HBM)
            for a in (
                tokens, cotangent, w_qkv, w_out.T,
                mod_scale[None, :], mod_shift[None, :], mod_gate[None, :], counts, edge_index,
            )
        )
    )
    grad_tokens, grad_qkv, grad_out = pl.pallas_call(
        write_out,
        out_shape=tuple(jax.ShapeDtypeStruct(a.shape, a.dtype) for a in (grad_tokens, grad_qkv, grad_out)),
        in_specs=[vmem] * 3,
        out_specs=(anywhere,) * 3,
        scratch_shapes=[dma((3,))],
        compiler_params=pltpu.CompilerParams(vmem_limit_bytes=4 * 1024 * 1024),
    )(grad_tokens, grad_qkv, grad_out)
    return (grad_tokens, grad_qkv, grad_out.T)


def solution(mesh, nxh=2):
    placed = (
        P(("slab", "enc"), None),
        P(("slab", "enc"), None),
        P("slab", "enc"),
        P("enc", "slab"),
        P(),
        P(),
        P(),
        P("slab"),
        P("slab", None),
    )
    return jax.shard_map(
        functools.partial(on_device, nxh),
        mesh=mesh,
        in_specs=placed,
        out_specs=(P(("slab", "enc"), None), P("slab", "enc"), P("enc", "slab")),
        check_vma=False,
    )
```
